8 devices in a mesh: dp: 1 (over z), tp: 8 (over y, x, core).
Axes of the slice: x: 2, y: 2, z: 1, core: 2. Of those that a mesh axis runs over, the one named last changes fastest.
Arguments:
- hidden: bfloat16 [16, 64, 5120], P('dp')
- tree_mask: int32 [16, 64, 64], P('dp')
- depth: int32 [16, 64], P('dp')
- ctx_len: int32 [16], P('dp')
- block_table: int32 [16, 32], P('dp')
- score_id: int32 [16, 64], P('dp')
- k_cache: bfloat16 [512, 16, 40, 128], P('dp', None, 'tp')
- v_cache: bfloat16 [512, 16, 40, 128], P('dp', None, 'tp')
- attn_norm: bfloat16 [5120], replicated
- w_q: bfloat16 [5120, 5120], P(None, 'tp')
- w_k: bfloat16 [5120, 5120], P(None, 'tp')
- w_v: bfloat16 [5120, 5120], P(None, 'tp')
- w_o: bfloat16 [5120, 5120], P('tp')
- mlp_norm: bfloat16 [5120], replicated
- w_gate: bfloat16 [5120, 13824], P(None, 'tp')
- w_up: bfloat16 [5120, 13824], P(None, 'tp')
- w_down: bfloat16 [13824, 5120], P('tp')
- final_norm: bfloat16 [5120], replicated
- w_lm: bfloat16 [5120, 32000], P(None, 'tp')
Outputs:
- output 1: float32 [16, 64], P('dp')
- output 2: float32 [16, 64], P('dp')
- output 3: bfloat16 [512, 16, 40, 128], P('dp', None, 'tp')
- output 4: bfloat16 [512, 16, 40, 128], P('dp', None, 'tp')
All inputs are finite; a program needn't handle non-finite values.
Results may differ from the reference program's by a relative error of at most 0.00355428.
Values are sent between devices in bfloat16 or wider.
A program may use at most 1 GiB of HBM per device.

```python
import math
import jax
import jax.numpy as jnp
from jax import lax

REQUESTS = 16
NODES = 64
PAGES = 32
PAGE_SIZE = 16
MODEL_DIM = 5120
HEADS = 40
KV_HEADS = 40
HEAD_DIM = 128
FFN_DIM = 13824
VOCAB_SIZE = 32000
ROPE_THETA = 500000
RMS_EPS = 1e-5
BLOCKS = REQUESTS * PAGES
SPAN = PAGES * PAGE_SIZE
MAX_CTX = SPAN - NODES
GROUP = HEADS // KV_HEADS


def draw_routing(key):
    k_spread, k_step, k_ctx, k_table, k_score = jax.random.split(key, 5)
    spread = jax.random.randint(k_spread, (REQUESTS, 1), 1, 4)
    step = jnp.minimum(jax.random.randint(k_step, (REQUESTS, NODES), 0, 4), spread)
    node_ids = jnp.arange(NODES)
    parent = jnp.maximum(node_ids[None, :] - 1 - step, 0)
    linked = (parent[:, :, None] == node_ids[None, None, :]) & (node_ids[None, :, None] > 0)
    reach = linked | (node_ids[:, None] == node_ids[None, :])[None]
    for _ in range(int(math.log2(NODES)) + 1):
        reach = jnp.any(reach[:, :, :, None] & reach[:, None, :, :], axis=2)
    tree_mask = reach.astype(jnp.int32)
    depth = jnp.sum(tree_mask, axis=-1).astype(jnp.int32) - 1
    ctx_len = jax.random.randint(k_ctx, (REQUESTS,), 1, MAX_CTX + 1).astype(jnp.int32)
    ctx_len = ctx_len.at[0].set(MAX_CTX)
    block_table = jax.random.permutation(k_table, BLOCKS).astype(jnp.int32).reshape(REQUESTS, PAGES)
    score_id = jax.random.randint(k_score, (REQUESTS, NODES), 0, VOCAB_SIZE).astype(jnp.int32)
    score_id = score_id.at[0, 0].set(VOCAB_SIZE - 1)
    return tree_mask, depth, ctx_len, block_table, score_id


def normal_weight(key, shape, scale):
    return (scale * jax.random.normal(key, shape, jnp.float32)).astype(jnp.bfloat16)


def gain_vector(key):
    return (1.0 + 0.3 * jax.random.normal(key, (MODEL_DIM,), jnp.float32)).astype(jnp.bfloat16)


def setup_inputs(seed: int = 0, part: int = 0) -> dict:
    part_key = jax.random.fold_in(jax.random.key(seed), part)
    keys = jax.random.split(part_key, 4)
    tree_mask, depth, ctx_len, block_table, score_id = draw_routing(keys[0])
    shared = jax.random.split(jax.random.key(seed + 1), 11)
    cache_shape = (BLOCKS, PAGE_SIZE, KV_HEADS, HEAD_DIM)
    return {
        "hidden": normal_weight(keys[1], (REQUESTS, NODES, MODEL_DIM), 1.0),
        "tree_mask": tree_mask,
        "depth": depth,
        "ctx_len": ctx_len,
        "block_table": block_table,
        "score_id": score_id,
        "k_cache": normal_weight(keys[2], cache_shape, 1.0),
        "v_cache": normal_weight(keys[3], cache_shape, 1.0),
        "attn_norm": gain_vector(shared[0]),
        "w_q": normal_weight(shared[1], (MODEL_DIM, HEADS * HEAD_DIM), 2.5 * MODEL_DIM ** -0.5),
        "w_k": normal_weight(shared[2], (MODEL_DIM, KV_HEADS * HEAD_DIM), 1.5 * MODEL_DIM ** -0.5),
        "w_v": normal_weight(shared[3], (MODEL_DIM, KV_HEADS * HEAD_DIM), MODEL_DIM ** -0.5),
        "w_o": normal_weight(shared[4], (HEADS * HEAD_DIM, MODEL_DIM), 1.5 * (HEADS * HEAD_DIM) ** -0.5),
        "mlp_norm": gain_vector(shared[5]),
        "w_gate": normal_weight(shared[6], (MODEL_DIM, FFN_DIM), MODEL_DIM ** -0.5),
        "w_up": normal_weight(shared[7], (MODEL_DIM, FFN_DIM), MODEL_DIM ** -0.5),
        "w_down": normal_weight(shared[8], (FFN_DIM, MODEL_DIM), 1.5 * FFN_DIM ** -0.5),
        "final_norm": gain_vector(shared[9]),
        "w_lm": normal_weight(shared[10], (MODEL_DIM, VOCAB_SIZE), 3.0 * MODEL_DIM ** -0.5),
    }


def rms_norm(values, gain):
    widened = values.astype(jnp.float32)
    scale = lax.rsqrt(jnp.mean(widened * widened, axis=-1, keepdims=True) + RMS_EPS)
    return (widened * scale * gain.astype(jnp.float32)).astype(jnp.bfloat16)


def rotate(values, positions):
    head_dim = values.shape[-1]
    half = head_dim // 2
    inv_freq = 1.0 / (ROPE_THETA ** (jnp.arange(half, dtype=jnp.float32) * (2.0 / head_dim)))
    angles = positions.astype(jnp.float32)[..., None] * inv_freq
    cosine = jnp.cos(angles)[..., None, :]
    sine = jnp.sin(angles)[..., None, :]
    first = values[..., :half]
    second = values[..., half:]
    return jnp.concatenate([first * cosine - second * sine, second * cosine + first * sine], axis=-1)


def reference(hidden, tree_mask, depth, ctx_len, block_table, score_id, k_cache, v_cache, attn_norm, w_q, w_k, w_v, w_o, mlp_norm, w_gate, w_up, w_down, final_norm, w_lm):
    scale = HEAD_DIM ** -0.5
    slot_ids = jnp.arange(SPAN)

    def one_request(item):
        rows, mask_row, depth_row, context, table_row, targets = item
        normed = rms_norm(rows, attn_norm)
        positions = context + depth_row
        query = jnp.dot(normed, w_q, preferred_element_type=jnp.float32).reshape(NODES, HEADS, HEAD_DIM)
        query = rotate(query, positions).astype(jnp.bfloat16).reshape(NODES, KV_HEADS, GROUP, HEAD_DIM)
        key_new = jnp.dot(normed, w_k, preferred_element_type=jnp.float32).reshape(NODES, KV_HEADS, HEAD_DIM)
        key_new = rotate(key_new, positions).astype(jnp.bfloat16)
        val_new = jnp.dot(normed, w_v, preferred_element_type=jnp.float32).astype(jnp.bfloat16).reshape(NODES, KV_HEADS, HEAD_DIM)
        key_old = k_cache[table_row].reshape(SPAN, KV_HEADS, HEAD_DIM)
        val_old = v_cache[table_row].reshape(SPAN, KV_HEADS, HEAD_DIM)
        query_wide = query.astype(jnp.float32)
        score_old = jnp.einsum("tkgh,skh->tkgs", query_wide, key_old.astype(jnp.float32)) * scale
        score_old = jnp.where((slot_ids < context)[None, None, None, :], score_old, -jnp.inf)
        score_new = jnp.einsum("tkgh,jkh->tkgj", query_wide, key_new.astype(jnp.float32)) * scale
        score_new = jnp.where((mask_row > 0)[:, None, None, :], score_new, -jnp.inf)
        top = jnp.maximum(jnp.max(score_old, axis=-1), jnp.max(score_new, axis=-1))[..., None]
        prob_old = jnp.exp(score_old - top)
        prob_new = jnp.exp(score_new - top)
        total = jnp.sum(prob_old, axis=-1) + jnp.sum(prob_new, axis=-1)
        mixed = jnp.einsum("tkgs,skh->tkgh", prob_old.astype(jnp.bfloat16).astype(jnp.float32), val_old.astype(jnp.float32))
        mixed = mixed + jnp.einsum("tkgj,jkh->tkgh", prob_new.astype(jnp.bfloat16).astype(jnp.float32), val_new.astype(jnp.float32))
        attended = (mixed / total[..., None]).astype(jnp.bfloat16).reshape(NODES, HEADS * HEAD_DIM)
        attn_out = jnp.dot(attended, w_o, preferred_element_type=jnp.float32).astype(jnp.bfloat16)
        residual = (rows.astype(jnp.float32) + attn_out.astype(jnp.float32)).astype(jnp.bfloat16)
        normed_mlp = rms_norm(residual, mlp_norm)
        gate = jnp.dot(normed_mlp, w_gate, preferred_element_type=jnp.float32)
        upper = jnp.dot(normed_mlp, w_up, preferred_element_type=jnp.float32)
        product = (jax.nn.silu(gate) * upper).astype(jnp.bfloat16)
        mlp_out = jnp.dot(product, w_down, preferred_element_type=jnp.float32).astype(jnp.bfloat16)
        layer_out = (residual.astype(jnp.float32) + mlp_out.astype(jnp.float32)).astype(jnp.bfloat16)
        logits = jnp.dot(rms_norm(layer_out, final_norm), w_lm, preferred_element_type=jnp.float32)
        log_norm = jax.nn.logsumexp(logits, axis=-1)
        picked = jnp.take_along_axis(logits, targets[:, None], axis=-1)[:, 0]
        return log_norm, picked - log_norm, key_new, val_new

    log_norm, log_prob, key_new, val_new = lax.map(one_request, (hidden, tree_mask, depth, ctx_len, block_table, score_id))
    slots = ctx_len[:, None] + jnp.arange(NODES)[None, :]
    slot_blocks = jnp.take_along_axis(block_table, slots // PAGE_SIZE, axis=1)
    k_out = k_cache.at[slot_blocks, slots % PAGE_SIZE].set(key_new)
    v_out = v_cache.at[slot_blocks, slots % PAGE_SIZE].set(val_new)
    return (log_norm, log_prob, k_out, v_out)
```

```python
import functools

import jax
import jax.numpy as jnp
from jax import lax
from jax.experimental import pallas as pl
from jax.experimental.pallas import tpu as pltpu
from jax.sharding import PartitionSpec as P

RMS_EPS = 1e-5
ROPE_THETA = 500000
MESH = pl.DeviceIdType.MESH
NT_DIMS = (((1,), (1,)), ((), ()))
VMEM_MAX = 67043328


def dot_nt(left, right):
    return lax.dot_general(left, right, NT_DIMS, preferred_element_type=jnp.float32)


def qkv_kernel(hid_ref, gain_ref, cos_ref, sin_ref, wq_ref, wk_ref, wv_ref, q_ref, k_ref, v_ref):
    requests, heads, nodes, head_dim = q_ref.shape
    widened = hid_ref[...].astype(jnp.float32)
    scale = lax.rsqrt(jnp.mean(widened * widened, axis=-1, keepdims=True) + RMS_EPS)
    normed = (widened * scale * gain_ref[...].astype(jnp.float32)).astype(jnp.bfloat16)
    cosine = cos_ref[...]
    sine = sin_ref[...]

    def put(out_ref, weight_ref, turned):
        product = jnp.dot(normed, weight_ref[...], preferred_element_type=jnp.float32)
        for h in range(heads):
            part = product[:, h * head_dim : (h + 1) * head_dim]
            if turned:
                part = part * cosine + pltpu.roll(part, head_dim // 2, 1) * sine
            out_ref[:, h] = part.astype(jnp.bfloat16).reshape(requests, nodes, head_dim)

    put(q_ref, wq_ref, True)
    put(k_ref, wk_ref, True)
    put(v_ref, wv_ref, False)


def project(hidden, gain, cosine, sine, w_q, w_k, w_v, requests, nodes, head_dim, group):
    rows, dim = hidden.shape
    cols = w_q.shape[1]
    heads = cols // head_dim
    block = group * nodes
    full = pl.BlockSpec((dim, cols), lambda i: (0, 0), pipeline_mode=pl.Buffered(1))
    out = pl.BlockSpec((group, heads, nodes, head_dim), lambda i: (i, 0, 0, 0))
    shape = jax.ShapeDtypeStruct((requests, heads, nodes, head_dim), jnp.bfloat16)
    return pl.pallas_call(
        qkv_kernel,
        grid=(rows // block,),
        in_specs=[
            pl.BlockSpec((block, dim), lambda i: (i, 0)),
            pl.BlockSpec((1, dim), lambda i: (0, 0)),
            pl.BlockSpec((block, head_dim), lambda i: (i, 0)),
            pl.BlockSpec((block, head_dim), lambda i: (i, 0)),
            full,
            full,
            full,
        ],
        out_specs=[out, out, out],
        out_shape=[shape, shape, shape],
        compiler_params=pltpu.CompilerParams(vmem_limit_bytes=VMEM_MAX),
        name="project",
    )(hidden, gain, cosine, sine, w_q, w_k, w_v)


def attend_kernel(table_ref, ctx_ref, q_ref, kn_ref, vn_ref, mask_ref, kc_ref, vc_ref, out_ref, ko_ref, vo_ref, kbuf, vbuf, rsem, wsem):
    b = pl.program_id(0)
    count = pl.num_programs(0)
    heads, span, head_dim = kbuf.shape[1:]
    nodes = q_ref.shape[2]
    page = kc_ref.shape[2]
    pages = span // page
    window = nodes + page

    def load(i, slot):
        def one(s, _):
            block = table_ref[i, s]
            rows = pl.ds(pl.multiple_of(s * page, page), page)
            pltpu.make_async_copy(kc_ref.at[block], kbuf.at[slot, :, rows], rsem.at[0, slot]).start()
            pltpu.make_async_copy(vc_ref.at[block], vbuf.at[slot, :, rows], rsem.at[1, slot]).start()
            return 0

        lax.fori_loop(0, pages, one, 0)

    def save(i, slot):
        def one(s, _):
            block = table_ref[i, s]
            rows = pl.ds(pl.multiple_of(s * page, page), page)
            pltpu.make_async_copy(kbuf.at[slot, :, rows], ko_ref.at[block], wsem.at[0, slot]).start()
            pltpu.make_async_copy(vbuf.at[slot, :, rows], vo_ref.at[block], wsem.at[1, slot]).start()
            return 0

        lax.fori_loop(0, pages, one, 0)

    def whole(slot, sem):
        pltpu.make_async_copy(kbuf.at[slot], kbuf.at[slot], sem.at[0, slot]).wait()
        pltpu.make_async_copy(vbuf.at[slot], vbuf.at[slot], sem.at[1, slot]).wait()

    slot = lax.rem(b, 3)
    after = lax.rem(b + 1, 3)

    @pl.when(b == 0)
    def _():
        load(0, 0)

    @pl.when(b >= 2)
    def _():
        whole(after, wsem)

    @pl.when(b + 1 < count)
    def _():
        load(b + 1, after)

    whole(slot, rsem)
    ctx = ctx_ref[b]
    base = pl.multiple_of(jnp.minimum((ctx // page) * page, span - window), page)
    row = base + lax.broadcasted_iota(jnp.int32, (window, nodes), 0)
    node = ctx + lax.broadcasted_iota(jnp.int32, (window, nodes), 1)
    place = jnp.where(row == node, 1.0, 0.0).astype(jnp.bfloat16)
    slot_id = base + lax.broadcasted_iota(jnp.int32, (window, head_dim), 0)
    fresh = (slot_id >= ctx) & (slot_id < ctx + nodes)
    for h in range(heads):
        for buf, new_ref in ((kbuf, kn_ref), (vbuf, vn_ref)):
            moved = jnp.dot(place, new_ref[0, h], preferred_element_type=jnp.float32)
            old = buf[slot, h, pl.ds(base, window), :]
            buf[slot, h, pl.ds(base, window), :] = jnp.where(fresh, moved, old.astype(jnp.float32)).astype(jnp.bfloat16)
    save(b, slot)
    spread = jnp.where(
        ctx + lax.broadcasted_iota(jnp.int32, (nodes, span), 0) == lax.broadcasted_iota(jnp.int32, (nodes, span), 1), 1.0, 0.0
    ).astype(jnp.bfloat16)
    linked = jnp.where(mask_ref[0] > 0, 1.0, 0.0).astype(jnp.bfloat16)
    seen_new = jnp.dot(linked, spread, preferred_element_type=jnp.float32) > 0.5
    seen = seen_new | (lax.broadcasted_iota(jnp.int32, (nodes, span), 1) < ctx)
    scale = head_dim**-0.5
    for h in range(heads):
        score = dot_nt(q_ref[0, h], kbuf[slot, h]) * scale
        score = jnp.where(seen, score, -jnp.inf)
        top = jnp.max(score, axis=-1, keepdims=True)
        prob = jnp.exp(score - top)
        total = jnp.sum(prob, axis=-1, keepdims=True)
        mixed = jnp.dot(prob.astype(jnp.bfloat16), vbuf[slot, h], preferred_element_type=jnp.float32)
        out_ref[:, h * head_dim : (h + 1) * head_dim] = (mixed / total).astype(jnp.bfloat16)

    @pl.when(b == count - 1)
    def _():
        whole(lax.rem(b + 2, 3), wsem)
        whole(slot, wsem)


def attend(table, ctx_len, query, key_new, val_new, tree_mask, k_cache, v_cache):
    requests, heads, nodes, head_dim = query.shape
    page = k_cache.shape[2]
    span = table.shape[1] * page
    node_spec = pl.BlockSpec((1, heads, nodes, head_dim), lambda b, *_: (b, 0, 0, 0))
    anywhere = pl.BlockSpec(memory_space=pl.ANY)
    return pl.pallas_call(
        attend_kernel,
        grid_spec=pltpu.PrefetchScalarGridSpec(
            num_scalar_prefetch=2,
            grid=(requests,),
            in_specs=[
                node_spec,
                node_spec,
                node_spec,
                pl.BlockSpec((1, nodes, nodes), lambda b, *_: (b, 0, 0)),
                anywhere,
                anywhere,
            ],
            out_specs=[pl.BlockSpec((nodes, heads * head_dim), lambda b, *_: (b, 0)), anywhere, anywhere],
            scratch_shapes=[
                pltpu.VMEM((3, heads, span, head_dim), jnp.bfloat16),
                pltpu.VMEM((3, heads, span, head_dim), jnp.bfloat16),
                pltpu.SemaphoreType.DMA((2, 3)),
                pltpu.SemaphoreType.DMA((2, 3)),
            ],
        ),
        out_shape=[
            jax.ShapeDtypeStruct((requests * nodes, heads * head_dim), jnp.bfloat16),
            jax.ShapeDtypeStruct(k_cache.shape, k_cache.dtype),
            jax.ShapeDtypeStruct(v_cache.shape, v_cache.dtype),
        ],
        name="attend",
    )(table, ctx_len, query, key_new, val_new, tree_mask, k_cache, v_cache)


def rms_norm(values, gain):
    widened = values.astype(jnp.float32)
    scale = lax.rsqrt(jnp.mean(widened * widened, axis=-1, keepdims=True) + RMS_EPS)
    return (widened * scale * gain.astype(jnp.float32)).astype(jnp.bfloat16)


def rope_tables(positions, head_dim):
    half = head_dim // 2
    inv_freq = 1.0 / (ROPE_THETA ** (jnp.arange(half, dtype=jnp.float32) * (2.0 / head_dim)))
    angles = positions.astype(jnp.float32)[:, None] * inv_freq
    cosine = jnp.cos(angles)
    sine = jnp.sin(angles)
    return jnp.concatenate([cosine, cosine], axis=-1), jnp.concatenate([-sine, sine], axis=-1)


def solution(mesh):
    def group_step(hidden, tree_mask, depth, ctx_len, block_table, score_id, k_cache, v_cache, attn_norm, w_q, w_k, w_v, w_o, mlp_norm, w_gate, w_up, w_down, final_norm, w_lm):
        requests, nodes, dim = hidden.shape
        head_dim = k_cache.shape[3]
        rows = requests * nodes
        flat = hidden.reshape(rows, dim)
        cosine, sine = rope_tables((ctx_len[:, None] + depth).reshape(rows), head_dim)
        query, key_new, val_new = project(flat, attn_norm.reshape(1, dim), cosine, sine, w_q, w_k, w_v, requests, nodes, head_dim, 4)
        attended, k_out, v_out = attend(
            block_table, ctx_len, query, key_new, val_new, tree_mask, jnp.transpose(k_cache, (0, 2, 1, 3)), jnp.transpose(v_cache, (0, 2, 1, 3))
        )
        k_out = jnp.transpose(k_out, (0, 2, 1, 3))
        v_out = jnp.transpose(v_out, (0, 2, 1, 3))

        attn_sum = lax.psum(jnp.dot(attended, w_o, preferred_element_type=jnp.float32).astype(jnp.bfloat16), "tp")
        residual = (flat.astype(jnp.float32) + attn_sum.astype(jnp.float32)).astype(jnp.bfloat16)
        normed_mlp = rms_norm(residual, mlp_norm)
        gate = jnp.dot(normed_mlp, w_gate, preferred_element_type=jnp.float32)
        upper = jnp.dot(normed_mlp, w_up, preferred_element_type=jnp.float32)
        product = (jax.nn.silu(gate) * upper).astype(jnp.bfloat16)
        mlp_sum = lax.psum(jnp.dot(product, w_down, preferred_element_type=jnp.float32).astype(jnp.bfloat16), "tp")
        layer_out = (residual.astype(jnp.float32) + mlp_sum.astype(jnp.float32)).astype(jnp.bfloat16)
        logits = jnp.dot(rms_norm(layer_out, final_norm), w_lm, preferred_element_type=jnp.float32)
        vocab_local = logits.shape[-1]
        local_id = score_id.reshape(rows, 1) - lax.axis_index("tp") * vocab_local
        top = jnp.max(logits, axis=-1)
        part = jnp.sum(jnp.exp(logits - top[:, None]), axis=-1)
        hit = lax.broadcasted_iota(jnp.int32, logits.shape, 1) == local_id
        picked = jnp.sum(jnp.where(hit, logits, 0.0), axis=-1)
        stats = lax.all_gather(jnp.stack([top, part, picked]), "tp")
        global_top = jnp.max(stats[:, 0], axis=0)
        total = jnp.sum(stats[:, 1] * jnp.exp(stats[:, 0] - global_top), axis=0)
        log_norm = global_top + jnp.log(total)
        log_prob = jnp.sum(stats[:, 2], axis=0) - log_norm
        return log_norm.reshape(requests, nodes), log_prob.reshape(requests, nodes), k_out, v_out

    request_spec = P("dp", None, None)
    node_spec = P("dp", None)
    cache_spec = P("dp", None, "tp", None)
    shared_spec = P(None)
    column_spec = P(None, "tp")
    row_spec = P("tp", None)
    in_specs = (request_spec, request_spec, node_spec, P("dp"), node_spec, node_spec, cache_spec, cache_spec, shared_spec, column_spec, column_spec, column_spec, row_spec, shared_spec, column_spec, column_spec, row_spec, shared_spec, column_spec)
    out_specs = (node_spec, node_spec, cache_spec, cache_spec)
    return jax.shard_map(group_step, mesh=mesh, in_specs=in_specs, out_specs=out_specs, check_vma=False)
```

```python
import functools

import jax
import jax.numpy as jnp
from jax import lax
from jax.experimental import pallas as pl
from jax.experimental.pallas import tpu as pltpu
from jax.sharding import PartitionSpec as P

RMS_EPS = 1e-5
ROPE_THETA = 500000
MESH = pl.DeviceIdType.MESH
NT_DIMS = (((1,), (1,)), ((), ()))
VMEM_MAX = 67043328


def dot_nt(left, right):
    return lax.dot_general(left, right, NT_DIMS, preferred_element_type=jnp.float32)


def qkv_kernel(hid_ref, gain_ref, cos_ref, sin_ref, wq_ref, wk_ref, wv_ref, q_ref, k_ref, v_ref):
    requests, heads, nodes, head_dim = q_ref.shape
    widened = hid_ref[...].astype(jnp.float32)
    scale = lax.rsqrt(jnp.mean(widened * widened, axis=-1, keepdims=True) + RMS_EPS)
    normed = (widened * scale * gain_ref[...].astype(jnp.float32)).astype(jnp.bfloat16)
    cosine = cos_ref[...]
    sine = sin_ref[...]

    def put(out_ref, weight_ref, turned):
        product = jnp.dot(normed, weight_ref[...], preferred_element_type=jnp.float32)
        for h in range(heads):
            part = product[:, h * head_dim : (h + 1) * head_dim]
            if turned:
                part = part * cosine + pltpu.roll(part, head_dim // 2, 1) * sine
            out_ref[:, h] = part.astype(jnp.bfloat16).reshape(requests, nodes, head_dim)

    put(q_ref, wq_ref, True)
    put(k_ref, wk_ref, True)
    put(v_ref, wv_ref, False)


def project(hidden, gain, cosine, sine, w_q, w_k, w_v, requests, nodes, head_dim, group):
    rows, dim = hidden.shape
    cols = w_q.shape[1]
    heads = cols // head_dim
    block = group * nodes
    full = pl.BlockSpec((dim, cols), lambda i: (0, 0), pipeline_mode=pl.Buffered(1))
    out = pl.BlockSpec((group, heads, nodes, head_dim), lambda i: (i, 0, 0, 0))
    shape = jax.ShapeDtypeStruct((requests, heads, nodes, head_dim), jnp.bfloat16)
    return pl.pallas_call(
        qkv_kernel,
        grid=(rows // block,),
        in_specs=[
            pl.BlockSpec((block, dim), lambda i: (i, 0)),
            pl.BlockSpec((1, dim), lambda i: (0, 0)),
            pl.BlockSpec((block, head_dim), lambda i: (i, 0)),
            pl.BlockSpec((block, head_dim), lambda i: (i, 0)),
            full,
            full,
            full,
        ],
        out_specs=[out, out, out],
        out_shape=[shape, shape, shape],
        compiler_params=pltpu.CompilerParams(vmem_limit_bytes=VMEM_MAX),
        name="project",
    )(hidden, gain, cosine, sine, w_q, w_k, w_v)


def attend_kernel(table_ref, ctx_ref, q_ref, kn_ref, vn_ref, mask_ref, kc_ref, vc_ref, out_ref, ko_ref, vo_ref, kbuf, vbuf, rsem, wsem):
    b = pl.program_id(0)
    count = pl.num_programs(0)
    heads, span, head_dim = kbuf.shape[1:]
    nodes = q_ref.shape[2]
    page = kc_ref.shape[2]
    pages = span // page
    window = nodes + page

    def load(i, slot):
        def one(s, _):
            block = table_ref[i, s]
            rows = pl.ds(pl.multiple_of(s * page, page), page)
            pltpu.make_async_copy(kc_ref.at[block], kbuf.at[slot, :, rows], rsem.at[0, slot]).start()
            pltpu.make_async_copy(vc_ref.at[block], vbuf.at[slot, :, rows], rsem.at[1, slot]).start()
            return 0

        lax.fori_loop(0, pages, one, 0)

    def save(i, slot):
        def one(s, _):
            block = table_ref[i, s]
            rows = pl.ds(pl.multiple_of(s * page, page), page)
            pltpu.make_async_copy(kbuf.at[slot, :, rows], ko_ref.at[block], wsem.at[0, slot]).start()
            pltpu.make_async_copy(vbuf.at[slot, :, rows], vo_ref.at[block], wsem.at[1, slot]).start()
            return 0

        lax.fori_loop(0, pages, one, 0)

    def whole(slot, sem):
        pltpu.make_async_copy(kbuf.at[slot], kbuf.at[slot], sem.at[0, slot]).wait()
        pltpu.make_async_copy(vbuf.at[slot], vbuf.at[slot], sem.at[1, slot]).wait()

    slot = lax.rem(b, 3)
    after = lax.rem(b + 1, 3)

    @pl.when(b == 0)
    def _():
        load(0, 0)

    @pl.when(b >= 2)
    def _():
        whole(after, wsem)

    @pl.when(b + 1 < count)
    def _():
        load(b + 1, after)

    whole(slot, rsem)
    ctx = ctx_ref[b]
    base = pl.multiple_of(jnp.minimum((ctx // page) * page, span - window), page)
    row = base + lax.broadcasted_iota(jnp.int32, (window, nodes), 0)
    node = ctx + lax.broadcasted_iota(jnp.int32, (window, nodes), 1)
    place = jnp.where(row == node, 1.0, 0.0).astype(jnp.bfloat16)
    slot_id = base + lax.broadcasted_iota(jnp.int32, (window, head_dim), 0)
    fresh = (slot_id >= ctx) & (slot_id < ctx + nodes)
    for h in range(heads):
        for buf, new_ref in ((kbuf, kn_ref), (vbuf, vn_ref)):
            moved = jnp.dot(place, new_ref[0, h], preferred_element_type=jnp.float32)
            old = buf[slot, h, pl.ds(base, window), :]
            buf[slot, h, pl.ds(base, window), :] = jnp.where(fresh, moved, old.astype(jnp.float32)).astype(jnp.bfloat16)
    save(b, slot)
    spread = jnp.where(
        ctx + lax.broadcasted_iota(jnp.int32, (nodes, span), 0) == lax.broadcasted_iota(jnp.int32, (nodes, span), 1), 1.0, 0.0
    ).astype(jnp.bfloat16)
    linked = jnp.where(mask_ref[0] > 0, 1.0, 0.0).astype(jnp.bfloat16)
    seen_new = jnp.dot(linked, spread, preferred_element_type=jnp.float32) > 0.5
    seen = seen_new | (lax.broadcasted_iota(jnp.int32, (nodes, span), 1) < ctx)
    scale = head_dim**-0.5
    for h in range(heads):
        score = dot_nt(q_ref[0, h], kbuf[slot, h]) * scale
        score = jnp.where(seen, score, -jnp.inf)
        top = jnp.max(score, axis=-1, keepdims=True)
        prob = jnp.exp(score - top)
        total = jnp.sum(prob, axis=-1, keepdims=True)
        mixed = jnp.dot(prob.astype(jnp.bfloat16), vbuf[slot, h], preferred_element_type=jnp.float32)
        out_ref[:, h * head_dim : (h + 1) * head_dim] = (mixed / total).astype(jnp.bfloat16)

    @pl.when(b == count - 1)
    def _():
        whole(lax.rem(b + 2, 3), wsem)
        whole(slot, wsem)


def attend(table, ctx_len, query, key_new, val_new, tree_mask, k_cache, v_cache):
    requests, heads, nodes, head_dim = query.shape
    page = k_cache.shape[2]
    span = table.shape[1] * page
    node_spec = pl.BlockSpec((1, heads, nodes, head_dim), lambda b, *_: (b, 0, 0, 0))
    anywhere = pl.BlockSpec(memory_space=pl.ANY)
    return pl.pallas_call(
        attend_kernel,
        grid_spec=pltpu.PrefetchScalarGridSpec(
            num_scalar_prefetch=2,
            grid=(requests,),
            in_specs=[
                node_spec,
                node_spec,
                node_spec,
                pl.BlockSpec((1, nodes, nodes), lambda b, *_: (b, 0, 0)),
                anywhere,
                anywhere,
            ],
            out_specs=[pl.BlockSpec((nodes, heads * head_dim), lambda b, *_: (b, 0)), anywhere, anywhere],
            scratch_shapes=[
                pltpu.VMEM((3, heads, span, head_dim), jnp.bfloat16),
                pltpu.VMEM((3, heads, span, head_dim), jnp.bfloat16),
                pltpu.SemaphoreType.DMA((2, 3)),
                pltpu.SemaphoreType.DMA((2, 3)),
            ],
        ),
        out_shape=[
            jax.ShapeDtypeStruct((requests * nodes, heads * head_dim), jnp.bfloat16),
            jax.ShapeDtypeStruct(k_cache.shape, k_cache.dtype),
            jax.ShapeDtypeStruct(v_cache.shape, v_cache.dtype),
        ],
        name="attend",
    )(table, ctx_len, query, key_new, val_new, tree_mask, k_cache, v_cache)


TILE = 512
HALF = TILE // 2
PAIR, X1, Y1, X2, Y2, GX, GY, GP, FX, FY, PX, PY, PD = range(13)


def seat():
    me = lax.axis_index("tp")
    core = me % 2
    x = (me // 2) % 2
    y = me // 4
    to_x = y * 4 + (1 - x) * 2 + core
    to_y = (1 - y) * 4 + x * 2 + core
    to_pair = y * 4 + x * 2 + (1 - core)
    return me, core, x, y, to_x, to_y, to_pair


def send(src, dst, ssem, rsem, kind, t, target):
    pltpu.make_async_remote_copy(
        src_ref=src, dst_ref=dst, send_sem=ssem.at[kind], recv_sem=rsem.at[kind, t], device_id={"tp": target}, device_id_type=MESH
    ).start()


def landed(ref, rsem, kind, t):
    pltpu.make_async_copy(ref, ref, rsem.at[kind, t]).wait()


def sent(ref, ssem, kind):
    pltpu.make_async_copy(ref, ref, ssem.at[kind]).wait()


def reduce_norm_gather(left_ref, w_hbm, wbuf, wsem, resid, resid_ready, gain_ref, h_ref, mbuf, r1, rx, ry, r2x, r2y, ssq, ssem, rsem, free, idle_work, compute):
    me, core, x, y, to_x, to_y, to_pair = seat()
    tiles = mbuf.shape[0]
    rows = mbuf.shape[4]
    depth = w_hbm.shape[0]

    def fetch(t):
        cols = pl.ds(pl.multiple_of(t * TILE, TILE), TILE)
        return pltpu.make_async_copy(w_hbm.at[:, cols], wbuf.at[t % 2, pl.ds(0, depth)], wsem.at[t % 2])

    fetch(0).start()
    fetch(1).start()

    def scatter_step(j, _):
        @pl.when(j < tiles)
        def _():
            fetch(j).wait()
            for half in range(2):
                cols = pl.ds(half * HALF, HALF)
                part = jnp.dot(left_ref[...], wbuf[j % 2, :, cols], preferred_element_type=jnp.float32)
                mbuf[j, :, :, :, :, cols] = part.astype(jnp.bfloat16).reshape(2, 2, 2, rows, HALF)

            @pl.when(j + 2 < tiles)
            def _():
                fetch(j + 2).start()

            send(mbuf.at[j, :, :, 1 - core], r1.at[j], ssem, rsem, PAIR, j, to_pair)
            idle_work(j)

        @pl.when((j >= 1) & (j < tiles + 1))
        def _():
            t = j - 1
            landed(r1.at[t], rsem, PAIR, t)
            for yy in range(2):
                for xx in range(2):
                    mbuf[t, yy, xx, core] = mbuf[t, yy, xx, core] + r1[t, yy, xx]
            send(mbuf.at[t, :, 1 - x, core, :, pl.ds(0, HALF)], rx.at[t], ssem, rsem, X1, t, to_x)
            send(mbuf.at[t, 1 - y, :, core, :, pl.ds(HALF, HALF)], ry.at[t], ssem, rsem, Y1, t, to_y)

        @pl.when((j >= 2) & (j < tiles + 2))
        def _():
            t = j - 2
            landed(rx.at[t], rsem, X1, t)
            for yy in range(2):
                mbuf[t, yy, x, core, :, pl.ds(0, HALF)] = mbuf[t, yy, x, core, :, pl.ds(0, HALF)] + rx[t, yy]
            send(mbuf.at[t, 1 - y, x, core, :, pl.ds(0, HALF)], r2y.at[t], ssem, rsem, Y2, t, to_y)
            landed(ry.at[t], rsem, Y1, t)
            for xx in range(2):
                mbuf[t, y, xx, core, :, pl.ds(HALF, HALF)] = mbuf[t, y, xx, core, :, pl.ds(HALF, HALF)] + ry[t, xx]
            send(mbuf.at[t, y, 1 - x, core, :, pl.ds(HALF, HALF)], r2x.at[t], ssem, rsem, X2, t, to_x)

        @pl.when(j == 3)
        def _():
            resid_ready()
            ssq[...] = jnp.zeros_like(ssq)

        @pl.when(j >= 3)
        def _():
            t = j - 3
            landed(r2y.at[t], rsem, Y2, t)
            landed(r2x.at[t], rsem, X2, t)
            for half, other in ((0, r2y), (1, r2x)):
                cols = pl.ds(half * HALF, HALF)
                total = (mbuf[t, y, x, core, :, cols] + other[t]).astype(jnp.float32)
                new = (resid[t, :, cols].astype(jnp.float32) + total).astype(jnp.bfloat16)
                h_ref[t, :, cols] = new
                wide = new.astype(jnp.float32)
                wide = wide * wide
                for lane in range(0, HALF, 128):
                    ssq[...] += wide[:, lane : lane + 128]

        return 0

    lax.fori_loop(0, tiles + 3, scatter_step, 0)
    sent(r1, ssem, PAIR)
    sent(rx, ssem, X1)
    sent(ry, ssem, Y1)
    sent(r2x, ssem, X2)
    sent(r2y, ssem, Y2)
    for target in (to_x, to_y, to_pair):
        pl.semaphore_signal(free, inc=1, device_id={"tp": target}, device_id_type=MESH)
    scale = lax.rsqrt(jnp.sum(ssq[...], axis=-1, keepdims=True) * (1.0 / (tiles * TILE)) + RMS_EPS)

    def norm_step(t, _):
        mbuf[t, y, x, core] = (h_ref[t].astype(jnp.float32) * scale * gain_ref[t].astype(jnp.float32)).astype(jnp.bfloat16)
        return 0

    lax.fori_loop(0, tiles, norm_step, 0)
    pl.semaphore_wait(free, 3)

    def own(t):
        mine = mbuf.at[t, y, x, core]
        send(mine, mine, ssem, rsem, GX, t, to_x)
        send(mine, mine, ssem, rsem, GY, t, to_y)
        send(mine, mine, ssem, rsem, GP, t, to_pair)

    own(0)
    own(1)

    def gather_step(j, _):
        @pl.when(j + 2 < tiles)
        def _():
            own(j + 2)

        @pl.when(j < tiles)
        def _():
            from_x = mbuf.at[j, y, 1 - x, core]
            from_y = mbuf.at[j, 1 - y, x, core]
            landed(from_x, rsem, GX, j)
            upper = from_x.at[pl.ds(0, rows // 2)]
            send(upper, upper, ssem, rsem, FY, j, to_y)
            send(from_x, from_x, ssem, rsem, PX, j, to_pair)
            landed(from_y, rsem, GY, j)
            lower = from_y.at[pl.ds(rows // 2, rows // 2)]
            send(lower, lower, ssem, rsem, FX, j, to_x)
            send(from_y, from_y, ssem, rsem, PY, j, to_pair)

        @pl.when((j >= 1) & (j < tiles + 1))
        def _():
            t = j - 1
            far = mbuf.at[t, 1 - y, 1 - x, core]
            landed(far.at[pl.ds(0, rows // 2)], rsem, FY, t)
            landed(far.at[pl.ds(rows // 2, rows // 2)], rsem, FX, t)
            send(far, far, ssem, rsem, PD, t, to_pair)

        @pl.when(j >= 2)
        def _():
            t = j - 2
            landed(mbuf.at[t, y, x, 1 - core], rsem, GP, t)
            landed(mbuf.at[t, y, 1 - x, 1 - core], rsem, PX, t)
            landed(mbuf.at[t, 1 - y, x, 1 - core], rsem, PY, t)
            landed(mbuf.at[t, 1 - y, 1 - x, 1 - core], rsem, PD, t)
            compute(t)

        return 0

    lax.fori_loop(0, tiles + 2, gather_step, 0)
    for kind in (GX, GY, GP, PX, PY, PD):
        sent(h_ref, ssem, kind)
    for kind in (FX, FY):
        sent(h_ref.at[pl.ds(0, tiles // 2)], ssem, kind)


def greet(targets):
    barrier = pltpu.get_barrier_semaphore()
    for target in targets:
        pl.semaphore_signal(barrier, inc=1, device_id={"tp": target}, device_id_type=MESH)
    pl.semaphore_wait(barrier, len(targets))


def mlp_kernel(att_ref, gain_ref, hid_hbm, wo_hbm, wg_hbm, wu_hbm, prod_ref, h_ref, mbuf, r1, rx, ry, r2x, r2y, ssq, wo_buf, resid, wg_buf, wu_buf, acc_g, acc_u, ssem, rsem, wsem, gsem, hsem, free):
    me, core, x, y, to_x, to_y, to_pair = seat()
    tiles = mbuf.shape[0]
    rows = mbuf.shape[4]
    width = wg_hbm.shape[0]
    blocks = acc_g.shape[0]
    padded = wg_buf.shape[1]

    def fetch(t):
        cols = pl.ds(pl.multiple_of(t * TILE, TILE), TILE)
        slot = t % 2
        return (
            pltpu.make_async_copy(wg_hbm.at[:, cols], wg_buf.at[slot, pl.ds(0, width)], gsem.at[0, slot]),
            pltpu.make_async_copy(wu_hbm.at[:, cols], wu_buf.at[slot, pl.ds(0, width)], gsem.at[1, slot]),
        )

    greet((to_x, to_y, to_pair))
    if padded > width:
        for slot in range(2):
            wg_buf[slot, pl.ds(width, padded - width)] = jnp.zeros((padded - width, TILE), jnp.bfloat16)
            wu_buf[slot, pl.ds(width, padded - width)] = jnp.zeros((padded - width, TILE), jnp.bfloat16)
    for t in range(2):
        for copy in fetch(t):
            copy.start()

    def hidden_copy(t):
        cols = pl.ds(t * TILE, TILE)
        return pltpu.make_async_copy(hid_hbm.at[pl.ds(pl.multiple_of(me * rows, rows), rows), cols], resid.at[t], hsem)

    for t in range(tiles):
        hidden_copy(t).start()

    def resid_ready():
        pltpu.make_async_copy(resid, resid, hsem).wait()

    def idle_work(j):
        @pl.when(j < blocks)
        def _():
            acc_g[j] = jnp.zeros(acc_g.shape[1:], jnp.float32)
            acc_u[j] = jnp.zeros(acc_u.shape[1:], jnp.float32)

    def compute(t):
        slot = t % 2
        for copy in fetch(t):
            copy.wait()

        def one(n, _):
            cols = pl.ds(pl.multiple_of(n * 256, 256), 256)
            left = mbuf[t].reshape(8 * rows, TILE)
            acc_g[n] += dot_nt(left, wg_buf[slot, cols])
            acc_u[n] += dot_nt(left, wu_buf[slot, cols])
            return 0

        lax.fori_loop(0, blocks, one, 0)

        @pl.when(t + 2 < tiles)
        def _():
            for copy in fetch(t + 2):
                copy.start()

    reduce_norm_gather(att_ref, wo_hbm, wo_buf, wsem, resid, resid_ready, gain_ref, h_ref, mbuf, r1, rx, ry, r2x, r2y, ssq, ssem, rsem, free, idle_work, compute)

    def finish(n, _):
        cols = pl.ds(pl.multiple_of(n * 256, 256), 256)
        prod_ref[:, cols] = (jax.nn.silu(acc_g[n]) * acc_u[n]).astype(jnp.bfloat16)
        return 0

    lax.fori_loop(0, blocks, finish, 0)


def head_kernel(prod_ref, gain_ref, res_ref, id_ref, wd_hbm, wl_hbm, out_ref, h_ref, mbuf, r1, rx, ry, r2x, r2y, ssq, wd_buf, wl_buf, acc, stats, ssem, rsem, wsem, lsem, tsem, usem, free):
    me, core, x, y, to_x, to_y, to_pair = seat()
    tiles = mbuf.shape[0]
    rows = mbuf.shape[4]
    depth = wd_hbm.shape[0]
    padded = wd_buf.shape[1]
    blocks, block = acc.shape[0], acc.shape[1]
    vocab = wl_hbm.shape[0]
    others = [(me + i) % 8 for i in range(1, 8)]

    def fetch(t):
        cols = pl.ds(pl.multiple_of(t * TILE, TILE), TILE)
        return pltpu.make_async_copy(wl_hbm.at[:, cols], wl_buf.at[t % 2], lsem.at[t % 2])

    greet(others)
    if padded > depth:
        for slot in range(2):
            wd_buf[slot, pl.ds(depth, padded - depth)] = jnp.zeros((padded - depth, TILE), jnp.bfloat16)
    fetch(0).start()
    fetch(1).start()

    def resid_ready():
        pass

    def idle_work(j):
        @pl.when(j < blocks)
        def _():
            acc[j] = jnp.zeros(acc.shape[1:], jnp.float32)

    def compute(t):
        fetch(t).wait()

        def one(n, _):
            part = pl.ds(pl.multiple_of(n * block, block), block)
            acc[n] += dot_nt(wl_buf[t % 2, part], mbuf[t].reshape(8 * rows, TILE))
            return 0

        lax.fori_loop(0, blocks, one, 0)

        @pl.when(t + 2 < tiles)
        def _():
            fetch(t + 2).start()

    reduce_norm_gather(prod_ref, wd_hbm, wd_buf, wsem, res_ref, resid_ready, gain_ref, h_ref, mbuf, r1, rx, ry, r2x, r2y, ssq, ssem, rsem, free, idle_work, compute)

    count = 8 * rows

    def top_step(n, best):
        return jnp.maximum(best, jnp.max(acc[n].reshape(block // 8, 8, count), axis=0))

    best = lax.fori_loop(0, blocks, top_step, jnp.full((8, count), -jnp.inf, jnp.float32))
    best = jnp.max(best, axis=0, keepdims=True)
    local_id = id_ref[...] - me * vocab

    def sum_step(n, carry):
        total, picked = carry
        value = acc[n]
        hit = lax.broadcasted_iota(jnp.int32, (block, count), 0) + n * block == local_id
        total = total + jnp.sum(jnp.exp(value - best).reshape(block // 8, 8, count), axis=0)
        picked = picked + jnp.sum(jnp.where(hit, value, 0.0).reshape(block // 8, 8, count), axis=0)
        return total, picked

    zero = jnp.zeros((8, count), jnp.float32)
    total, picked = lax.fori_loop(0, blocks, sum_step, (zero, zero))

    def pack(values):
        return jnp.concatenate([values[:, i * 128 : (i + 1) * 128] for i in range(8)], axis=0)

    stats[me, 0] = pack(best)
    stats[me, 1] = pack(jnp.sum(total, axis=0, keepdims=True))
    stats[me, 2] = pack(jnp.sum(picked, axis=0, keepdims=True))
    copies = []
    for i, other in enumerate(others):
        copy = pltpu.make_async_remote_copy(
            src_ref=stats.at[me], dst_ref=stats.at[me], send_sem=tsem.at[i], recv_sem=usem.at[i], device_id={"tp": other}, device_id_type=MESH
        )
        copy.start()
        copies.append(copy)
    for copy in copies:
        copy.wait()
    top = stats[0, 0]
    for d in range(1, 8):
        top = jnp.maximum(top, stats[d, 0])
    whole = jnp.zeros_like(top)
    score = jnp.zeros_like(top)
    for d in range(8):
        whole = whole + stats[d, 1] * jnp.exp(stats[d, 0] - top)
        score = score + stats[d, 2]
    norm = top + jnp.log(whole)
    out_ref[0] = norm
    out_ref[1] = score - norm


def exchange_scratch(tiles, rows):
    bf16 = jnp.bfloat16
    return [
        pltpu.VMEM((tiles, 2, 2, 2, rows, TILE), bf16),
        pltpu.VMEM((tiles, 2, 2, rows, TILE), bf16),
        pltpu.VMEM((tiles, 2, rows, HALF), bf16),
        pltpu.VMEM((tiles, 2, rows, HALF), bf16),
        pltpu.VMEM((tiles, rows, HALF), bf16),
        pltpu.VMEM((tiles, rows, HALF), bf16),
        pltpu.VMEM((rows, 128), jnp.float32),
    ]


def mlp_stage(attended, gain, hidden, w_o, gate_t, up_t):
    count, dim = hidden.shape
    tiles = dim // TILE
    rows = count // 8
    width = gate_t.shape[0]
    blocks = pl.cdiv(width, 256)
    padded = blocks * 256
    vmem = pl.BlockSpec(memory_space=pltpu.VMEM)
    anywhere = pl.BlockSpec(memory_space=pl.ANY)
    bf16 = jnp.bfloat16
    return pl.pallas_call(
        mlp_kernel,
        in_specs=[vmem, vmem, anywhere, anywhere, anywhere, anywhere],
        out_specs=[vmem, vmem],
        out_shape=[jax.ShapeDtypeStruct((count, padded), bf16), jax.ShapeDtypeStruct((tiles, rows, TILE), bf16)],
        scratch_shapes=exchange_scratch(tiles, rows)
        + [
            pltpu.VMEM((2, w_o.shape[0], TILE), bf16),
            pltpu.VMEM((tiles, rows, TILE), bf16),
            pltpu.VMEM((2, padded, TILE), bf16),
            pltpu.VMEM((2, padded, TILE), bf16),
            pltpu.VMEM((blocks, count, 256), jnp.float32),
            pltpu.VMEM((blocks, count, 256), jnp.float32),
            pltpu.SemaphoreType.DMA((13,)),
            pltpu.SemaphoreType.DMA((13, tiles)),
            pltpu.SemaphoreType.DMA((2,)),
            pltpu.SemaphoreType.DMA((2, 2)),
            pltpu.SemaphoreType.DMA,
            pltpu.SemaphoreType.REGULAR,
        ],
        compiler_params=pltpu.CompilerParams(collective_id=1, has_side_effects=True, vmem_limit_bytes=VMEM_MAX),
        name="mlp_stage",
    )(attended, gain, hidden, w_o, gate_t, up_t)


def head_stage(product, gain, residual, score_id, w_down, head_t):
    count, padded = product.shape
    tiles, rows, _ = residual.shape
    vocab = head_t.shape[0]
    block = vocab // 5
    vmem = pl.BlockSpec(memory_space=pltpu.VMEM)
    anywhere = pl.BlockSpec(memory_space=pl.ANY)
    bf16 = jnp.bfloat16
    return pl.pallas_call(
        head_kernel,
        in_specs=[vmem, vmem, vmem, vmem, anywhere, anywhere],
        out_specs=vmem,
        out_shape=jax.ShapeDtypeStruct((2, 8, count // 8), jnp.float32),
        scratch_shapes=[pltpu.VMEM((tiles, rows, TILE), bf16)]
        + exchange_scratch(tiles, rows)
        + [
            pltpu.VMEM((2, padded, TILE), bf16),
            pltpu.VMEM((2, vocab, TILE), bf16),
            pltpu.VMEM((5, block, count), jnp.float32),
            pltpu.VMEM((8, 3, 8, count // 8), jnp.float32),
            pltpu.SemaphoreType.DMA((13,)),
            pltpu.SemaphoreType.DMA((13, tiles)),
            pltpu.SemaphoreType.DMA((2,)),
            pltpu.SemaphoreType.DMA((2,)),
            pltpu.SemaphoreType.DMA((7,)),
            pltpu.SemaphoreType.DMA((7,)),
            pltpu.SemaphoreType.REGULAR,
        ],
        compiler_params=pltpu.CompilerParams(collective_id=2, has_side_effects=True, vmem_limit_bytes=VMEM_MAX),
        name="head_stage",
    )(product, gain, residual, score_id, w_down, head_t)


def rope_tables(positions, head_dim):
    half = head_dim // 2
    inv_freq = 1.0 / (ROPE_THETA ** (jnp.arange(half, dtype=jnp.float32) * (2.0 / head_dim)))
    angles = positions.astype(jnp.float32)[:, None] * inv_freq
    cosine = jnp.cos(angles)
    sine = jnp.sin(angles)
    return jnp.concatenate([cosine, cosine], axis=-1), jnp.concatenate([-sine, sine], axis=-1)


def solution(mesh):
    def group_step(hidden, tree_mask, depth, ctx_len, block_table, score_id, k_cache, v_cache, attn_norm, w_q, w_k, w_v, w_o, mlp_norm, w_gate, w_up, w_down, final_norm, w_lm):
        requests, nodes, dim = hidden.shape
        head_dim = k_cache.shape[3]
        rows = requests * nodes
        flat = hidden.reshape(rows, dim)
        cosine, sine = rope_tables((ctx_len[:, None] + depth).reshape(rows), head_dim)
        query, key_new, val_new = project(flat, attn_norm.reshape(1, dim), cosine, sine, w_q, w_k, w_v, requests, nodes, head_dim, 4)
        attended, k_out, v_out = attend(
            block_table, ctx_len, query, key_new, val_new, tree_mask, jnp.transpose(k_cache, (0, 2, 1, 3)), jnp.transpose(v_cache, (0, 2, 1, 3))
        )
        k_out = jnp.transpose(k_out, (0, 2, 1, 3))
        v_out = jnp.transpose(v_out, (0, 2, 1, 3))

        tiles = dim // TILE
        product, residual = mlp_stage(attended, mlp_norm.reshape(tiles, 1, TILE), flat, w_o, w_gate.T, w_up.T)
        scores = head_stage(product, final_norm.reshape(tiles, 1, TILE), residual, score_id.reshape(1, rows), w_down, w_lm.T)
        log_norm = scores[0]
        log_prob = scores[1]
        return log_norm.reshape(requests, nodes), log_prob.reshape(requests, nodes), k_out, v_out

    request_spec = P("dp", None, None)
    node_spec = P("dp", None)
    cache_spec = P("dp", None, "tp", None)
    shared_spec = P(None)
    column_spec = P(None, "tp")
    row_spec = P("tp", None)
    in_specs = (request_spec, request_spec, node_spec, P("dp"), node_spec, node_spec, cache_spec, cache_spec, shared_spec, column_spec, column_spec, column_spec, row_spec, shared_spec, column_spec, column_spec, row_spec, shared_spec, column_spec)
    out_specs = (node_spec, node_spec, cache_spec, cache_spec)
    return jax.shard_map(group_step, mesh=mesh, in_specs=in_specs, out_specs=out_specs, check_vma=False)
```

```python
import functools

import jax
import jax.numpy as jnp
from jax import lax
from jax.experimental import pallas as pl
from jax.experimental.pallas import tpu as pltpu
from jax.sharding import PartitionSpec as P

RMS_EPS = 1e-5
ROPE_THETA = 500000
MESH = pl.DeviceIdType.MESH
NT_DIMS = (((1,), (1,)), ((), ()))
VMEM_MAX = 67043328


def dot_nt(left, right):
    return lax.dot_general(left, right, NT_DIMS, preferred_element_type=jnp.float32)


def qkv_kernel(hid_ref, gain_ref, cos_ref, sin_ref, wq_ref, wk_ref, wv_ref, q_ref, k_ref, v_ref):
    requests, heads, nodes, head_dim = q_ref.shape
    widened = hid_ref[...].astype(jnp.float32)
    scale = lax.rsqrt(jnp.mean(widened * widened, axis=-1, keepdims=True) + RMS_EPS)
    gain = gain_ref[...].reshape(1, widened.shape[1]).astype(jnp.float32)
    normed = (widened * scale * gain).astype(jnp.bfloat16)
    cosine = cos_ref[...]
    sine = sin_ref[...]

    def put(out_ref, weight_ref, turned):
        product = jnp.dot(normed, weight_ref[...], preferred_element_type=jnp.float32)
        for h in range(heads):
            part = product[:, h * head_dim : (h + 1) * head_dim]
            if turned:
                part = part * cosine + pltpu.roll(part, head_dim // 2, 1) * sine
            out_ref[:, h] = part.astype(jnp.bfloat16).reshape(requests, nodes, head_dim)

    put(q_ref, wq_ref, True)
    put(k_ref, wk_ref, True)
    put(v_ref, wv_ref, False)


def project(hidden, gain, cosine, sine, w_q, w_k, w_v, requests, nodes, head_dim, group):
    rows, dim = hidden.shape
    cols = w_q.shape[1]
    heads = cols // head_dim
    block = group * nodes
    full = pl.BlockSpec((dim, cols), lambda i: (0, 0), pipeline_mode=pl.Buffered(1))
    out = pl.BlockSpec((group, heads, nodes, head_dim), lambda i: (i, 0, 0, 0))
    shape = jax.ShapeDtypeStruct((requests, heads, nodes, head_dim), jnp.bfloat16)
    return pl.pallas_call(
        qkv_kernel,
        grid=(rows // block,),
        in_specs=[
            pl.BlockSpec((block, dim), lambda i: (i, 0)),
            pl.BlockSpec((dim,), lambda i: (0,)),
            pl.BlockSpec((block, head_dim), lambda i: (i, 0)),
            pl.BlockSpec((block, head_dim), lambda i: (i, 0)),
            full,
            full,
            full,
        ],
        out_specs=[out, out, out],
        out_shape=[shape, shape, shape],
        compiler_params=pltpu.CompilerParams(vmem_limit_bytes=VMEM_MAX),
        name="project",
    )(hidden, gain, cosine, sine, w_q, w_k, w_v)


def attend_kernel(table_ref, ctx_ref, q_ref, kn_ref, vn_ref, mask_ref, kc_ref, vc_ref, out_ref, ko_ref, vo_ref, kbuf, vbuf, rsem, wsem):
    b = pl.program_id(0)
    count = pl.num_programs(0)
    pages, heads, page, head_dim = kbuf.shape[1:]
    span = pages * page
    nodes = q_ref.shape[2]
    window = nodes + page

    def load(i, slot):
        for s in range(pages):
            block = table_ref[i, s]
            pltpu.make_async_copy(kc_ref.at[block], kbuf.at[slot, s], rsem.at[0, slot]).start()
            pltpu.make_async_copy(vc_ref.at[block], vbuf.at[slot, s], rsem.at[1, slot]).start()

    def save(i, slot):
        for s in range(pages):
            block = table_ref[i, s]
            pltpu.make_async_copy(kbuf.at[slot, s], ko_ref.at[block], wsem.at[0, slot]).start()
            pltpu.make_async_copy(vbuf.at[slot, s], vo_ref.at[block], wsem.at[1, slot]).start()

    def whole(slot, sem):
        pltpu.make_async_copy(kbuf.at[slot], kbuf.at[slot], sem.at[0, slot]).wait()
        pltpu.make_async_copy(vbuf.at[slot], vbuf.at[slot], sem.at[1, slot]).wait()

    slot = lax.rem(b, 3)
    after = lax.rem(b + 1, 3)

    @pl.when(b == 0)
    def _():
        load(0, 0)

    @pl.when(b >= 2)
    def _():
        whole(after, wsem)

    whole(slot, rsem)
    load(jnp.minimum(b + 1, count - 1), after)
    ctx = ctx_ref[b]
    first = jnp.minimum(ctx // page, pages - window // page)
    base = first * page
    row = base + lax.broadcasted_iota(jnp.int32, (window, nodes), 0)
    node = ctx + lax.broadcasted_iota(jnp.int32, (window, nodes), 1)
    place = jnp.where(row == node, 1.0, 0.0).astype(jnp.bfloat16)
    slot_id = base + lax.broadcasted_iota(jnp.int32, (window, head_dim), 0)
    fresh = (slot_id >= ctx) & (slot_id < ctx + nodes)
    for buf, new_ref in ((kbuf, kn_ref), (vbuf, vn_ref)):
        moved = [jnp.dot(place, new_ref[0, h], preferred_element_type=jnp.float32) for h in range(heads)]
        for h in range(heads):
            for i in range(window // page):
                rows = slice(i * page, (i + 1) * page)
                old = buf[slot, first + i, h].astype(jnp.float32)
                buf[slot, first + i, h] = jnp.where(fresh[rows], moved[h][rows], old).astype(jnp.bfloat16)
    save(b, slot)
    spread = jnp.where(
        ctx + lax.broadcasted_iota(jnp.int32, (nodes, span), 0) == lax.broadcasted_iota(jnp.int32, (nodes, span), 1), 1.0, 0.0
    ).astype(jnp.bfloat16)
    linked = jnp.where(mask_ref[0] > 0, 1.0, 0.0).astype(jnp.bfloat16)
    seen_new = jnp.dot(linked, spread, preferred_element_type=jnp.float32) > 0.5
    seen = seen_new | (lax.broadcasted_iota(jnp.int32, (nodes, span), 1) < ctx)
    scale = head_dim**-0.5
    scores = [dot_nt(q_ref[0, h], kbuf[slot, :, h].reshape(span, head_dim)) for h in range(heads)]
    scores = [jnp.where(seen, score * scale, -jnp.inf) for score in scores]
    tops = [jnp.max(score, axis=-1, keepdims=True) for score in scores]
    probs = [jnp.exp(score - top) for score, top in zip(scores, tops)]
    totals = [jnp.sum(prob, axis=-1, keepdims=True) for prob in probs]
    mixed = [
        jnp.dot(prob.astype(jnp.bfloat16), vbuf[slot, :, h].reshape(span, head_dim), preferred_element_type=jnp.float32)
        for h, prob in enumerate(probs)
    ]
    for h in range(heads):
        out_ref[:, h * head_dim : (h + 1) * head_dim] = (mixed[h] / totals[h]).astype(jnp.bfloat16)

    @pl.when(b == count - 1)
    def _():
        whole(lax.rem(b + 2, 3), wsem)
        whole(slot, wsem)
        whole(after, rsem)


def attend(table, ctx_len, query, key_new, val_new, tree_mask, k_cache, v_cache):
    requests, heads, nodes, head_dim = query.shape
    page = k_cache.shape[2]
    pages = table.shape[1]
    node_spec = pl.BlockSpec((1, heads, nodes, head_dim), lambda b, *_: (b, 0, 0, 0))
    anywhere = pl.BlockSpec(memory_space=pl.ANY)
    return pl.pallas_call(
        attend_kernel,
        grid_spec=pltpu.PrefetchScalarGridSpec(
            num_scalar_prefetch=2,
            grid=(requests,),
            in_specs=[
                node_spec,
                node_spec,
                node_spec,
                pl.BlockSpec((1, nodes, nodes), lambda b, *_: (b, 0, 0)),
                anywhere,
                anywhere,
            ],
            out_specs=[pl.BlockSpec((nodes, heads * head_dim), lambda b, *_: (b, 0)), anywhere, anywhere],
            scratch_shapes=[
                pltpu.VMEM((3, pages, heads, page, head_dim), jnp.bfloat16),
                pltpu.VMEM((3, pages, heads, page, head_dim), jnp.bfloat16),
                pltpu.SemaphoreType.DMA((2, 3)),
                pltpu.SemaphoreType.DMA((2, 3)),
            ],
        ),
        out_shape=[
            jax.ShapeDtypeStruct((requests * nodes, heads * head_dim), jnp.bfloat16),
            jax.ShapeDtypeStruct(k_cache.shape, k_cache.dtype),
            jax.ShapeDtypeStruct(v_cache.shape, v_cache.dtype),
        ],
        name="attend",
    )(table, ctx_len, query, key_new, val_new, tree_mask, k_cache, v_cache)


TILE = 512
HALF = TILE // 2
PAIR, X1, Y1, X2, Y2, GX, GY, GP, FX, FY, PX, PY, PD = range(13)


def seat():
    me = lax.axis_index("tp")
    core = me % 2
    x = (me // 2) % 2
    y = me // 4
    to_x = y * 4 + (1 - x) * 2 + core
    to_y = (1 - y) * 4 + x * 2 + core
    to_pair = y * 4 + x * 2 + (1 - core)
    return me, core, x, y, to_x, to_y, to_pair


def send(src, dst, ssem, rsem, kind, t, target):
    pltpu.make_async_remote_copy(
        src_ref=src, dst_ref=dst, send_sem=ssem.at[kind], recv_sem=rsem.at[kind, t], device_id={"tp": target}, device_id_type=MESH
    ).start()


def landed(ref, rsem, kind, t):
    pltpu.make_async_copy(ref, ref, rsem.at[kind, t]).wait()


def sent(ref, ssem, kind):
    pltpu.make_async_copy(ref, ref, ssem.at[kind]).wait()


def reduce_norm_gather(left_ref, w_hbm, wbuf, wsem, resid, resid_ready, gain_ref, h_ref, mbuf, r1, rx, ry, r2x, r2y, ssq, ssem, rsem, free, idle_work, compute):
    me, core, x, y, to_x, to_y, to_pair = seat()
    tiles = mbuf.shape[0]
    rows = mbuf.shape[4]
    depth = w_hbm.shape[0]

    def fetch(t):
        cols = pl.ds(pl.multiple_of(t * TILE, TILE), TILE)
        return pltpu.make_async_copy(w_hbm.at[:, cols], wbuf.at[t % 2, pl.ds(0, depth)], wsem.at[t % 2])

    fetch(0).start()
    fetch(1).start()

    def scatter_step(j, _):
        @pl.when(j < tiles)
        def _():
            fetch(j).wait()
            for half in range(2):
                cols = pl.ds(half * HALF, HALF)
                part = jnp.dot(left_ref[...], wbuf[j % 2, :, cols], preferred_element_type=jnp.float32)
                mbuf[j, :, :, :, :, cols] = part.astype(jnp.bfloat16).reshape(2, 2, 2, rows, HALF)

            @pl.when(j + 2 < tiles)
            def _():
                fetch(j + 2).start()

            send(mbuf.at[j, :, :, 1 - core], r1.at[j], ssem, rsem, PAIR, j, to_pair)
            idle_work(j)

        @pl.when((j >= 1) & (j < tiles + 1))
        def _():
            t = j - 1
            landed(r1.at[t], rsem, PAIR, t)
            for yy in range(2):
                for xx in range(2):
                    mbuf[t, yy, xx, core] = mbuf[t, yy, xx, core] + r1[t, yy, xx]
            send(mbuf.at[t, :, 1 - x, core, :, pl.ds(0, HALF)], rx.at[t], ssem, rsem, X1, t, to_x)
            send(mbuf.at[t, 1 - y, :, core, :, pl.ds(HALF, HALF)], ry.at[t], ssem, rsem, Y1, t, to_y)

        @pl.when((j >= 2) & (j < tiles + 2))
        def _():
            t = j - 2
            landed(rx.at[t], rsem, X1, t)
            for yy in range(2):
                mbuf[t, yy, x, core, :, pl.ds(0, HALF)] = mbuf[t, yy, x, core, :, pl.ds(0, HALF)] + rx[t, yy]
            send(mbuf.at[t, 1 - y, x, core, :, pl.ds(0, HALF)], r2y.at[t], ssem, rsem, Y2, t, to_y)
            landed(ry.at[t], rsem, Y1, t)
            for xx in range(2):
                mbuf[t, y, xx, core, :, pl.ds(HALF, HALF)] = mbuf[t, y, xx, core, :, pl.ds(HALF, HALF)] + ry[t, xx]
            send(mbuf.at[t, y, 1 - x, core, :, pl.ds(HALF, HALF)], r2x.at[t], ssem, rsem, X2, t, to_x)

        @pl.when(j == 3)
        def _():
            resid_ready()
            ssq[...] = jnp.zeros_like(ssq)

        @pl.when(j >= 3)
        def _():
            t = j - 3
            landed(r2y.at[t], rsem, Y2, t)
            landed(r2x.at[t], rsem, X2, t)
            for half, other in ((0, r2y), (1, r2x)):
                cols = pl.ds(half * HALF, HALF)
                total = (mbuf[t, y, x, core, :, cols] + other[t]).astype(jnp.float32)
                new = (resid[t, :, cols].astype(jnp.float32) + total).astype(jnp.bfloat16)
                h_ref[t, :, cols] = new
                wide = new.astype(jnp.float32)
                wide = wide * wide
                for lane in range(0, HALF, 128):
                    ssq[...] += wide[:, lane : lane + 128]

        return 0

    lax.fori_loop(0, tiles + 3, scatter_step, 0)
    sent(r1, ssem, PAIR)
    sent(rx, ssem, X1)
    sent(ry, ssem, Y1)
    sent(r2x, ssem, X2)
    sent(r2y, ssem, Y2)
    for target in (to_x, to_y, to_pair):
        pl.semaphore_signal(free, inc=1, device_id={"tp": target}, device_id_type=MESH)
    scale = lax.rsqrt(jnp.sum(ssq[...], axis=-1, keepdims=True) * (1.0 / (tiles * TILE)) + RMS_EPS)

    for t in range(tiles):
        gain = gain_ref[pl.ds(t * TILE, TILE)].reshape(1, TILE).astype(jnp.float32)
        mbuf[t, y, x, core] = (h_ref[t].astype(jnp.float32) * scale * gain).astype(jnp.bfloat16)

    pl.semaphore_wait(free, 3)

    def own(t):
        mine = mbuf.at[t, y, x, core]
        send(mine, mine, ssem, rsem, GX, t, to_x)
        send(mine, mine, ssem, rsem, GY, t, to_y)
        send(mine, mine, ssem, rsem, GP, t, to_pair)

    own(0)
    own(1)

    def gather_step(j, _):
        @pl.when(j + 2 < tiles)
        def _():
            own(j + 2)

        @pl.when(j < tiles)
        def _():
            from_x = mbuf.at[j, y, 1 - x, core]
            from_y = mbuf.at[j, 1 - y, x, core]
            landed(from_x, rsem, GX, j)
            upper = from_x.at[pl.ds(0, rows // 2)]
            send(upper, upper, ssem, rsem, FY, j, to_y)
            send(from_x, from_x, ssem, rsem, PX, j, to_pair)
            landed(from_y, rsem, GY, j)
            lower = from_y.at[pl.ds(rows // 2, rows // 2)]
            send(lower, lower, ssem, rsem, FX, j, to_x)
            send(from_y, from_y, ssem, rsem, PY, j, to_pair)

        @pl.when((j >= 1) & (j < tiles + 1))
        def _():
            t = j - 1
            far = mbuf.at[t, 1 - y, 1 - x, core]
            landed(far.at[pl.ds(0, rows // 2)], rsem, FY, t)
            landed(far.at[pl.ds(rows // 2, rows // 2)], rsem, FX, t)
            send(far, far, ssem, rsem, PD, t, to_pair)

        @pl.when(j >= 2)
        def _():
            t = j - 2
            landed(mbuf.at[t, y, x, 1 - core], rsem, GP, t)
            landed(mbuf.at[t, y, 1 - x, 1 - core], rsem, PX, t)
            landed(mbuf.at[t, 1 - y, x, 1 - core], rsem, PY, t)
            landed(mbuf.at[t, 1 - y, 1 - x, 1 - core], rsem, PD, t)
            compute(t)

        return 0

    lax.fori_loop(0, tiles + 2, gather_step, 0)
    for kind in (GX, GY, GP, PX, PY, PD):
        sent(h_ref, ssem, kind)
    for kind in (FX, FY):
        sent(h_ref.at[pl.ds(0, tiles // 2)], ssem, kind)


def greet(targets):
    barrier = pltpu.get_barrier_semaphore()
    for target in targets:
        pl.semaphore_signal(barrier, inc=1, device_id={"tp": target}, device_id_type=MESH)
    pl.semaphore_wait(barrier, len(targets))


def mlp_kernel(att_ref, gain_ref, hid_hbm, wo_hbm, wg_hbm, wu_hbm, prod_ref, h_ref, mbuf, r1, rx, ry, r2x, r2y, ssq, wo_buf, resid, wg_buf, wu_buf, acc_g, acc_u, ssem, rsem, wsem, gsem, hsem, free):
    me, core, x, y, to_x, to_y, to_pair = seat()
    tiles = mbuf.shape[0]
    rows = mbuf.shape[4]
    width = wg_hbm.shape[0]
    padded = wg_buf.shape[1]
    blocks = padded // 256

    def fetch(t):
        cols = pl.ds(pl.multiple_of(t * TILE, TILE), TILE)
        slot = t % 2
        return (
            pltpu.make_async_copy(wg_hbm.at[:, cols], wg_buf.at[slot, pl.ds(0, width)], gsem.at[0, slot]),
            pltpu.make_async_copy(wu_hbm.at[:, cols], wu_buf.at[slot, pl.ds(0, width)], gsem.at[1, slot]),
        )

    greet((to_x, to_y, to_pair))
    if padded > width:
        for slot in range(2):
            wg_buf[slot, pl.ds(width, padded - width)] = jnp.zeros((padded - width, TILE), jnp.bfloat16)
            wu_buf[slot, pl.ds(width, padded - width)] = jnp.zeros((padded - width, TILE), jnp.bfloat16)
    for t in range(2):
        for copy in fetch(t):
            copy.start()

    def hidden_copy(t):
        cols = pl.ds(t * TILE, TILE)
        return pltpu.make_async_copy(hid_hbm.at[pl.ds(pl.multiple_of(me * rows, rows), rows), cols], resid.at[t], hsem)

    for t in range(tiles):
        hidden_copy(t).start()

    def resid_ready():
        pltpu.make_async_copy(resid, resid, hsem).wait()

    def idle_work(j):
        @pl.when(j < blocks)
        def _():
            cols = pl.ds(pl.multiple_of(j * 256, 256), 256)
            acc_g[:, cols] = jnp.zeros((8 * rows, 256), jnp.float32)
            acc_u[:, cols] = jnp.zeros((8 * rows, 256), jnp.float32)

    def compute(t):
        slot = t % 2
        for copy in fetch(t):
            copy.wait()

        left = mbuf[t].reshape(8 * rows, TILE)
        acc_g[...] += dot_nt(left, wg_buf[slot])
        acc_u[...] += dot_nt(left, wu_buf[slot])

        @pl.when(t + 2 < tiles)
        def _():
            for copy in fetch(t + 2):
                copy.start()

    reduce_norm_gather(att_ref, wo_hbm, wo_buf, wsem, resid, resid_ready, gain_ref, h_ref, mbuf, r1, rx, ry, r2x, r2y, ssq, ssem, rsem, free, idle_work, compute)

    def finish(n, _):
        cols = pl.ds(pl.multiple_of(n * 256, 256), 256)
        prod_ref[:, cols] = (jax.nn.silu(acc_g[:, cols]) * acc_u[:, cols]).astype(jnp.bfloat16)
        return 0

    lax.fori_loop(0, blocks, finish, 0)


def head_kernel(prod_ref, gain_ref, res_ref, id_ref, wd_hbm, wl_hbm, norm_ref, prob_ref, h_ref, mbuf, r1, rx, ry, r2x, r2y, ssq, wd_buf, wl_buf, acc, stats, ssem, rsem, wsem, lsem, tsem, usem, free):
    me, core, x, y, to_x, to_y, to_pair = seat()
    tiles = mbuf.shape[0]
    rows = mbuf.shape[4]
    depth = wd_hbm.shape[0]
    padded = wd_buf.shape[1]
    blocks, block = acc.shape[0], acc.shape[1]
    vocab = wl_hbm.shape[0]
    others = [(me + i) % 8 for i in range(1, 8)]

    def fetch(t):
        cols = pl.ds(pl.multiple_of(t * TILE, TILE), TILE)
        return pltpu.make_async_copy(wl_hbm.at[:, cols], wl_buf.at[t % 2], lsem.at[t % 2])

    greet(others)
    if padded > depth:
        for slot in range(2):
            wd_buf[slot, pl.ds(depth, padded - depth)] = jnp.zeros((padded - depth, TILE), jnp.bfloat16)
    fetch(0).start()
    fetch(1).start()

    def resid_ready():
        pass

    def idle_work(j):
        @pl.when(j < blocks)
        def _():
            acc[j] = jnp.zeros(acc.shape[1:], jnp.float32)

    def compute(t):
        fetch(t).wait()

        def one(n, _):
            part = pl.ds(pl.multiple_of(n * block, block), block)
            acc[n] += dot_nt(wl_buf[t % 2, part], mbuf[t].reshape(8 * rows, TILE))
            return 0

        lax.fori_loop(0, blocks, one, 0)

        @pl.when(t + 2 < tiles)
        def _():
            fetch(t + 2).start()

    reduce_norm_gather(prod_ref, wd_hbm, wd_buf, wsem, res_ref, resid_ready, gain_ref, h_ref, mbuf, r1, rx, ry, r2x, r2y, ssq, ssem, rsem, free, idle_work, compute)

    count = 8 * rows

    def top_step(n, best):
        return jnp.maximum(best, jnp.max(acc[n].reshape(block // 8, 8, count), axis=0))

    best = lax.fori_loop(0, blocks, top_step, jnp.full((8, count), -jnp.inf, jnp.float32))
    best = jnp.max(best, axis=0, keepdims=True)
    local_id = jnp.concatenate([id_ref[i : i + 1] for i in range(id_ref.shape[0])], axis=1) - me * vocab

    def sum_step(n, carry):
        total, picked = carry
        value = acc[n]
        hit = lax.broadcasted_iota(jnp.int32, (block, count), 0) + n * block == local_id
        total = total + jnp.sum(jnp.exp(value - best).reshape(block // 8, 8, count), axis=0)
        picked = picked + jnp.sum(jnp.where(hit, value, 0.0).reshape(block // 8, 8, count), axis=0)
        return total, picked

    zero = jnp.zeros((8, count), jnp.float32)
    total, picked = lax.fori_loop(0, blocks, sum_step, (zero, zero))

    def pack(values):
        return jnp.concatenate([values[:, i * 128 : (i + 1) * 128] for i in range(8)], axis=0)

    stats[me, 0] = pack(best)
    stats[me, 1] = pack(jnp.sum(total, axis=0, keepdims=True))
    stats[me, 2] = pack(jnp.sum(picked, axis=0, keepdims=True))
    copies = []
    for i, other in enumerate(others):
        copy = pltpu.make_async_remote_copy(
            src_ref=stats.at[me], dst_ref=stats.at[me], send_sem=tsem.at[i], recv_sem=usem.at[i], device_id={"tp": other}, device_id_type=MESH
        )
        copy.start()
        copies.append(copy)
    for copy in copies:
        copy.wait()
    top = stats[0, 0]
    for d in range(1, 8):
        top = jnp.maximum(top, stats[d, 0])
    whole = jnp.zeros_like(top)
    score = jnp.zeros_like(top)
    for d in range(8):
        whole = whole + stats[d, 1] * jnp.exp(stats[d, 0] - top)
        score = score + stats[d, 2]
    norm = top + jnp.log(whole)
    for ref, values in ((norm_ref, norm), (prob_ref, score - norm)):
        nodes = ref.shape[1]
        for i in range(ref.shape[0]):
            start = i * nodes
            ref[i : i + 1] = values[start // 128 : start // 128 + 1, start % 128 : start % 128 + nodes]


def exchange_scratch(tiles, rows):
    bf16 = jnp.bfloat16
    return [
        pltpu.VMEM((tiles, 2, 2, 2, rows, TILE), bf16),
        pltpu.VMEM((tiles, 2, 2, rows, TILE), bf16),
        pltpu.VMEM((tiles, 2, rows, HALF), bf16),
        pltpu.VMEM((tiles, 2, rows, HALF), bf16),
        pltpu.VMEM((tiles, rows, HALF), bf16),
        pltpu.VMEM((tiles, rows, HALF), bf16),
        pltpu.VMEM((rows, 128), jnp.float32),
    ]


def mlp_stage(attended, gain, hidden, w_o, gate_t, up_t):
    count, dim = hidden.shape
    tiles = dim // TILE
    rows = count // 8
    width = gate_t.shape[0]
    blocks = pl.cdiv(width, 256)
    padded = blocks * 256
    vmem = pl.BlockSpec(memory_space=pltpu.VMEM)
    anywhere = pl.BlockSpec(memory_space=pl.ANY)
    bf16 = jnp.bfloat16
    return pl.pallas_call(
        mlp_kernel,
        in_specs=[vmem, vmem, anywhere, anywhere, anywhere, anywhere],
        out_specs=[vmem, vmem],
        out_shape=[jax.ShapeDtypeStruct((count, padded), bf16), jax.ShapeDtypeStruct((tiles, rows, TILE), bf16)],
        scratch_shapes=exchange_scratch(tiles, rows)
        + [
            pltpu.VMEM((2, w_o.shape[0], TILE), bf16),
            pltpu.VMEM((tiles, rows, TILE), bf16),
            pltpu.VMEM((2, padded, TILE), bf16),
            pltpu.VMEM((2, padded, TILE), bf16),
            pltpu.VMEM((count, padded), jnp.float32),
            pltpu.VMEM((count, padded), jnp.float32),
            pltpu.SemaphoreType.DMA((13,)),
            pltpu.SemaphoreType.DMA((13, tiles)),
            pltpu.SemaphoreType.DMA((2,)),
            pltpu.SemaphoreType.DMA((2, 2)),
            pltpu.SemaphoreType.DMA,
            pltpu.SemaphoreType.REGULAR,
        ],
        compiler_params=pltpu.CompilerParams(collective_id=1, has_side_effects=True, vmem_limit_bytes=VMEM_MAX),
        name="mlp_stage",
    )(attended, gain, hidden, w_o, gate_t, up_t)


def head_stage(product, gain, residual, score_id, w_down, head_t):
    count, padded = product.shape
    tiles, rows, _ = residual.shape
    vocab = head_t.shape[0]
    block = vocab // 2
    vmem = pl.BlockSpec(memory_space=pltpu.VMEM)
    anywhere = pl.BlockSpec(memory_space=pl.ANY)
    bf16 = jnp.bfloat16
    return pl.pallas_call(
        head_kernel,
        in_specs=[vmem, vmem, vmem, vmem, anywhere, anywhere],
        out_specs=[vmem, vmem],
        out_shape=[jax.ShapeDtypeStruct(score_id.shape, jnp.float32)] * 2,
        scratch_shapes=[pltpu.VMEM((tiles, rows, TILE), bf16)]
        + exchange_scratch(tiles, rows)
        + [
            pltpu.VMEM((2, padded, TILE), bf16),
            pltpu.VMEM((2, vocab, TILE), bf16),
            pltpu.VMEM((2, block, count), jnp.float32),
            pltpu.VMEM((8, 3, 8, count // 8), jnp.float32),
            pltpu.SemaphoreType.DMA((13,)),
            pltpu.SemaphoreType.DMA((13, tiles)),
            pltpu.SemaphoreType.DMA((2,)),
            pltpu.SemaphoreType.DMA((2,)),
            pltpu.SemaphoreType.DMA((7,)),
            pltpu.SemaphoreType.DMA((7,)),
            pltpu.SemaphoreType.REGULAR,
        ],
        compiler_params=pltpu.CompilerParams(collective_id=2, has_side_effects=True, vmem_limit_bytes=VMEM_MAX),
        name="head_stage",
    )(product, gain, residual, score_id, w_down, head_t)


def rope_tables(positions, head_dim):
    half = head_dim // 2
    lane = jnp.arange(head_dim, dtype=jnp.int32)
    inv_freq = 1.0 / (ROPE_THETA ** ((lane % half).astype(jnp.float32) * (2.0 / head_dim)))
    angles = positions.astype(jnp.float32)[:, None] * inv_freq
    return jnp.cos(angles), jnp.sin(angles) * jnp.where(lane < half, -1.0, 1.0)


def solution(mesh):
    def group_step(hidden, tree_mask, depth, ctx_len, block_table, score_id, k_cache, v_cache, attn_norm, w_q, w_k, w_v, w_o, mlp_norm, w_gate, w_up, w_down, final_norm, w_lm):
        requests, nodes, dim = hidden.shape
        head_dim = k_cache.shape[3]
        rows = requests * nodes
        flat = hidden.reshape(rows, dim)
        cosine, sine = rope_tables((ctx_len[:, None] + depth).reshape(rows), head_dim)
        query, key_new, val_new = project(flat, attn_norm, cosine, sine, w_q, w_k, w_v, requests, nodes, head_dim, 4)
        attended, k_out, v_out = attend(
            block_table, ctx_len, query, key_new, val_new, tree_mask, jnp.transpose(k_cache, (0, 2, 1, 3)), jnp.transpose(v_cache, (0, 2, 1, 3))
        )
        k_out = jnp.transpose(k_out, (0, 2, 1, 3))
        v_out = jnp.transpose(v_out, (0, 2, 1, 3))

        product, residual = mlp_stage(attended, mlp_norm, flat, w_o, w_gate.T, w_up.T)
        log_norm, log_prob = head_stage(product, final_norm, residual, score_id, w_down, w_lm.T)
        return log_norm.reshape(requests, nodes), log_prob.reshape(requests, nodes), k_out, v_out

    request_spec = P("dp", None, None)
    node_spec = P("dp", None)
    cache_spec = P("dp", None, "tp", None)
    shared_spec = P(None)
    column_spec = P(None, "tp")
    row_spec = P("tp", None)
    in_specs = (request_spec, request_spec, node_spec, P("dp"), node_spec, node_spec, cache_spec, cache_spec, shared_spec, column_spec, column_spec, column_spec, row_spec, shared_spec, column_spec, column_spec, row_spec, shared_spec, column_spec)
    out_specs = (node_spec, node_spec, cache_spec, cache_spec)
    return jax.shard_map(group_step, mesh=mesh, in_specs=in_specs, out_specs=out_specs, check_vma=False)
```

```python
import jax
import jax.numpy as jnp
from jax import lax
from jax.experimental import pallas as pl
from jax.experimental.pallas import tpu as pltpu
from jax.sharding import PartitionSpec as P

RMS_EPS = 1e-5
ROPE_THETA = 500000
MESH = pl.DeviceIdType.MESH
NT_DIMS = (((1,), (1,)), ((), ()))
VMEM_MAX = 67043328


def dot_nt(left, right):
    return lax.dot_general(left, right, NT_DIMS, preferred_element_type=jnp.float32)


def qkv_kernel(hid_ref, gain_ref, cos_ref, sin_ref, wq_ref, wk_ref, wv_ref, q_ref, k_ref, v_ref):
    requests, heads, nodes, head_dim = q_ref.shape
    widened = hid_ref[...].astype(jnp.float32)
    scale = lax.rsqrt(jnp.mean(widened * widened, axis=-1, keepdims=True) + RMS_EPS)
    gain = gain_ref[...].reshape(1, widened.shape[1]).astype(jnp.float32)
    normed = (widened * scale * gain).astype(jnp.bfloat16)
    cosine = cos_ref[...]
    sine = sin_ref[...]

    def put(out_ref, weight_ref, turned):
        product = jnp.dot(normed, weight_ref[...], preferred_element_type=jnp.float32)
        for h in range(heads):
            part = product[:, h * head_dim : (h + 1) * head_dim]
            if turned:
                part = part * cosine + pltpu.roll(part, head_dim // 2, 1) * sine
            out_ref[:, h] = part.astype(jnp.bfloat16).reshape(requests, nodes, head_dim)

    put(q_ref, wq_ref, True)
    put(k_ref, wk_ref, True)
    put(v_ref, wv_ref, False)


def project(hidden, gain, cosine, sine, w_q, w_k, w_v, requests, nodes, head_dim, group):
    rows, dim = hidden.shape
    cols = w_q.shape[1]
    heads = cols // head_dim
    block = group * nodes
    full = pl.BlockSpec((dim, cols), lambda i: (0, 0), pipeline_mode=pl.Buffered(1))
    out = pl.BlockSpec((group, heads, nodes, head_dim), lambda i: (i, 0, 0, 0))
    shape = jax.ShapeDtypeStruct((requests, heads, nodes, head_dim), jnp.bfloat16)
    return pl.pallas_call(
        qkv_kernel,
        grid=(rows // block,),
        in_specs=[
            pl.BlockSpec((block, dim), lambda i: (i, 0)),
            pl.BlockSpec((dim,), lambda i: (0,)),
            pl.BlockSpec((block, head_dim), lambda i: (i, 0)),
            pl.BlockSpec((block, head_dim), lambda i: (i, 0)),
            full,
            full,
            full,
        ],
        out_specs=[out, out, out],
        out_shape=[shape, shape, shape],
        compiler_params=pltpu.CompilerParams(vmem_limit_bytes=VMEM_MAX),
        name="project",
    )(hidden, gain, cosine, sine, w_q, w_k, w_v)


def attend_kernel(table_ref, ctx_ref, q_ref, kn_ref, vn_ref, mask_ref, kc_ref, vc_ref, out_ref, ko_ref, vo_ref, kbuf, vbuf, rsem, wsem):
    b = pl.program_id(0)
    count = pl.num_programs(0)
    pages, heads, page, head_dim = kbuf.shape[1:]
    span = pages * page
    nodes = q_ref.shape[2]
    window = nodes + page

    def load(i, slot):
        for s in range(pages):
            block = table_ref[i, s]
            pltpu.make_async_copy(kc_ref.at[block], kbuf.at[slot, s], rsem.at[0, slot]).start()
            pltpu.make_async_copy(vc_ref.at[block], vbuf.at[slot, s], rsem.at[1, slot]).start()

    def save(i, slot):
        for s in range(pages):
            block = table_ref[i, s]
            pltpu.make_async_copy(kbuf.at[slot, s], ko_ref.at[block], wsem.at[0, slot]).start()
            pltpu.make_async_copy(vbuf.at[slot, s], vo_ref.at[block], wsem.at[1, slot]).start()

    def whole(slot, sem):
        pltpu.make_async_copy(kbuf.at[slot], kbuf.at[slot], sem.at[0, slot]).wait()
        pltpu.make_async_copy(vbuf.at[slot], vbuf.at[slot], sem.at[1, slot]).wait()

    slot = lax.rem(b, 3)
    after = lax.rem(b + 1, 3)

    @pl.when(b == 0)
    def _():
        load(0, 0)

    @pl.when(b >= 2)
    def _():
        whole(after, wsem)

    whole(slot, rsem)
    load(jnp.minimum(b + 1, count - 1), after)
    ctx = ctx_ref[b]
    first = jnp.minimum(ctx // page, pages - window // page)
    base = first * page
    row = base + lax.broadcasted_iota(jnp.int32, (window, nodes), 0)
    node = ctx + lax.broadcasted_iota(jnp.int32, (window, nodes), 1)
    place = jnp.where(row == node, 1.0, 0.0).astype(jnp.bfloat16)
    slot_id = base + lax.broadcasted_iota(jnp.int32, (window, head_dim), 0)
    fresh = (slot_id >= ctx) & (slot_id < ctx + nodes)
    for buf, new_ref in ((kbuf, kn_ref), (vbuf, vn_ref)):
        moved = [jnp.dot(place, new_ref[0, h], preferred_element_type=jnp.float32) for h in range(heads)]
        for h in range(heads):
            for i in range(window // page):
                rows = slice(i * page, (i + 1) * page)
                old = buf[slot, first + i, h].astype(jnp.float32)
                buf[slot, first + i, h] = jnp.where(fresh[rows], moved[h][rows], old).astype(jnp.bfloat16)
    save(b, slot)
    spread = jnp.where(
        ctx + lax.broadcasted_iota(jnp.int32, (nodes, span), 0) == lax.broadcasted_iota(jnp.int32, (nodes, span), 1), 1.0, 0.0
    ).astype(jnp.bfloat16)
    linked = jnp.where(mask_ref[0] > 0, 1.0, 0.0).astype(jnp.bfloat16)
    seen_new = jnp.dot(linked, spread, preferred_element_type=jnp.float32) > 0.5
    seen = seen_new | (lax.broadcasted_iota(jnp.int32, (nodes, span), 1) < ctx)
    scale = head_dim**-0.5
    scores = [dot_nt(q_ref[0, h], kbuf[slot, :, h].reshape(span, head_dim)) for h in range(heads)]
    scores = [jnp.where(seen, score * scale, -jnp.inf) for score in scores]
    tops = [jnp.max(score, axis=-1, keepdims=True) for score in scores]
    probs = [jnp.exp(score - top) for score, top in zip(scores, tops)]
    totals = [jnp.sum(prob, axis=-1, keepdims=True) for prob in probs]
    mixed = [
        jnp.dot(prob.astype(jnp.bfloat16), vbuf[slot, :, h].reshape(span, head_dim), preferred_element_type=jnp.float32)
        for h, prob in enumerate(probs)
    ]
    for h in range(heads):
        out_ref[:, h * head_dim : (h + 1) * head_dim] = (mixed[h] / totals[h]).astype(jnp.bfloat16)

    @pl.when(b == count - 1)
    def _():
        whole(lax.rem(b + 2, 3), wsem)
        whole(slot, wsem)
        whole(after, rsem)


def attend(table, ctx_len, query, key_new, val_new, tree_mask, k_cache, v_cache):
    requests, heads, nodes, head_dim = query.shape
    page = k_cache.shape[2]
    pages = table.shape[1]
    node_spec = pl.BlockSpec((1, heads, nodes, head_dim), lambda b, *_: (b, 0, 0, 0))
    anywhere = pl.BlockSpec(memory_space=pl.ANY)
    return pl.pallas_call(
        attend_kernel,
        grid_spec=pltpu.PrefetchScalarGridSpec(
            num_scalar_prefetch=2,
            grid=(requests,),
            in_specs=[
                node_spec,
                node_spec,
                node_spec,
                pl.BlockSpec((1, nodes, nodes), lambda b, *_: (b, 0, 0)),
                anywhere,
                anywhere,
            ],
            out_specs=[pl.BlockSpec((nodes, heads * head_dim), lambda b, *_: (b, 0)), anywhere, anywhere],
            scratch_shapes=[
                pltpu.VMEM((3, pages, heads, page, head_dim), jnp.bfloat16),
                pltpu.VMEM((3, pages, heads, page, head_dim), jnp.bfloat16),
                pltpu.SemaphoreType.DMA((2, 3)),
                pltpu.SemaphoreType.DMA((2, 3)),
            ],
        ),
        out_shape=[
            jax.ShapeDtypeStruct((requests * nodes, heads * head_dim), jnp.bfloat16),
            jax.ShapeDtypeStruct(k_cache.shape, k_cache.dtype),
            jax.ShapeDtypeStruct(v_cache.shape, v_cache.dtype),
        ],
        name="attend",
    )(table, ctx_len, query, key_new, val_new, tree_mask, k_cache, v_cache)


TILE = 512
HALF = TILE // 2
PAIR, X1, Y1, X2, Y2, GX, GY, GP, FX, FY, PX, PY, PD = range(13)


def seat():
    me = lax.axis_index("tp")
    core = me % 2
    x = (me // 2) % 2
    y = me // 4
    blocks = []
    for dy in range(2):
        for dx in range(2):
            for dc in range(2):
                blocks.append((1 - y if dy else y) * 4 + (1 - x if dx else x) * 2 + (1 - core if dc else core))
    return me, blocks


def landed(ref, rsem, kind, t):
    pltpu.make_async_copy(ref, ref, rsem.at[kind, t]).wait()


def sent(ref, ssem, kind):
    pltpu.make_async_copy(ref, ref, ssem.at[kind]).wait()


def reduce_norm_gather(left_ref, fetch, wbuf, depth, resid_ref, resid_ready, gain_ref, h_ref, mbuf, bufs, ssem, rsem, free, idle_work, gather_work, pre, rest):
    r1, rx, ry, r2x, r2y, ssq = bufs
    _, blocks = seat()
    to_pair, to_x, to_y = blocks[1], blocks[2], blocks[4]
    tiles = mbuf.shape[0]
    rows = mbuf.shape[4]
    low = pl.ds(0, HALF)
    high = pl.ds(HALF, HALF)

    def send(src, dst, kind, t, target):
        pltpu.make_async_remote_copy(
            src_ref=src, dst_ref=dst, send_sem=ssem.at[kind], recv_sem=rsem.at[kind, t], device_id={"tp": target}, device_id_type=MESH
        ).start()

    def scatter_step(j, _):
        @pl.when(j < tiles)
        def _():
            fetch(j).wait()
            for half in range(2):
                cols = pl.ds(half * HALF, HALF)
                part = jnp.dot(left_ref[...].reshape(8 * rows, depth), wbuf[j % 2, pl.ds(0, depth), cols], preferred_element_type=jnp.float32)
                mbuf[j, :, :, :, :, cols] = part.astype(jnp.bfloat16).reshape(2, 2, 2, rows, HALF)

            @pl.when(j + 2 < tiles)
            def _():
                fetch(j + 2).start()

            send(mbuf.at[j, :, :, 1], r1.at[j], PAIR, j, to_pair)
            idle_work(j)

        @pl.when((j >= 1) & (j < tiles + 1))
        def _():
            t = j - 1
            landed(r1.at[t], rsem, PAIR, t)
            mbuf[t, :, :, 0] = mbuf[t, :, :, 0] + r1[t]
            send(mbuf.at[t, :, 1, 0, :, low], rx.at[t], X1, t, to_x)
            send(mbuf.at[t, 1, :, 0, :, high], ry.at[t], Y1, t, to_y)

        @pl.when((j >= 2) & (j < tiles + 2))
        def _():
            t = j - 2
            landed(rx.at[t], rsem, X1, t)
            mbuf[t, :, 0, 0, :, low] = mbuf[t, :, 0, 0, :, low] + rx[t]
            send(mbuf.at[t, 1, 0, 0, :, low], r2y.at[t], Y2, t, to_y)
            landed(ry.at[t], rsem, Y1, t)
            mbuf[t, 0, :, 0, :, high] = mbuf[t, 0, :, 0, :, high] + ry[t]
            send(mbuf.at[t, 0, 1, 0, :, high], r2x.at[t], X2, t, to_x)

        @pl.when(j == 3)
        def _():
            resid_ready()
            ssq[...] = jnp.zeros_like(ssq)

        @pl.when(j >= 3)
        def _():
            t = j - 3
            landed(r2y.at[t], rsem, Y2, t)
            landed(r2x.at[t], rsem, X2, t)
            for cols, other in ((low, r2y), (high, r2x)):
                total = (mbuf[t, 0, 0, 0, :, cols] + other[t]).astype(jnp.float32)
                new = (resid_ref[t, :, cols].astype(jnp.float32) + total).astype(jnp.bfloat16)
                h_ref[t, :, cols] = new
                wide = new.astype(jnp.float32)
                wide = wide * wide
                ssq[...] += sum(wide[:, lane : lane + 128] for lane in range(0, HALF, 128))

        return 0

    lax.fori_loop(0, tiles + 3, scatter_step, 0)
    sent(r1, ssem, PAIR)
    sent(rx, ssem, X1)
    sent(ry, ssem, Y1)
    sent(r2x, ssem, X2)
    sent(r2y, ssem, Y2)
    for target in (to_x, to_y, to_pair):
        pl.semaphore_signal(free, inc=1, device_id={"tp": target}, device_id_type=MESH)
    scale = lax.rsqrt(jnp.sum(ssq[...], axis=-1, keepdims=True) * (1.0 / (tiles * TILE)) + RMS_EPS)
    for t in range(tiles):
        gain = gain_ref[pl.ds(t * TILE, TILE)].reshape(1, TILE).astype(jnp.float32)
        mbuf[t, 0, 0, 0] = (h_ref[t].astype(jnp.float32) * scale * gain).astype(jnp.bfloat16)
    pl.semaphore_wait(free, 3)

    def own(t):
        mine = mbuf.at[t, 0, 0, 0]
        send(mine, mbuf.at[t, 0, 1, 0], GX, t, to_x)
        send(mine, mbuf.at[t, 1, 0, 0], GY, t, to_y)

    own(0)
    own(1)

    def own_pair(t, _):
        send(mbuf.at[t, 0, 0, 0], mbuf.at[t, 0, 0, 1], GP, t, to_pair)
        return 0

    lax.fori_loop(0, tiles, own_pair, 0)
    gather_work()

    def pre_step(t, _):
        landed(mbuf.at[t, 0, 0, 1], rsem, GP, t)
        pre(t)
        return 0

    def gather_step(j, _):
        @pl.when(j < 3)
        def _():
            lax.fori_loop(j * 3 + (j + 2) // 3, j * 3 + 4, pre_step, 0)

        @pl.when(j + 2 < tiles)
        def _():
            own(j + 2)

        @pl.when(j < tiles)
        def _():
            upper = pl.ds(0, rows // 2)
            lower = pl.ds(rows // 2, rows // 2)
            landed(mbuf.at[j, 0, 1, 0], rsem, GX, j)
            send(mbuf.at[j, 0, 1, 0, upper], mbuf.at[j, 1, 1, 0, upper], FY, j, to_y)
            send(mbuf.at[j, 0, 1, 0], mbuf.at[j, 0, 1, 1], PX, j, to_pair)
            landed(mbuf.at[j, 1, 0, 0], rsem, GY, j)
            send(mbuf.at[j, 1, 0, 0, lower], mbuf.at[j, 1, 1, 0, lower], FX, j, to_x)
            send(mbuf.at[j, 1, 0, 0], mbuf.at[j, 1, 0, 1], PY, j, to_pair)

        @pl.when((j >= 1) & (j < tiles + 1))
        def _():
            t = j - 1
            landed(mbuf.at[t, 1, 1, 0, pl.ds(0, rows // 2)], rsem, FY, t)
            landed(mbuf.at[t, 1, 1, 0, pl.ds(rows // 2, rows // 2)], rsem, FX, t)
            send(mbuf.at[t, 1, 1, 0], mbuf.at[t, 1, 1, 1], PD, t, to_pair)

        @pl.when(j >= 2)
        def _():
            t = j - 2
            landed(mbuf.at[t, 0, 1, 1], rsem, PX, t)
            landed(mbuf.at[t, 1, 0, 1], rsem, PY, t)
            landed(mbuf.at[t, 1, 1, 1], rsem, PD, t)
            rest(t)

        return 0

    lax.fori_loop(0, tiles + 2, gather_step, 0)
    for kind in (GX, GY, GP, PX, PY, PD):
        sent(h_ref, ssem, kind)
    for kind in (FX, FY):
        sent(h_ref.at[pl.ds(0, tiles // 2)], ssem, kind)


def tail_kernel(mlp_gain, final_gain, id_ref, att_hbm, hid_hbm, wo_hbm, wg_hbm, wu_hbm, wd_hbm, wl_hbm, norm_ref, prob_ref, mbuf, r1, rx, ry, r2x, r2y, ssq, left, prod, resid, h_buf, wbuf, nbuf, acc, stats, ssem, rsem, wsem, nsem, isem, tsem, usem, free):
    me, blocks = seat()
    tiles = mbuf.shape[0]
    rows = mbuf.shape[4]
    count = 8 * rows
    heads_width = left.shape[2]
    width = wg_hbm.shape[0]
    padded = wbuf.shape[1]
    vocab = wl_hbm.shape[0]
    parts = acc.shape[0]
    side = acc.shape[1]
    piece = pl.cdiv(vocab, parts * 16) * 16
    pieces = [(n * piece, min(piece, vocab - n * piece)) for n in range(parts)]
    others = [(me + i) % 8 for i in range(1, 8)]

    def columns(t):
        return pl.ds(pl.multiple_of(t * TILE, TILE), TILE)

    def fetch_o(t):
        return pltpu.make_async_copy(wo_hbm.at[:, columns(t)], wbuf.at[t % 2, pl.ds(0, heads_width)], wsem.at[t % 2])

    def fetch_d(t):
        return pltpu.make_async_copy(wd_hbm.at[:, columns(t)], wbuf.at[t % 2, pl.ds(0, width)], wsem.at[t % 2])

    def fetch_in(i):
        t = i % tiles
        slot = i % 2
        return (
            pltpu.make_async_copy(wg_hbm.at[:, columns(t)], nbuf.at[slot, pl.ds(0, width)], nsem.at[0, slot]),
            pltpu.make_async_copy(wu_hbm.at[:, columns(t)], nbuf.at[slot, pl.ds(padded, width)], nsem.at[1, slot]),
        )

    def fetch_l(i):
        slot = i % 2
        return (pltpu.make_async_copy(wl_hbm.at[:, columns(i % tiles)], nbuf.at[slot, pl.ds(0, vocab)], nsem.at[0, slot]),)

    fetch_o(0).start()
    for k, block in enumerate(blocks):
        pltpu.make_async_copy(att_hbm.at[pl.ds(pl.multiple_of(block * rows, rows), rows)], left.at[k], isem.at[0]).start()
    fetch_o(1).start()
    barrier = pltpu.get_barrier_semaphore()
    for other in others:
        pl.semaphore_signal(barrier, inc=1, device_id={"tp": other}, device_id_type=MESH)
    pl.semaphore_wait(barrier, 7)
    for t in range(tiles):
        pltpu.make_async_copy(hid_hbm.at[pl.ds(pl.multiple_of(me * rows, rows), rows), pl.ds(t * TILE, TILE)], resid.at[t], isem.at[1]).start()
    pltpu.make_async_copy(left, left, isem.at[0]).wait()

    def resid_ready():
        pltpu.make_async_copy(resid, resid, isem.at[1]).wait()

    def clear(j):
        @pl.when(j < parts)
        def _():
            acc[j] = jnp.zeros(acc.shape[1:], jnp.float32)

    def idle_in(j):
        clear(j)

        @pl.when(j == 4)
        def _():
            for slot in range(2):
                gap = jnp.zeros((padded - width, TILE), jnp.bfloat16)
                wbuf[slot, pl.ds(width, padded - width)] = gap
                nbuf[slot, pl.ds(width, padded - width)] = gap
                nbuf[slot, pl.ds(padded + width, padded - width)] = gap
                for copy in fetch_in(slot):
                    copy.start()

    def gather_in():
        fetch_d(0).start()
        fetch_d(1).start()

    def streamed(fetch, i, work):
        for copy in fetch(i):
            copy.wait()
        work(i % 2)

        @pl.when(i + 2 < 2 * tiles)
        def _():
            for copy in fetch(i + 2):
                copy.start()

    def in_part(slot, left_rows, some):
        for half in range(2):
            for n in range(2):
                wide = min(side, padded - n * side)
                weights = nbuf[slot, pl.ds(half * padded + n * side, wide)]
                acc[half * 2 + n, some, pl.ds(0, wide)] += dot_nt(left_rows, weights)

    def pre_in(t):
        streamed(fetch_in, t, lambda slot: in_part(slot, mbuf[t, 0, 0].reshape(2 * rows, TILE), pl.ds(0, 2 * rows)))

    def rest_in(t):
        def work(slot):
            far = mbuf[t].reshape(8 * rows, TILE)[2 * rows :]
            in_part(slot, far, pl.ds(2 * rows, 6 * rows))

        streamed(fetch_in, t + tiles, work)

    bufs = (r1, rx, ry, r2x, r2y, ssq)
    reduce_norm_gather(left, fetch_o, wbuf, heads_width, resid, resid_ready, mlp_gain, h_buf, mbuf, bufs, ssem.at[0], rsem.at[0], free.at[0], idle_in, gather_in, pre_in, rest_in)

    def finish(n, _):
        cols = pl.ds(pl.multiple_of(n % 4 * 256, 256), 256)
        value = jax.nn.silu(acc[n // 4, :, cols]) * acc[2 + n // 4, :, cols]
        prod[:, pl.ds(pl.multiple_of(n * 256, 256), 256)] = value.astype(jnp.bfloat16)
        return 0

    lax.fori_loop(0, padded // 256, finish, 0)

    def idle_head(j):
        clear(j)

        @pl.when(j == 1)
        def _():
            for slot in range(2):
                for copy in fetch_l(slot):
                    copy.start()

    def head_part(slot, right_rows, some):
        for n, (start, size) in enumerate(pieces):
            acc[n, pl.ds(0, size), some] += dot_nt(nbuf[slot, pl.ds(start, size)], right_rows)

    def pre_head(t):
        streamed(fetch_l, t, lambda slot: head_part(slot, mbuf[t, 0, 0].reshape(2 * rows, TILE), pl.ds(0, 2 * rows)))

    def rest_head(t):
        def work(slot):
            far = mbuf[t].reshape(8 * rows, TILE)[2 * rows :]
            head_part(slot, far, pl.ds(2 * rows, 6 * rows))

        streamed(fetch_l, t + tiles, work)

    reduce_norm_gather(prod, fetch_d, wbuf, padded, h_buf, lambda: None, final_gain, h_buf, mbuf, bufs, ssem.at[1], rsem.at[1], free.at[1], idle_head, lambda: None, pre_head, rest_head)

    best = jnp.full((8, count), -jnp.inf, jnp.float32)
    for n, (start, size) in enumerate(pieces):
        best = jnp.maximum(best, jnp.max(acc[n, pl.ds(0, size)].reshape(size // 8, 8, count), axis=0))
    best = jnp.max(best, axis=0, keepdims=True)
    ids = []
    for block in blocks:
        ids += [id_ref[pl.ds(2 * block, 1)], id_ref[pl.ds(2 * block + 1, 1)]]
    local_id = jnp.concatenate(ids, axis=1) - me * vocab

    total = jnp.zeros((8, count), jnp.float32)
    picked = jnp.zeros((8, count), jnp.float32)
    for n, (start, size) in enumerate(pieces):
        value = acc[n, pl.ds(0, size)]
        hit = lax.broadcasted_iota(jnp.int32, (size, count), 0) + start == local_id
        total = total + jnp.sum(jnp.exp(value - best).reshape(size // 8, 8, count), axis=0)
        picked = picked + jnp.sum(jnp.where(hit, value, 0.0).reshape(size // 8, 8, count), axis=0)
    for i, values in enumerate((best, jnp.sum(total, axis=0, keepdims=True), jnp.sum(picked, axis=0, keepdims=True))):
        for k, block in enumerate(blocks):
            stats[me, i, pl.ds(block, 1)] = values[:, k * rows : (k + 1) * rows]
    copies = []
    for i, other in enumerate(others):
        copy = pltpu.make_async_remote_copy(
            src_ref=stats.at[me], dst_ref=stats.at[me], send_sem=tsem.at[i], recv_sem=usem.at[i], device_id={"tp": other}, device_id_type=MESH
        )
        copy.start()
        copies.append(copy)
    for copy in copies:
        copy.wait()
    top = stats[0, 0]
    for d in range(1, 8):
        top = jnp.maximum(top, stats[d, 0])
    whole = jnp.zeros_like(top)
    score = jnp.zeros_like(top)
    for d in range(8):
        whole = whole + stats[d, 1] * jnp.exp(stats[d, 0] - top)
        score = score + stats[d, 2]
    norm = top + jnp.log(whole)
    for ref, values in ((norm_ref, norm), (prob_ref, score - norm)):
        nodes = ref.shape[1]
        for i in range(ref.shape[0]):
            start = i * nodes
            ref[i : i + 1] = values[start // 128 : start // 128 + 1, start % 128 : start % 128 + nodes]


def tail_stage(mlp_gain, final_gain, score_id, attended, hidden, w_o, gate_t, up_t, w_down, head_t):
    count, dim = hidden.shape
    tiles = dim // TILE
    rows = count // 8
    padded = pl.cdiv(gate_t.shape[0], 256) * 256
    vocab = head_t.shape[0]
    vmem = pl.BlockSpec(memory_space=pltpu.VMEM)
    anywhere = pl.BlockSpec(memory_space=pl.ANY)
    bf16 = jnp.bfloat16
    return pl.pallas_call(
        tail_kernel,
        in_specs=[vmem] * 3 + [anywhere] * 7,
        out_specs=[vmem, vmem],
        out_shape=[jax.ShapeDtypeStruct(score_id.shape, jnp.float32)] * 2,
        scratch_shapes=[
            pltpu.VMEM((tiles, 2, 2, 2, rows, TILE), bf16),
            pltpu.VMEM((tiles, 2, 2, rows, TILE), bf16),
            pltpu.VMEM((tiles, 2, rows, HALF), bf16),
            pltpu.VMEM((tiles, 2, rows, HALF), bf16),
            pltpu.VMEM((tiles, rows, HALF), bf16),
            pltpu.VMEM((tiles, rows, HALF), bf16),
            pltpu.VMEM((rows, 128), jnp.float32),
            pltpu.VMEM((8, rows, w_o.shape[0]), bf16),
            pltpu.VMEM((count, padded), bf16),
            pltpu.VMEM((tiles, rows, TILE), bf16),
            pltpu.VMEM((tiles, rows, TILE), bf16),
            pltpu.VMEM((2, padded, TILE), bf16),
            pltpu.VMEM((2, max(2 * padded, vocab), TILE), bf16),
            pltpu.VMEM((4, 1024, count), jnp.float32),
            pltpu.VMEM((8, 3, 8, count // 8), jnp.float32),
            pltpu.SemaphoreType.DMA((2, 13)),
            pltpu.SemaphoreType.DMA((2, 13, tiles)),
            pltpu.SemaphoreType.DMA((2,)),
            pltpu.SemaphoreType.DMA((2, 2)),
            pltpu.SemaphoreType.DMA((2,)),
            pltpu.SemaphoreType.DMA((7,)),
            pltpu.SemaphoreType.DMA((7,)),
            pltpu.SemaphoreType.REGULAR((2,)),
        ],
        compiler_params=pltpu.CompilerParams(collective_id=1, has_side_effects=True, vmem_limit_bytes=VMEM_MAX),
        name="tail_stage",
    )(mlp_gain, final_gain, score_id, attended, hidden, w_o, gate_t, up_t, w_down, head_t)


def rope_tables(positions, head_dim):
    half = head_dim // 2
    lane = jnp.arange(head_dim, dtype=jnp.int32)
    inv_freq = 1.0 / (ROPE_THETA ** ((lane % half).astype(jnp.float32) * (2.0 / head_dim)))
    angles = positions.astype(jnp.float32)[:, None] * inv_freq
    return jnp.cos(angles), jnp.sin(angles) * jnp.where(lane < half, -1.0, 1.0)


def solution(mesh):
    def group_step(hidden, tree_mask, depth, ctx_len, block_table, score_id, k_cache, v_cache, attn_norm, w_q, w_k, w_v, w_o, mlp_norm, w_gate, w_up, w_down, final_norm, w_lm):
        requests, nodes, dim = hidden.shape
        head_dim = k_cache.shape[3]
        rows = requests * nodes
        flat = hidden.reshape(rows, dim)
        cosine, sine = rope_tables((ctx_len[:, None] + depth).reshape(rows), head_dim)
        query, key_new, val_new = project(flat, attn_norm, cosine, sine, w_q, w_k, w_v, requests, nodes, head_dim, 4)
        attended, k_out, v_out = attend(
            block_table, ctx_len, query, key_new, val_new, tree_mask, jnp.transpose(k_cache, (0, 2, 1, 3)), jnp.transpose(v_cache, (0, 2, 1, 3))
        )
        k_out = jnp.transpose(k_out, (0, 2, 1, 3))
        v_out = jnp.transpose(v_out, (0, 2, 1, 3))

        log_norm, log_prob = tail_stage(mlp_norm, final_norm, score_id, attended, flat, w_o, w_gate.T, w_up.T, w_down, w_lm.T)
        return log_norm.reshape(requests, nodes), log_prob.reshape(requests, nodes), k_out, v_out

    request_spec = P("dp", None, None)
    node_spec = P("dp", None)
    cache_spec = P("dp", None, "tp", None)
    shared_spec = P(None)
    column_spec = P(None, "tp")
    row_spec = P("tp", None)
    in_specs = (request_spec, request_spec, node_spec, P("dp"), node_spec, node_spec, cache_spec, cache_spec, shared_spec, column_spec, column_spec, column_spec, row_spec, shared_spec, column_spec, column_spec, row_spec, shared_spec, column_spec)
    out_specs = (node_spec, node_spec, cache_spec, cache_spec)
    return jax.shard_map(group_step, mesh=mesh, in_specs=in_specs, out_specs=out_specs, check_vma=False)
```

```python
import jax
import jax.numpy as jnp
from jax import lax
from jax.experimental import pallas as pl
from jax.experimental.pallas import tpu as pltpu
from jax.sharding import PartitionSpec as P

RMS_EPS = 1e-5
ROPE_THETA = 500000
MESH = pl.DeviceIdType.MESH
NT_DIMS = (((1,), (1,)), ((), ()))
VMEM_MAX = 67043328


def dot_nt(left, right):
    return lax.dot_general(left, right, NT_DIMS, preferred_element_type=jnp.float32)


def qkv_kernel(hid_ref, gain_ref, cos_ref, sin_ref, wq_ref, wk_ref, wv_ref, q_ref, k_ref, v_ref):
    requests, heads, nodes, head_dim = q_ref.shape
    widened = hid_ref[...].astype(jnp.float32)
    scale = lax.rsqrt(jnp.mean(widened * widened, axis=-1, keepdims=True) + RMS_EPS)
    gain = gain_ref[...].reshape(1, widened.shape[1]).astype(jnp.float32)
    normed = (widened * scale * gain).astype(jnp.bfloat16)
    cosine = cos_ref[...]
    sine = sin_ref[...]

    def put(out_ref, weight_ref, turned):
        product = jnp.dot(normed, weight_ref[...], preferred_element_type=jnp.float32)
        for h in range(heads):
            part = product[:, h * head_dim : (h + 1) * head_dim]
            if turned:
                part = part * cosine + pltpu.roll(part, head_dim // 2, 1) * sine
            out_ref[:, h] = part.astype(jnp.bfloat16).reshape(requests, nodes, head_dim)

    put(q_ref, wq_ref, True)
    put(k_ref, wk_ref, True)
    put(v_ref, wv_ref, False)


def project(hidden, gain, cosine, sine, w_q, w_k, w_v, requests, nodes, head_dim, group):
    rows, dim = hidden.shape
    cols = w_q.shape[1]
    heads = cols // head_dim
    block = group * nodes
    full = pl.BlockSpec((dim, cols), lambda i: (0, 0), pipeline_mode=pl.Buffered(1))
    out = pl.BlockSpec((group, heads, nodes, head_dim), lambda i: (i, 0, 0, 0))
    shape = jax.ShapeDtypeStruct((requests, heads, nodes, head_dim), jnp.bfloat16)
    return pl.pallas_call(
        qkv_kernel,
        grid=(rows // block,),
        in_specs=[
            pl.BlockSpec((block, dim), lambda i: (i, 0)),
            pl.BlockSpec((dim,), lambda i: (0,)),
            pl.BlockSpec((block, head_dim), lambda i: (i, 0)),
            pl.BlockSpec((block, head_dim), lambda i: (i, 0)),
            full,
            full,
            full,
        ],
        out_specs=[out, out, out],
        out_shape=[shape, shape, shape],
        compiler_params=pltpu.CompilerParams(vmem_limit_bytes=VMEM_MAX),
        name="project",
    )(hidden, gain, cosine, sine, w_q, w_k, w_v)


def attend_kernel(table_ref, ctx_ref, q_ref, kn_ref, vn_ref, mask_ref, kc_ref, vc_ref, out_ref, ko_ref, vo_ref, kbuf, vbuf, rsem, wsem):
    b = pl.program_id(0)
    count = pl.num_programs(0)
    pages, heads, page, head_dim = kbuf.shape[1:]
    span = pages * page
    nodes = q_ref.shape[2]
    window = nodes + page

    def load(i, slot):
        for s in range(pages):
            block = table_ref[i, s]
            pltpu.make_async_copy(kc_ref.at[block], kbuf.at[slot, s], rsem.at[0, slot]).start()
            pltpu.make_async_copy(vc_ref.at[block], vbuf.at[slot, s], rsem.at[1, slot]).start()

    def save(i, slot):
        for s in range(pages):
            block = table_ref[i, s]
            pltpu.make_async_copy(kbuf.at[slot, s], ko_ref.at[block], wsem.at[0, slot]).start()
            pltpu.make_async_copy(vbuf.at[slot, s], vo_ref.at[block], wsem.at[1, slot]).start()

    def whole(slot, sem):
        pltpu.make_async_copy(kbuf.at[slot], kbuf.at[slot], sem.at[0, slot]).wait()
        pltpu.make_async_copy(vbuf.at[slot], vbuf.at[slot], sem.at[1, slot]).wait()

    slot = lax.rem(b, 3)
    after = lax.rem(b + 1, 3)

    @pl.when(b == 0)
    def _():
        load(0, 0)

    @pl.when(b >= 2)
    def _():
        whole(after, wsem)

    whole(slot, rsem)
    load(jnp.minimum(b + 1, count - 1), after)
    ctx = ctx_ref[b]
    first = jnp.minimum(ctx // page, pages - window // page)
    base = first * page
    row = base + lax.broadcasted_iota(jnp.int32, (window, nodes), 0)
    node = ctx + lax.broadcasted_iota(jnp.int32, (window, nodes), 1)
    place = jnp.where(row == node, 1.0, 0.0).astype(jnp.bfloat16)
    slot_id = base + lax.broadcasted_iota(jnp.int32, (window, head_dim), 0)
    fresh = (slot_id >= ctx) & (slot_id < ctx + nodes)
    for buf, new_ref in ((kbuf, kn_ref), (vbuf, vn_ref)):
        moved = [jnp.dot(place, new_ref[0, h], preferred_element_type=jnp.float32) for h in range(heads)]
        for h in range(heads):
            for i in range(window // page):
                rows = slice(i * page, (i + 1) * page)
                old = buf[slot, first + i, h].astype(jnp.float32)
                buf[slot, first + i, h] = jnp.where(fresh[rows], moved[h][rows], old).astype(jnp.bfloat16)
    save(b, slot)
    spread = jnp.where(
        ctx + lax.broadcasted_iota(jnp.int32, (nodes, span), 0) == lax.broadcasted_iota(jnp.int32, (nodes, span), 1), 1.0, 0.0
    ).astype(jnp.bfloat16)
    linked = jnp.where(mask_ref[0] > 0, 1.0, 0.0).astype(jnp.bfloat16)
    seen_new = jnp.dot(linked, spread, preferred_element_type=jnp.float32) > 0.5
    seen = seen_new | (lax.broadcasted_iota(jnp.int32, (nodes, span), 1) < ctx)
    scale = head_dim**-0.5
    scores = [dot_nt(q_ref[0, h], kbuf[slot, :, h].reshape(span, head_dim)) for h in range(heads)]
    scores = [jnp.where(seen, score * scale, -jnp.inf) for score in scores]
    tops = [jnp.max(score, axis=-1, keepdims=True) for score in scores]
    probs = [jnp.exp(score - top) for score, top in zip(scores, tops)]
    totals = [jnp.sum(prob, axis=-1, keepdims=True) for prob in probs]
    mixed = [
        jnp.dot(prob.astype(jnp.bfloat16), vbuf[slot, :, h].reshape(span, head_dim), preferred_element_type=jnp.float32)
        for h, prob in enumerate(probs)
    ]
    for h in range(heads):
        out_ref[:, h * head_dim : (h + 1) * head_dim] = (mixed[h] / totals[h]).astype(jnp.bfloat16)

    @pl.when(b == count - 1)
    def _():
        whole(lax.rem(b + 2, 3), wsem)
        whole(slot, wsem)
        whole(after, rsem)


def attend(table, ctx_len, query, key_new, val_new, tree_mask, k_cache, v_cache):
    requests, heads, nodes, head_dim = query.shape
    page = k_cache.shape[2]
    pages = table.shape[1]
    node_spec = pl.BlockSpec((1, heads, nodes, head_dim), lambda b, *_: (b, 0, 0, 0))
    anywhere = pl.BlockSpec(memory_space=pl.ANY)
    return pl.pallas_call(
        attend_kernel,
        grid_spec=pltpu.PrefetchScalarGridSpec(
            num_scalar_prefetch=2,
            grid=(requests,),
            in_specs=[
                node_spec,
                node_spec,
                node_spec,
                pl.BlockSpec((1, nodes, nodes), lambda b, *_: (b, 0, 0)),
                anywhere,
                anywhere,
            ],
            out_specs=[pl.BlockSpec((nodes, heads * head_dim), lambda b, *_: (b, 0)), anywhere, anywhere],
            scratch_shapes=[
                pltpu.VMEM((3, pages, heads, page, head_dim), jnp.bfloat16),
                pltpu.VMEM((3, pages, heads, page, head_dim), jnp.bfloat16),
                pltpu.SemaphoreType.DMA((2, 3)),
                pltpu.SemaphoreType.DMA((2, 3)),
            ],
        ),
        out_shape=[
            jax.ShapeDtypeStruct((requests * nodes, heads * head_dim), jnp.bfloat16),
            jax.ShapeDtypeStruct(k_cache.shape, k_cache.dtype),
            jax.ShapeDtypeStruct(v_cache.shape, v_cache.dtype),
        ],
        name="attend",
    )(table, ctx_len, query, key_new, val_new, tree_mask, k_cache, v_cache)


TILE = 512
HALF = TILE // 2
PAIR, X1, Y1, X2, Y2, GX, GY, GP, FX, FY, PX, PY, PD = range(13)


def seat():
    me = lax.axis_index("tp")
    core = me % 2
    x = (me // 2) % 2
    y = me // 4
    blocks = []
    for dy in range(2):
        for dx in range(2):
            for dc in range(2):
                blocks.append((1 - y if dy else y) * 4 + (1 - x if dx else x) * 2 + (1 - core if dc else core))
    return me, blocks


class Exchange:
    def __init__(self, left, fetch, wbuf, depth, resid, gain, h_buf, mbuf, bufs, ssem, rsem, free, scatter_work, gather_work, compute):
        self.left, self.fetch, self.wbuf, self.depth = left, fetch, wbuf, depth
        self.resid, self.gain, self.h_buf, self.mbuf = resid, gain, h_buf, mbuf
        self.r1, self.rx, self.ry, self.r2x, self.r2y, self.ssq = bufs
        self.ssem, self.rsem, self.free = ssem, rsem, free
        self.scatter_work, self.gather_work, self.compute = scatter_work, gather_work, compute
        _, blocks = seat()
        self.to_pair, self.to_x, self.to_y = blocks[1], blocks[2], blocks[4]
        self.steps = mbuf.shape[0]
        self.tiles = self.steps // 2
        self.rows = mbuf.shape[4]

    def send(self, src, dst, kind, i, target):
        pltpu.make_async_remote_copy(
            src_ref=src,
            dst_ref=dst,
            send_sem=self.ssem.at[i // self.tiles, kind],
            recv_sem=self.rsem.at[kind, i],
            device_id={"tp": target},
            device_id_type=MESH,
        ).start()

    def landed(self, ref, kind, i):
        pltpu.make_async_copy(ref, ref, self.rsem.at[kind, i]).wait()

    def sent(self, ref, kind, h):
        pltpu.make_async_copy(ref, ref, self.ssem.at[h, kind]).wait()

    def scatter_step(self, i):
        mbuf, steps, rows = self.mbuf, self.steps, self.rows
        low = pl.ds(0, HALF)
        high = pl.ds(HALF, HALF)

        @pl.when(i < steps)
        def _():
            self.fetch(i).wait()
            left = self.left[i // self.tiles].reshape(8 * rows, self.depth)
            part = jnp.dot(left, self.wbuf[i % 2, pl.ds(0, self.depth)], preferred_element_type=jnp.float32)
            mbuf[i] = part.astype(jnp.bfloat16).reshape(2, 2, 2, rows, TILE)

            @pl.when(i + 2 < steps)
            def _():
                self.fetch(i + 2).start()

            self.send(mbuf.at[i, :, :, 1], self.r1.at[i], PAIR, i, self.to_pair)

        @pl.when((i >= 1) & (i < steps + 1))
        def _():
            t = i - 1
            self.landed(self.r1.at[t], PAIR, t)
            mbuf[t, :, :, 0] = mbuf[t, :, :, 0] + self.r1[t]
            self.send(mbuf.at[t, :, 1, 0, :, low], self.rx.at[t], X1, t, self.to_x)
            self.send(mbuf.at[t, 1, :, 0, :, high], self.ry.at[t], Y1, t, self.to_y)

        @pl.when((i >= 3) & (i < steps + 3))
        def _():
            t = i - 3
            self.landed(self.rx.at[t], X1, t)
            mbuf[t, :, 0, 0, :, low] = mbuf[t, :, 0, 0, :, low] + self.rx[t]
            self.send(mbuf.at[t, 1, 0, 0, :, low], self.r2y.at[t], Y2, t, self.to_y)
            self.landed(self.ry.at[t], Y1, t)
            mbuf[t, 0, :, 0, :, high] = mbuf[t, 0, :, 0, :, high] + self.ry[t]
            self.send(mbuf.at[t, 0, 1, 0, :, high], self.r2x.at[t], X2, t, self.to_x)

        @pl.when(i >= 5)
        def _():
            t = i - 5
            h = t // self.tiles
            self.landed(self.r2y.at[t], Y2, t)
            self.landed(self.r2x.at[t], X2, t)
            for cols, other in ((low, self.r2y), (high, self.r2x)):
                total = (mbuf[t, 0, 0, 0, :, cols] + other[t]).astype(jnp.float32)
                new = (self.resid[t, :, cols].astype(jnp.float32) + total).astype(jnp.bfloat16)
                self.h_buf[t, :, cols] = new
                wide = new.astype(jnp.float32)
                wide = wide * wide
                self.ssq[h] += sum(wide[:, lane : lane + 128] for lane in range(0, HALF, 128))

        @pl.when(i == self.tiles + 5)
        def _():
            self.norm(0)

        @pl.when(i == steps + 1)
        def _():
            self.open(0)

        self.scatter_work(i)

    def norm(self, h):
        tiles = self.tiles
        part = pl.ds(h * tiles, tiles)
        self.sent(self.r1.at[part], PAIR, h)
        self.sent(self.rx.at[part], X1, h)
        self.sent(self.ry.at[part], Y1, h)
        self.sent(self.r2x.at[part], X2, h)
        self.sent(self.r2y.at[part], Y2, h)
        for target in (self.to_x, self.to_y, self.to_pair):
            pl.semaphore_signal(self.free.at[h], inc=1, device_id={"tp": target}, device_id_type=MESH)
        scale = lax.rsqrt(jnp.sum(self.ssq[h], axis=-1, keepdims=True) * (1.0 / (tiles * TILE)) + RMS_EPS)
        for t in range(tiles):
            gain = self.gain[pl.ds(t * TILE, TILE)].reshape(1, TILE).astype(jnp.float32)
            i = h * tiles + t
            self.mbuf[i, 0, 0, 0] = (self.h_buf[i].astype(jnp.float32) * scale * gain).astype(jnp.bfloat16)

    def own(self, i):
        mine = self.mbuf.at[i, 0, 0, 0]
        self.send(mine, self.mbuf.at[i, 0, 1, 0], GX, i, self.to_x)
        self.send(mine, self.mbuf.at[i, 1, 0, 0], GY, i, self.to_y)
        self.send(mine, self.mbuf.at[i, 0, 0, 1], GP, i, self.to_pair)

    def open(self, h):
        pl.semaphore_wait(self.free.at[h], 3)
        if h == 0:
            for i in range(2):
                self.own(i)

    def gather_step(self, i):
        mbuf, steps, rows = self.mbuf, self.steps, self.rows
        upper = pl.ds(0, rows // 2)
        lower = pl.ds(rows // 2, rows // 2)

        @pl.when(i == 6)
        def _():
            self.open(1)

        @pl.when(i < steps)
        def _():
            self.landed(mbuf.at[i, 0, 1, 0], GX, i)
            self.send(mbuf.at[i, 0, 1, 0, upper], mbuf.at[i, 1, 1, 0, upper], FY, i, self.to_y)
            self.send(mbuf.at[i, 0, 1, 0], mbuf.at[i, 0, 1, 1], PX, i, self.to_pair)
            self.landed(mbuf.at[i, 1, 0, 0], GY, i)
            self.send(mbuf.at[i, 1, 0, 0, lower], mbuf.at[i, 1, 1, 0, lower], FX, i, self.to_x)
            self.send(mbuf.at[i, 1, 0, 0], mbuf.at[i, 1, 0, 1], PY, i, self.to_pair)

        @pl.when(i + 2 < steps)
        def _():
            self.own(i + 2)

        @pl.when((i >= 2) & (i < steps + 2))
        def _():
            t = i - 2
            self.landed(mbuf.at[t, 1, 1, 0, upper], FY, t)
            self.landed(mbuf.at[t, 1, 1, 0, lower], FX, t)
            self.send(mbuf.at[t, 1, 1, 0], mbuf.at[t, 1, 1, 1], PD, t, self.to_pair)

        self.gather_work(i)

        @pl.when(i >= 3)
        def _():
            t = i - 3
            self.landed(mbuf.at[t, 0, 0, 1], GP, t)
            self.landed(mbuf.at[t, 0, 1, 1], PX, t)
            self.landed(mbuf.at[t, 1, 0, 1], PY, t)
            self.landed(mbuf.at[t, 1, 1, 1], PD, t)
            self.compute(t)

    def close(self, h):
        part = pl.ds(h * self.tiles, self.tiles)
        for kind in (GX, GY, GP, PX, PY, PD):
            self.sent(self.h_buf.at[part], kind, h)
        half = pl.ds(h * self.tiles, self.tiles // 2)
        for kind in (FX, FY):
            self.sent(self.h_buf.at[half], kind, h)


def loop(start, stop, step):
    def body(i, _):
        step(i)
        return 0

    lax.fori_loop(start, stop, body, 0)


def tail_kernel(mlp_gain, final_gain, id_ref, att_hbm, hid_hbm, wo_hbm, wg_hbm, wu_hbm, wd_hbm, wl_hbm, norm_ref, prob_ref, mbuf, r1, rx, ry, r2x, r2y, ssq, left, prod, resid, h_buf, wbuf, nbuf, acc, stats, ssem, rsem, wsem, nsem, isem, tsem, usem, free):
    me, blocks = seat()
    steps = mbuf.shape[0]
    tiles = steps // 2
    rows = mbuf.shape[4]
    half = 8 * rows
    count = 2 * half
    heads_width = left.shape[3]
    width = wg_hbm.shape[0]
    padded = wbuf.shape[1]
    vocab = wl_hbm.shape[0]
    parts = acc.shape[0]
    side = acc.shape[1]
    piece = pl.cdiv(vocab, parts * 16) * 16
    pieces = [(n * piece, min(piece, vocab - n * piece)) for n in range(parts)]
    others = [(me + i) % 8 for i in range(1, 8)]

    def columns(i):
        return pl.ds(pl.multiple_of(i % tiles * TILE, TILE), TILE)

    def fetch_o(i):
        return pltpu.make_async_copy(wo_hbm.at[:, columns(i)], wbuf.at[i % 2, pl.ds(0, heads_width)], wsem.at[i % 2])

    def fetch_d(i):
        return pltpu.make_async_copy(wd_hbm.at[:, columns(i)], wbuf.at[i % 2, pl.ds(0, width)], wsem.at[i % 2])

    def fetch_in(i):
        slot = i % 2
        return (
            pltpu.make_async_copy(wg_hbm.at[:, columns(i)], nbuf.at[slot, pl.ds(0, width)], nsem.at[0, slot]),
            pltpu.make_async_copy(wu_hbm.at[:, columns(i)], nbuf.at[slot, pl.ds(padded, width)], nsem.at[1, slot]),
        )

    def fetch_l(i):
        slot = i % 2
        return (pltpu.make_async_copy(wl_hbm.at[:, columns(i)], nbuf.at[slot, pl.ds(0, vocab)], nsem.at[0, slot]),)

    fetch_o(0).start()
    for h in range(2):
        for k, block in enumerate(blocks):
            source = pl.ds(pl.multiple_of(block * 2 * rows + h * rows, rows), rows)
            pltpu.make_async_copy(att_hbm.at[source], left.at[h, k], isem.at[0]).start()
    fetch_o(1).start()
    barrier = pltpu.get_barrier_semaphore()
    for other in others:
        pl.semaphore_signal(barrier, inc=1, device_id={"tp": other}, device_id_type=MESH)
    pl.semaphore_wait(barrier, 7)
    for i in range(steps):
        source = pl.ds(pl.multiple_of(me * 2 * rows + i // tiles * rows, rows), rows)
        pltpu.make_async_copy(hid_hbm.at[source, pl.ds(i % tiles * TILE, TILE)], resid.at[i], isem.at[1]).start()
    pltpu.make_async_copy(left, left, isem.at[0]).wait()
    ssq[...] = jnp.zeros_like(ssq)

    def clear(n):
        acc[n] = jnp.zeros(acc.shape[1:], jnp.float32)

    def finish(h):
        some = pl.ds(h * half, half)

        def one(n):
            cols = pl.ds(pl.multiple_of(n % 4 * 256, 256), 256)
            value = jax.nn.silu(acc[n // 4, some, cols]) * acc[2 + n // 4, some, cols]
            prod[h, :, pl.ds(pl.multiple_of(n * 256, 256), 256)] = value.astype(jnp.bfloat16)

        loop(0, padded // 256, one)

    def streamed(fetch, i, work):
        for copy in fetch(i):
            copy.wait()
        work(i % 2, pl.ds(pl.multiple_of(i // tiles * half, half), half))

        @pl.when(i + 2 < steps)
        def _():
            for copy in fetch(i + 2):
                copy.start()

    def work_one(i):
        @pl.when(i < parts)
        def _():
            clear(i)

        @pl.when(i == 4)
        def _():
            pltpu.make_async_copy(resid, resid, isem.at[1]).wait()
            for slot in range(2):
                gap = jnp.zeros((padded - width, TILE), jnp.bfloat16)
                wbuf[slot, pl.ds(width, padded - width)] = gap
                nbuf[slot, pl.ds(width, padded - width)] = gap
                nbuf[slot, pl.ds(padded + width, padded - width)] = gap
                for copy in fetch_in(slot):
                    copy.start()

    def compute_in(i):
        def work(slot, some):
            left_rows = mbuf[i].reshape(half, TILE)
            for which in range(2):
                for n in range(2):
                    wide = min(side, padded - n * side)
                    weights = nbuf[slot, pl.ds(which * padded + n * side, wide)]
                    acc[which * 2 + n, some, pl.ds(0, wide)] += dot_nt(left_rows, weights)

        streamed(fetch_in, i, work)

    def between(i):
        @pl.when(i == 0)
        def _():
            first.norm(1)
            fetch_d(0).start()
            fetch_d(1).start()
            ssq[...] = jnp.zeros_like(ssq)

        @pl.when(i == 13)
        def _():
            finish(0)

        @pl.when(i == 15)
        def _():
            first.close(0)

        @pl.when(i >= steps)
        def _():
            second.scatter_step(i - steps)

    def work_two(i):
        @pl.when(i == 3)
        def _():
            finish(1)
            first.close(1)
            for slot in range(2):
                for copy in fetch_l(slot):
                    copy.start()

        @pl.when((i >= 4) & (i < 4 + parts))
        def _():
            clear(i - 4)

    def compute_head(i):
        def work(slot, some):
            right_rows = mbuf[i].reshape(half, TILE)
            for n, (start, size) in enumerate(pieces):
                acc[n, pl.ds(0, size), some] += dot_nt(nbuf[slot, pl.ds(start, size)], right_rows)

        streamed(fetch_l, i, work)

    def last(i):
        @pl.when(i == 0)
        def _():
            second.norm(1)

    bufs = (r1, rx, ry, r2x, r2y, ssq)
    first = Exchange(left, fetch_o, wbuf, heads_width, resid, mlp_gain, h_buf, mbuf, bufs, ssem, rsem, free.at[0], work_one, between, compute_in)
    second = Exchange(prod, fetch_d, wbuf, padded, h_buf, final_gain, h_buf, mbuf, bufs, ssem, rsem, free.at[1], work_two, last, compute_head)
    loop(0, steps + 5, first.scatter_step)
    loop(0, steps + 3, first.gather_step)
    loop(3, steps + 5, second.scatter_step)
    loop(0, steps + 3, second.gather_step)
    second.close(0)
    second.close(1)

    best = jnp.full((8, count), -jnp.inf, jnp.float32)
    for n, (start, size) in enumerate(pieces):
        best = jnp.maximum(best, jnp.max(acc[n, pl.ds(0, size)].reshape(size // 8, 8, count), axis=0))
    best = jnp.max(best, axis=0, keepdims=True)
    ids = [id_ref[pl.ds(2 * block + h, 1)] for h in range(2) for block in blocks]
    local_id = jnp.concatenate(ids, axis=1) - me * vocab
    total = jnp.zeros((8, count), jnp.float32)
    picked = jnp.zeros((8, count), jnp.float32)
    for n, (start, size) in enumerate(pieces):
        value = acc[n, pl.ds(0, size)]
        hit = lax.broadcasted_iota(jnp.int32, (size, count), 0) + start == local_id
        total = total + jnp.sum(jnp.exp(value - best).reshape(size // 8, 8, count), axis=0)
        picked = picked + jnp.sum(jnp.where(hit, value, 0.0).reshape(size // 8, 8, count), axis=0)
    for n, values in enumerate((best, jnp.sum(total, axis=0, keepdims=True), jnp.sum(picked, axis=0, keepdims=True))):
        for h in range(2):
            for k, block in enumerate(blocks):
                start = h * half + k * rows
                stats[me, n, pl.ds(2 * block + h, 1)] = values[:, start : start + rows]
    copies = []
    for i, other in enumerate(others):
        copy = pltpu.make_async_remote_copy(
            src_ref=stats.at[me], dst_ref=stats.at[me], send_sem=tsem.at[i], recv_sem=usem.at[i], device_id={"tp": other}, device_id_type=MESH
        )
        copy.start()
        copies.append(copy)
    for copy in copies:
        copy.wait()
    top = stats[0, 0]
    for d in range(1, 8):
        top = jnp.maximum(top, stats[d, 0])
    whole = jnp.zeros_like(top)
    score = jnp.zeros_like(top)
    for d in range(8):
        whole = whole + stats[d, 1] * jnp.exp(stats[d, 0] - top)
        score = score + stats[d, 2]
    norm = top + jnp.log(whole)
    norm_ref[...] = norm
    prob_ref[...] = score - norm


def tail_stage(mlp_gain, final_gain, score_id, attended, hidden, w_o, gate_t, up_t, w_down, head_t):
    count, dim = hidden.shape
    steps = 2 * dim // TILE
    rows = count // 16
    padded = pl.cdiv(gate_t.shape[0], 256) * 256
    vocab = head_t.shape[0]
    vmem = pl.BlockSpec(memory_space=pltpu.VMEM)
    anywhere = pl.BlockSpec(memory_space=pl.ANY)
    bf16 = jnp.bfloat16
    return pl.pallas_call(
        tail_kernel,
        in_specs=[vmem] * 3 + [anywhere] * 7,
        out_specs=[vmem, vmem],
        out_shape=[jax.ShapeDtypeStruct(score_id.shape, jnp.float32)] * 2,
        scratch_shapes=[
            pltpu.VMEM((steps, 2, 2, 2, rows, TILE), bf16),
            pltpu.VMEM((steps, 2, 2, rows, TILE), bf16),
            pltpu.VMEM((steps, 2, rows, HALF), bf16),
            pltpu.VMEM((steps, 2, rows, HALF), bf16),
            pltpu.VMEM((steps, rows, HALF), bf16),
            pltpu.VMEM((steps, rows, HALF), bf16),
            pltpu.VMEM((2, rows, 128), jnp.float32),
            pltpu.VMEM((2, 8, rows, w_o.shape[0]), bf16),
            pltpu.VMEM((2, 8 * rows, padded), bf16),
            pltpu.VMEM((steps, rows, TILE), bf16),
            pltpu.VMEM((steps, rows, TILE), bf16),
            pltpu.VMEM((2, padded, TILE), bf16),
            pltpu.VMEM((2, max(2 * padded, vocab), TILE), bf16),
            pltpu.VMEM((4, 1024, count), jnp.float32),
            pltpu.VMEM((8, 3) + score_id.shape, jnp.float32),
            pltpu.SemaphoreType.DMA((2, 13)),
            pltpu.SemaphoreType.DMA((13, steps)),
            pltpu.SemaphoreType.DMA((2,)),
            pltpu.SemaphoreType.DMA((2, 2)),
            pltpu.SemaphoreType.DMA((2,)),
            pltpu.SemaphoreType.DMA((7,)),
            pltpu.SemaphoreType.DMA((7,)),
            pltpu.SemaphoreType.REGULAR((2, 2)),
        ],
        compiler_params=pltpu.CompilerParams(collective_id=1, has_side_effects=True, vmem_limit_bytes=VMEM_MAX),
        name="tail_stage",
    )(mlp_gain, final_gain, score_id, attended, hidden, w_o, gate_t, up_t, w_down, head_t)


def rope_tables(positions, head_dim):
    half = head_dim // 2
    lane = jnp.arange(head_dim, dtype=jnp.int32)
    inv_freq = 1.0 / (ROPE_THETA ** ((lane % half).astype(jnp.float32) * (2.0 / head_dim)))
    angles = positions.astype(jnp.float32)[:, None] * inv_freq
    return jnp.cos(angles), jnp.sin(angles) * jnp.where(lane < half, -1.0, 1.0)


def solution(mesh):
    def group_step(hidden, tree_mask, depth, ctx_len, block_table, score_id, k_cache, v_cache, attn_norm, w_q, w_k, w_v, w_o, mlp_norm, w_gate, w_up, w_down, final_norm, w_lm):
        requests, nodes, dim = hidden.shape
        head_dim = k_cache.shape[3]
        rows = requests * nodes
        flat = hidden.reshape(rows, dim)
        cosine, sine = rope_tables((ctx_len[:, None] + depth).reshape(rows), head_dim)
        query, key_new, val_new = project(flat, attn_norm, cosine, sine, w_q, w_k, w_v, requests, nodes, head_dim, 4)
        attended, k_out, v_out = attend(
            block_table, ctx_len, query, key_new, val_new, tree_mask, jnp.transpose(k_cache, (0, 2, 1, 3)), jnp.transpose(v_cache, (0, 2, 1, 3))
        )
        k_out = jnp.transpose(k_out, (0, 2, 1, 3))
        v_out = jnp.transpose(v_out, (0, 2, 1, 3))

        log_norm, log_prob = tail_stage(mlp_norm, final_norm, score_id, attended, flat, w_o, w_gate.T, w_up.T, w_down, w_lm.T)
        return log_norm.reshape(requests, nodes), log_prob.reshape(requests, nodes), k_out, v_out

    request_spec = P("dp", None, None)
    node_spec = P("dp", None)
    cache_spec = P("dp", None, "tp", None)
    shared_spec = P(None)
    column_spec = P(None, "tp")
    row_spec = P("tp", None)
    in_specs = (request_spec, request_spec, node_spec, P("dp"), node_spec, node_spec, cache_spec, cache_spec, shared_spec, column_spec, column_spec, column_spec, row_spec, shared_spec, column_spec, column_spec, row_spec, shared_spec, column_spec)
    out_specs = (node_spec, node_spec, cache_spec, cache_spec)
    return jax.shard_map(group_step, mesh=mesh, in_specs=in_specs, out_specs=out_specs, check_vma=False)
```

```python
import jax
import jax.numpy as jnp
from jax import lax
from jax.experimental import pallas as pl
from jax.experimental.pallas import tpu as pltpu
from jax.sharding import PartitionSpec as P

RMS_EPS = 1e-5
ROPE_THETA = 500000
MESH = pl.DeviceIdType.MESH
NT_DIMS = (((1,), (1,)), ((), ()))
VMEM_MAX = 67043328


def dot_nt(left, right):
    return lax.dot_general(left, right, NT_DIMS, preferred_element_type=jnp.float32)


def front_kernel(table_ref, ctx_ref, hid_ref, gain_ref, cos_ref, sin_ref, mask_ref, wq_hbm, wk_hbm, wv_hbm, kc_ref, vc_ref, out_ref, ko_ref, vo_ref, w_buf, n_buf, new, kbuf, vbuf, fixed, wsem, rsem, ssem, psem):
    g = pl.program_id(0)
    count = pl.num_programs(0) - 1
    _, heads, page, head_dim = kbuf.shape
    _, _, group, _, nodes, _ = new.shape
    pages = table_ref.shape[1]
    window = nodes // page + 1

    def weight(n):
        source = (wq_hbm, wk_hbm, wv_hbm)[n]
        return pltpu.make_async_copy(source, w_buf.at[n], wsem.at[n])

    spans = [pl.ds(i * (kbuf.shape[0] // 8), kbuf.shape[0] // 8) for i in range(8)]
    caches = ((kc_ref, kbuf, ko_ref), (vc_ref, vbuf, vo_ref))
    cache_in = [pltpu.make_async_copy(src.at[span], buf.at[span], rsem.at[n, i]) for n, (src, buf, _) in enumerate(caches) for i, span in enumerate(spans)]
    cache_out = [pltpu.make_async_copy(buf.at[span], dst.at[span], ssem.at[n, i]) for n, (_, buf, dst) in enumerate(caches) for i, span in enumerate(spans)]

    @pl.when(g == 0)
    def _():
        weight(0).start()
        weight(1).start()

    @pl.when(g < count)
    def _():
        widened = hid_ref[...].astype(jnp.float32)
        rms = lax.rsqrt(jnp.mean(widened * widened, axis=-1, keepdims=True) + RMS_EPS)
        gain = gain_ref[...].reshape(1, widened.shape[1]).astype(jnp.float32)
        n_buf[...] = (widened * rms * gain).astype(jnp.bfloat16)
        for n in range(3):

            @pl.when(g == 0)
            def _():
                weight(n).wait()
                if n == 0:
                    weight(2).start()
                if n == 2:
                    for copy in cache_in:
                        copy.start()

            product = jnp.dot(n_buf[...], w_buf[n], preferred_element_type=jnp.float32)
            for h in range(heads):
                part = product[:, h * head_dim : (h + 1) * head_dim]
                if n < 2:
                    part = part * cos_ref[...] + pltpu.roll(part, head_dim // 2, 1) * sin_ref[...]
                new[g % 2, n, :, h] = part.astype(jnp.bfloat16).reshape(group, nodes, head_dim)

    @pl.when(g == 1)
    def _():
        for copy in cache_in:
            copy.wait()
        for copy in cache_out:
            copy.start()

    turn = (g + 1) % 2

    def first_page(b):
        return jnp.minimum(ctx_ref[b] // page, pages - window)

    def attend(r, _):
        b = (g - 1) * group + r
        ctx = ctx_ref[b]
        first = first_page(b)
        base = first * page
        row = base + lax.broadcasted_iota(jnp.int32, (window * page, nodes), 0)
        node = ctx + lax.broadcasted_iota(jnp.int32, (window * page, nodes), 1)
        place = jnp.where(row == node, 1.0, 0.0).astype(jnp.bfloat16)
        slot_id = base + lax.broadcasted_iota(jnp.int32, (window * page, head_dim), 0)
        fresh = (slot_id >= ctx) & (slot_id < ctx + nodes)
        edge = [table_ref[b, first + i] for i in range(window)]
        for which, buf in ((0, kbuf), (1, vbuf)):
            moved = [jnp.dot(place, new[turn, 1 + which, r, h], preferred_element_type=jnp.float32) for h in range(heads)]
            for i, block in enumerate(edge):
                rows = slice(i * page, (i + 1) * page)
                for h in range(heads):
                    old = buf[block, h].astype(jnp.float32)
                    fixed[which, b, i, h] = jnp.where(fresh[rows], moved[h][rows], old).astype(jnp.bfloat16)
        table = [table_ref[b, s] for s in range(pages)]
        seen = lax.broadcasted_iota(jnp.int32, (nodes, pages * page), 1) < ctx
        linked = mask_ref[r] > 0
        scale = head_dim**-0.5
        old_k = [jnp.concatenate([kbuf[block, h] for block in table], axis=0) for h in range(heads)]
        scores = [jnp.where(seen, dot_nt(new[turn, 0, r, h], old_k[h]) * scale, -jnp.inf) for h in range(heads)]
        fresh_scores = [jnp.where(linked, dot_nt(new[turn, 0, r, h], new[turn, 1, r, h]) * scale, -jnp.inf) for h in range(heads)]
        tops = [
            jnp.maximum(jnp.max(old, axis=-1, keepdims=True), jnp.max(fresh, axis=-1, keepdims=True))
            for old, fresh in zip(scores, fresh_scores)
        ]
        probs = [jnp.exp(score - top) for score, top in zip(scores, tops)]
        fresh_probs = [jnp.exp(score - top) for score, top in zip(fresh_scores, tops)]
        totals = [jnp.sum(old, axis=-1, keepdims=True) + jnp.sum(fresh, axis=-1, keepdims=True) for old, fresh in zip(probs, fresh_probs)]
        old_v = [jnp.concatenate([vbuf[block, h] for block in table], axis=0) for h in range(heads)]
        for h in range(heads):
            mixed = jnp.dot(probs[h].astype(jnp.bfloat16), old_v[h], preferred_element_type=jnp.float32)
            mixed = mixed + jnp.dot(fresh_probs[h].astype(jnp.bfloat16), new[turn, 2, r, h], preferred_element_type=jnp.float32)
            out_ref[r, :, h * head_dim : (h + 1) * head_dim] = (mixed / totals[h]).astype(jnp.bfloat16)
        return 0

    @pl.when(g > 0)
    def _():
        lax.fori_loop(0, group, attend, 0, unroll=2)

    @pl.when(g == count)
    def _():
        for copy in cache_out:
            copy.wait()

        def put(b, _):
            for i in range(window):
                block = table_ref[b, first_page(b) + i]
                pltpu.make_async_copy(fixed.at[0, b, i], ko_ref.at[block], psem).start()
                pltpu.make_async_copy(fixed.at[1, b, i], vo_ref.at[block], psem).start()
            return 0

        lax.fori_loop(0, group * count, put, 0)
        pltpu.make_async_copy(fixed, fixed, psem).wait()


def front_stage(table, ctx_len, hidden, gain, cosine, sine, tree_mask, w_q, w_k, w_v, k_cache, v_cache, group):
    requests, nodes, _ = tree_mask.shape
    rows, dim = hidden.shape
    _, heads, page, head_dim = k_cache.shape
    cols = w_q.shape[1]
    block = group * nodes
    last = requests // group - 1
    anywhere = pl.BlockSpec(memory_space=pl.ANY)
    return pl.pallas_call(
        front_kernel,
        grid_spec=pltpu.PrefetchScalarGridSpec(
            num_scalar_prefetch=2,
            grid=(requests // group + 1,),
            in_specs=[
                pl.BlockSpec((block, dim), lambda i, *_: (jnp.minimum(i, last), 0)),
                pl.BlockSpec((dim,), lambda i, *_: (0,)),
                pl.BlockSpec((block, head_dim), lambda i, *_: (jnp.minimum(i, last), 0)),
                pl.BlockSpec((block, head_dim), lambda i, *_: (jnp.minimum(i, last), 0)),
                pl.BlockSpec((group, nodes, nodes), lambda i, *_: (jnp.maximum(i - 1, 0), 0, 0)),
            ]
            + [anywhere] * 5,
            out_specs=[pl.BlockSpec((group, nodes, cols), lambda i, *_: (jnp.maximum(i - 1, 0), 0, 0)), anywhere, anywhere],
            scratch_shapes=[
                pltpu.VMEM((3, dim, cols), jnp.bfloat16),
                pltpu.VMEM((block, dim), jnp.bfloat16),
                pltpu.VMEM((2, 3, group, heads, nodes, head_dim), jnp.bfloat16),
                pltpu.VMEM(k_cache.shape, jnp.bfloat16),
                pltpu.VMEM(v_cache.shape, jnp.bfloat16),
                pltpu.VMEM((2, requests, nodes // page + 1, heads, page, head_dim), jnp.bfloat16),
                pltpu.SemaphoreType.DMA((3,)),
                pltpu.SemaphoreType.DMA((2, 8)),
                pltpu.SemaphoreType.DMA((2, 8)),
                pltpu.SemaphoreType.DMA,
            ],
        ),
        out_shape=[
            jax.ShapeDtypeStruct((requests, nodes, cols), jnp.bfloat16),
            jax.ShapeDtypeStruct(k_cache.shape, k_cache.dtype),
            jax.ShapeDtypeStruct(v_cache.shape, v_cache.dtype),
        ],
        compiler_params=pltpu.CompilerParams(vmem_limit_bytes=VMEM_MAX),
        name="front_stage",
    )(table, ctx_len, hidden, gain, cosine, sine, tree_mask, w_q, w_k, w_v, k_cache, v_cache)


TILE = 512
HALF = TILE // 2
PAIR, X1, Y1, X2, Y2, GX, GY, GP, FX, FY, PX, PY, PD = range(13)


def seat():
    me = lax.axis_index("tp")
    core = me % 2
    x = (me // 2) % 2
    y = me // 4
    blocks = []
    for dy in range(2):
        for dx in range(2):
            for dc in range(2):
                blocks.append((1 - y if dy else y) * 4 + (1 - x if dx else x) * 2 + (1 - core if dc else core))
    return me, blocks


class Exchange:
    def __init__(self, left, fetch, wbuf, depth, resid, gain, h_buf, mbuf, bufs, ssem, rsem, free, scatter_work, gather_work, compute):
        self.left, self.fetch, self.wbuf, self.depth = left, fetch, wbuf, depth
        self.resid, self.gain, self.h_buf, self.mbuf = resid, gain, h_buf, mbuf
        self.r1, self.rx, self.ry, self.r2x, self.r2y, self.ssq = bufs
        self.ssem, self.rsem, self.free = ssem, rsem, free
        self.scatter_work, self.gather_work, self.compute = scatter_work, gather_work, compute
        _, blocks = seat()
        self.to_pair, self.to_x, self.to_y = blocks[1], blocks[2], blocks[4]
        self.steps = mbuf.shape[0]
        self.tiles = self.steps // 2
        self.rows = mbuf.shape[4]

    def send(self, src, dst, kind, i, target):
        pltpu.make_async_remote_copy(
            src_ref=src,
            dst_ref=dst,
            send_sem=self.ssem.at[i // self.tiles, kind],
            recv_sem=self.rsem.at[kind, i],
            device_id={"tp": target},
            device_id_type=MESH,
        ).start()

    def landed(self, ref, kind, i):
        pltpu.make_async_copy(ref, ref, self.rsem.at[kind, i]).wait()

    def sent(self, ref, kind, h):
        pltpu.make_async_copy(ref, ref, self.ssem.at[h, kind]).wait()

    def scatter_step(self, i):
        mbuf, steps, rows = self.mbuf, self.steps, self.rows
        low = pl.ds(0, HALF)
        high = pl.ds(HALF, HALF)

        @pl.when(i < steps)
        def _():
            self.fetch(i).wait()
            left = self.left[i // self.tiles].reshape(8 * rows, self.depth)
            part = jnp.dot(left, self.wbuf[i % 2, pl.ds(0, self.depth)], preferred_element_type=jnp.float32)
            mbuf[i] = part.astype(jnp.bfloat16).reshape(2, 2, 2, rows, TILE)

            @pl.when(i + 2 < steps)
            def _():
                self.fetch(i + 2).start()

            self.send(mbuf.at[i, :, :, 1], self.r1.at[i], PAIR, i, self.to_pair)

        @pl.when((i >= 1) & (i < steps + 1))
        def _():
            t = i - 1
            self.landed(self.r1.at[t], PAIR, t)
            mbuf[t, :, :, 0] = mbuf[t, :, :, 0] + self.r1[t]
            self.send(mbuf.at[t, :, 1, 0, :, low], self.rx.at[t], X1, t, self.to_x)
            self.send(mbuf.at[t, 1, :, 0, :, high], self.ry.at[t], Y1, t, self.to_y)

        @pl.when((i >= 3) & (i < steps + 3))
        def _():
            t = i - 3
            self.landed(self.rx.at[t], X1, t)
            mbuf[t, :, 0, 0, :, low] = mbuf[t, :, 0, 0, :, low] + self.rx[t]
            self.send(mbuf.at[t, 1, 0, 0, :, low], self.r2y.at[t], Y2, t, self.to_y)
            self.landed(self.ry.at[t], Y1, t)
            mbuf[t, 0, :, 0, :, high] = mbuf[t, 0, :, 0, :, high] + self.ry[t]
            self.send(mbuf.at[t, 0, 1, 0, :, high], self.r2x.at[t], X2, t, self.to_x)

        @pl.when(i >= 5)
        def _():
            t = i - 5
            h = t // self.tiles
            self.landed(self.r2y.at[t], Y2, t)
            self.landed(self.r2x.at[t], X2, t)
            for cols, other in ((low, self.r2y), (high, self.r2x)):
                total = (mbuf[t, 0, 0, 0, :, cols] + other[t]).astype(jnp.float32)
                new = (self.resid[t, :, cols].astype(jnp.float32) + total).astype(jnp.bfloat16)
                self.h_buf[t, :, cols] = new
                wide = new.astype(jnp.float32)
                wide = wide * wide
                self.ssq[h] += sum(wide[:, lane : lane + 128] for lane in range(0, HALF, 128))

        @pl.when(i == self.tiles + 5)
        def _():
            self.norm(0)

        @pl.when(i == steps + 1)
        def _():
            self.open(0)

        self.scatter_work(i)

    def norm(self, h):
        tiles = self.tiles
        part = pl.ds(h * tiles, tiles)
        self.sent(self.r1.at[part], PAIR, h)
        self.sent(self.rx.at[part], X1, h)
        self.sent(self.ry.at[part], Y1, h)
        self.sent(self.r2x.at[part], X2, h)
        self.sent(self.r2y.at[part], Y2, h)
        for target in (self.to_x, self.to_y, self.to_pair):
            pl.semaphore_signal(self.free.at[h], inc=1, device_id={"tp": target}, device_id_type=MESH)
        scale = lax.rsqrt(jnp.sum(self.ssq[h], axis=-1, keepdims=True) * (1.0 / (tiles * TILE)) + RMS_EPS)
        for t in range(tiles):
            gain = self.gain[pl.ds(t * TILE, TILE)].reshape(1, TILE).astype(jnp.float32)
            i = h * tiles + t
            self.mbuf[i, 0, 0, 0] = (self.h_buf[i].astype(jnp.float32) * scale * gain).astype(jnp.bfloat16)

    def own(self, i):
        mine = self.mbuf.at[i, 0, 0, 0]
        self.send(mine, self.mbuf.at[i, 0, 1, 0], GX, i, self.to_x)
        self.send(mine, self.mbuf.at[i, 1, 0, 0], GY, i, self.to_y)
        self.send(mine, self.mbuf.at[i, 0, 0, 1], GP, i, self.to_pair)

    def open(self, h):
        pl.semaphore_wait(self.free.at[h], 3)
        if h == 0:
            for i in range(2):
                self.own(i)

    def gather_step(self, i):
        mbuf, steps, rows = self.mbuf, self.steps, self.rows
        upper = pl.ds(0, rows // 2)
        lower = pl.ds(rows // 2, rows // 2)

        @pl.when(i == 6)
        def _():
            self.open(1)

        @pl.when(i < steps)
        def _():
            self.landed(mbuf.at[i, 0, 1, 0], GX, i)
            self.send(mbuf.at[i, 0, 1, 0, upper], mbuf.at[i, 1, 1, 0, upper], FY, i, self.to_y)
            self.send(mbuf.at[i, 0, 1, 0], mbuf.at[i, 0, 1, 1], PX, i, self.to_pair)
            self.landed(mbuf.at[i, 1, 0, 0], GY, i)
            self.send(mbuf.at[i, 1, 0, 0, lower], mbuf.at[i, 1, 1, 0, lower], FX, i, self.to_x)
            self.send(mbuf.at[i, 1, 0, 0], mbuf.at[i, 1, 0, 1], PY, i, self.to_pair)

        @pl.when(i + 2 < steps)
        def _():
            self.own(i + 2)

        @pl.when((i >= 2) & (i < steps + 2))
        def _():
            t = i - 2
            self.landed(mbuf.at[t, 1, 1, 0, upper], FY, t)
            self.landed(mbuf.at[t, 1, 1, 0, lower], FX, t)
            self.send(mbuf.at[t, 1, 1, 0], mbuf.at[t, 1, 1, 1], PD, t, self.to_pair)

        self.gather_work(i)

        @pl.when(i >= 3)
        def _():
            t = i - 3
            self.landed(mbuf.at[t, 0, 0, 1], GP, t)
            self.landed(mbuf.at[t, 0, 1, 1], PX, t)
            self.landed(mbuf.at[t, 1, 0, 1], PY, t)
            self.landed(mbuf.at[t, 1, 1, 1], PD, t)
            self.compute(t)

    def close(self, h):
        part = pl.ds(h * self.tiles, self.tiles)
        for kind in (GX, GY, GP, PX, PY, PD):
            self.sent(self.h_buf.at[part], kind, h)
        half = pl.ds(h * self.tiles, self.tiles // 2)
        for kind in (FX, FY):
            self.sent(self.h_buf.at[half], kind, h)


def loop(start, stop, step):
    def body(i, _):
        step(i)
        return 0

    lax.fori_loop(start, stop, body, 0)


def tail_kernel(mlp_gain, final_gain, id_ref, att_hbm, hid_hbm, wo_hbm, wg_hbm, wu_hbm, wd_hbm, wl_hbm, norm_ref, prob_ref, mbuf, r1, rx, ry, r2x, r2y, ssq, left, prod, resid, h_buf, wbuf, nbuf, acc, stats, ssem, rsem, wsem, nsem, isem, tsem, usem, free):
    me, blocks = seat()
    steps = mbuf.shape[0]
    tiles = steps // 2
    rows = mbuf.shape[4]
    half = 8 * rows
    count = 2 * half
    heads_width = left.shape[3]
    width = wg_hbm.shape[0]
    padded = wbuf.shape[1]
    vocab = wl_hbm.shape[0]
    parts = acc.shape[0]
    side = acc.shape[1]
    piece = pl.cdiv(vocab, parts * 16) * 16
    pieces = [(n * piece, min(piece, vocab - n * piece)) for n in range(parts)]
    others = [(me + i) % 8 for i in range(1, 8)]

    def columns(i):
        return pl.ds(pl.multiple_of(i % tiles * TILE, TILE), TILE)

    def fetch_o(i):
        return pltpu.make_async_copy(wo_hbm.at[:, columns(i)], wbuf.at[i % 2, pl.ds(0, heads_width)], wsem.at[i % 2])

    def fetch_d(i):
        return pltpu.make_async_copy(wd_hbm.at[:, columns(i)], wbuf.at[i % 2, pl.ds(0, width)], wsem.at[i % 2])

    def fetch_in(i):
        slot = i % 2
        return (
            pltpu.make_async_copy(wg_hbm.at[:, columns(i)], nbuf.at[slot, pl.ds(0, width)], nsem.at[0, slot]),
            pltpu.make_async_copy(wu_hbm.at[:, columns(i)], nbuf.at[slot, pl.ds(padded, width)], nsem.at[1, slot]),
        )

    def fetch_l(i):
        slot = i % 2
        return (pltpu.make_async_copy(wl_hbm.at[:, columns(i)], nbuf.at[slot, pl.ds(0, vocab)], nsem.at[0, slot]),)

    fetch_o(0).start()
    for h in range(2):
        for k, block in enumerate(blocks):
            source = pl.ds(pl.multiple_of(block * 2 * rows + h * rows, rows), rows)
            pltpu.make_async_copy(att_hbm.at[source], left.at[h, k], isem.at[0]).start()
    fetch_o(1).start()
    barrier = pltpu.get_barrier_semaphore()
    for other in others:
        pl.semaphore_signal(barrier, inc=1, device_id={"tp": other}, device_id_type=MESH)
    pl.semaphore_wait(barrier, 7)
    for i in range(steps):
        source = pl.ds(pl.multiple_of(me * 2 * rows + i // tiles * rows, rows), rows)
        pltpu.make_async_copy(hid_hbm.at[source, pl.ds(i % tiles * TILE, TILE)], resid.at[i], isem.at[1]).start()
    pltpu.make_async_copy(left, left, isem.at[0]).wait()
    ssq[...] = jnp.zeros_like(ssq)

    def clear(n):
        acc[n] = jnp.zeros(acc.shape[1:], jnp.float32)

    def finish(h):
        some = pl.ds(h * half, half)

        def one(n):
            cols = pl.ds(pl.multiple_of(n % 4 * 256, 256), 256)
            value = jax.nn.silu(acc[n // 4, some, cols]) * acc[2 + n // 4, some, cols]
            prod[h, :, pl.ds(pl.multiple_of(n * 256, 256), 256)] = value.astype(jnp.bfloat16)

        loop(0, padded // 256, one)

    def streamed(fetch, i, work):
        for copy in fetch(i):
            copy.wait()
        work(i % 2, pl.ds(pl.multiple_of(i // tiles * half, half), half))

        @pl.when(i + 2 < steps)
        def _():
            for copy in fetch(i + 2):
                copy.start()

    def work_one(i):
        @pl.when(i < parts)
        def _():
            clear(i)

        @pl.when(i == 4)
        def _():
            pltpu.make_async_copy(resid, resid, isem.at[1]).wait()
            for slot in range(2):
                gap = jnp.zeros((padded - width, TILE), jnp.bfloat16)
                wbuf[slot, pl.ds(width, padded - width)] = gap
                nbuf[slot, pl.ds(width, padded - width)] = gap
                nbuf[slot, pl.ds(padded + width, padded - width)] = gap
                for copy in fetch_in(slot):
                    copy.start()

    def compute_in(i):
        def work(slot, some):
            left_rows = mbuf[i].reshape(half, TILE)
            for which in range(2):
                for n in range(2):
                    wide = min(side, padded - n * side)
                    weights = nbuf[slot, pl.ds(which * padded + n * side, wide)]
                    acc[which * 2 + n, some, pl.ds(0, wide)] += dot_nt(left_rows, weights)

        streamed(fetch_in, i, work)

    def between(i):
        @pl.when(i == 0)
        def _():
            first.norm(1)
            fetch_d(0).start()
            fetch_d(1).start()
            ssq[...] = jnp.zeros_like(ssq)

        @pl.when(i == 13)
        def _():
            finish(0)

        @pl.when(i == 15)
        def _():
            first.close(0)

        @pl.when(i >= steps)
        def _():
            second.scatter_step(i - steps)

    def work_two(i):
        @pl.when(i == 3)
        def _():
            finish(1)
            first.close(1)
            for slot in range(2):
                for copy in fetch_l(slot):
                    copy.start()

        @pl.when((i >= 4) & (i < 4 + parts))
        def _():
            clear(i - 4)

    def compute_head(i):
        def work(slot, some):
            right_rows = mbuf[i].reshape(half, TILE)
            for n, (start, size) in enumerate(pieces):
                acc[n, pl.ds(0, size), some] += dot_nt(nbuf[slot, pl.ds(start, size)], right_rows)

        streamed(fetch_l, i, work)

    def last(i):
        @pl.when(i == 0)
        def _():
            second.norm(1)

    bufs = (r1, rx, ry, r2x, r2y, ssq)
    first = Exchange(left, fetch_o, wbuf, heads_width, resid, mlp_gain, h_buf, mbuf, bufs, ssem, rsem, free.at[0], work_one, between, compute_in)
    second = Exchange(prod, fetch_d, wbuf, padded, h_buf, final_gain, h_buf, mbuf, bufs, ssem, rsem, free.at[1], work_two, last, compute_head)
    loop(0, steps + 5, first.scatter_step)
    loop(0, steps + 3, first.gather_step)
    loop(3, steps + 5, second.scatter_step)
    loop(0, steps + 3, second.gather_step)
    second.close(0)
    second.close(1)

    best = jnp.full((8, count), -jnp.inf, jnp.float32)
    for n, (start, size) in enumerate(pieces):
        best = jnp.maximum(best, jnp.max(acc[n, pl.ds(0, size)].reshape(size // 8, 8, count), axis=0))
    best = jnp.max(best, axis=0, keepdims=True)
    ids = [id_ref[pl.ds(2 * block + h, 1)] for h in range(2) for block in blocks]
    local_id = jnp.concatenate(ids, axis=1) - me * vocab
    total = jnp.zeros((8, count), jnp.float32)
    picked = jnp.zeros((8, count), jnp.float32)
    for n, (start, size) in enumerate(pieces):
        value = acc[n, pl.ds(0, size)]
        hit = lax.broadcasted_iota(jnp.int32, (size, count), 0) + start == local_id
        total = total + jnp.sum(jnp.exp(value - best).reshape(size // 8, 8, count), axis=0)
        picked = picked + jnp.sum(jnp.where(hit, value, 0.0).reshape(size // 8, 8, count), axis=0)
    for n, values in enumerate((best, jnp.sum(total, axis=0, keepdims=True), jnp.sum(picked, axis=0, keepdims=True))):
        for h in range(2):
            for k, block in enumerate(blocks):
                start = h * half + k * rows
                stats[me, n, pl.ds(2 * block + h, 1)] = values[:, start : start + rows]
    copies = []
    for i, other in enumerate(others):
        copy = pltpu.make_async_remote_copy(
            src_ref=stats.at[me], dst_ref=stats.at[me], send_sem=tsem.at[i], recv_sem=usem.at[i], device_id={"tp": other}, device_id_type=MESH
        )
        copy.start()
        copies.append(copy)
    for copy in copies:
        copy.wait()
    top = stats[0, 0]
    for d in range(1, 8):
        top = jnp.maximum(top, stats[d, 0])
    whole = jnp.zeros_like(top)
    score = jnp.zeros_like(top)
    for d in range(8):
        whole = whole + stats[d, 1] * jnp.exp(stats[d, 0] - top)
        score = score + stats[d, 2]
    norm = top + jnp.log(whole)
    norm_ref[...] = norm
    prob_ref[...] = score - norm


def tail_stage(mlp_gain, final_gain, score_id, attended, hidden, w_o, gate_t, up_t, w_down, head_t):
    count, dim = hidden.shape
    steps = 2 * dim // TILE
    rows = count // 16
    padded = pl.cdiv(gate_t.shape[0], 256) * 256
    vocab = head_t.shape[0]
    vmem = pl.BlockSpec(memory_space=pltpu.VMEM)
    anywhere = pl.BlockSpec(memory_space=pl.ANY)
    bf16 = jnp.bfloat16
    return pl.pallas_call(
        tail_kernel,
        in_specs=[vmem] * 3 + [anywhere] * 7,
        out_specs=[vmem, vmem],
        out_shape=[jax.ShapeDtypeStruct(score_id.shape, jnp.float32)] * 2,
        scratch_shapes=[
            pltpu.VMEM((steps, 2, 2, 2, rows, TILE), bf16),
            pltpu.VMEM((steps, 2, 2, rows, TILE), bf16),
            pltpu.VMEM((steps, 2, rows, HALF), bf16),
            pltpu.VMEM((steps, 2, rows, HALF), bf16),
            pltpu.VMEM((steps, rows, HALF), bf16),
            pltpu.VMEM((steps, rows, HALF), bf16),
            pltpu.VMEM((2, rows, 128), jnp.float32),
            pltpu.VMEM((2, 8, rows, w_o.shape[0]), bf16),
            pltpu.VMEM((2, 8 * rows, padded), bf16),
            pltpu.VMEM((steps, rows, TILE), bf16),
            pltpu.VMEM((steps, rows, TILE), bf16),
            pltpu.VMEM((2, padded, TILE), bf16),
            pltpu.VMEM((2, max(2 * padded, vocab), TILE), bf16),
            pltpu.VMEM((4, 1024, count), jnp.float32),
            pltpu.VMEM((8, 3) + score_id.shape, jnp.float32),
            pltpu.SemaphoreType.DMA((2, 13)),
            pltpu.SemaphoreType.DMA((13, steps)),
            pltpu.SemaphoreType.DMA((2,)),
            pltpu.SemaphoreType.DMA((2, 2)),
            pltpu.SemaphoreType.DMA((2,)),
            pltpu.SemaphoreType.DMA((7,)),
            pltpu.SemaphoreType.DMA((7,)),
            pltpu.SemaphoreType.REGULAR((2, 2)),
        ],
        compiler_params=pltpu.CompilerParams(collective_id=1, has_side_effects=True, vmem_limit_bytes=VMEM_MAX),
        name="tail_stage",
    )(mlp_gain, final_gain, score_id, attended, hidden, w_o, gate_t, up_t, w_down, head_t)


def rope_tables(positions, head_dim):
    half = head_dim // 2
    lane = jnp.arange(head_dim, dtype=jnp.int32)
    inv_freq = 1.0 / (ROPE_THETA ** ((lane % half).astype(jnp.float32) * (2.0 / head_dim)))
    angles = positions.astype(jnp.float32)[:, None] * inv_freq
    return jnp.cos(angles), jnp.sin(angles) * jnp.where(lane < half, -1.0, 1.0)


def solution(mesh):
    def group_step(hidden, tree_mask, depth, ctx_len, block_table, score_id, k_cache, v_cache, attn_norm, w_q, w_k, w_v, w_o, mlp_norm, w_gate, w_up, w_down, final_norm, w_lm):
        requests, nodes, dim = hidden.shape
        head_dim = k_cache.shape[3]
        rows = requests * nodes
        flat = hidden.reshape(rows, dim)
        cosine, sine = rope_tables((ctx_len[:, None] + depth).reshape(rows), head_dim)
        old_k = jnp.transpose(k_cache, (0, 2, 1, 3))
        old_v = jnp.transpose(v_cache, (0, 2, 1, 3))
        attended, k_out, v_out = front_stage(block_table, ctx_len, flat, attn_norm, cosine, sine, tree_mask, w_q, w_k, w_v, old_k, old_v, 4)
        attended = attended.reshape(rows, w_q.shape[1])
        k_out = jnp.transpose(k_out, (0, 2, 1, 3))
        v_out = jnp.transpose(v_out, (0, 2, 1, 3))

        log_norm, log_prob = tail_stage(mlp_norm, final_norm, score_id, attended, flat, w_o, w_gate.T, w_up.T, w_down, w_lm.T)
        return log_norm.reshape(requests, nodes), log_prob.reshape(requests, nodes), k_out, v_out

    request_spec = P("dp", None, None)
    node_spec = P("dp", None)
    cache_spec = P("dp", None, "tp", None)
    shared_spec = P(None)
    column_spec = P(None, "tp")
    row_spec = P("tp", None)
    in_specs = (request_spec, request_spec, node_spec, P("dp"), node_spec, node_spec, cache_spec, cache_spec, shared_spec, column_spec, column_spec, column_spec, row_spec, shared_spec, column_spec, column_spec, row_spec, shared_spec, column_spec)
    out_specs = (node_spec, node_spec, cache_spec, cache_spec)
    return jax.shard_map(group_step, mesh=mesh, in_specs=in_specs, out_specs=out_specs, check_vma=False)
```

```python
import jax
import jax.numpy as jnp
from jax import lax
from jax.experimental import pallas as pl
from jax.experimental.pallas import tpu as pltpu
from jax.sharding import PartitionSpec as P

RMS_EPS = 1e-5
ROPE_THETA = 500000
MESH = pl.DeviceIdType.MESH
NT_DIMS = (((1,), (1,)), ((), ()))
VMEM_MAX = 67043328


def dot_nt(left, right):
    return lax.dot_general(left, right, NT_DIMS, preferred_element_type=jnp.float32)


def front_kernel(table_ref, ctx_ref, hid_ref, gain_ref, cos_ref, sin_ref, mask_ref, wq_hbm, wk_hbm, wv_hbm, kc_ref, vc_ref, out_ref, ko_ref, vo_ref, w_buf, n_buf, new, kbuf, vbuf, fixed, wsem, rsem, ssem, psem):
    g = pl.program_id(0)
    count = pl.num_programs(0) - 1
    _, heads, page, head_dim = kbuf.shape
    _, _, group, _, nodes, _ = new.shape
    pages = table_ref.shape[1]
    window = nodes // page + 1

    def weight(n):
        source = (wq_hbm, wk_hbm, wv_hbm)[n]
        return pltpu.make_async_copy(source, w_buf.at[n], wsem.at[n])

    spans = [pl.ds(i * (kbuf.shape[0] // 8), kbuf.shape[0] // 8) for i in range(8)]
    caches = ((kc_ref, kbuf, ko_ref), (vc_ref, vbuf, vo_ref))
    cache_in = [pltpu.make_async_copy(src.at[span], buf.at[span], rsem.at[n, i]) for n, (src, buf, _) in enumerate(caches) for i, span in enumerate(spans)]
    cache_out = [pltpu.make_async_copy(buf.at[span], dst.at[span], ssem.at[n, i]) for n, (_, buf, dst) in enumerate(caches) for i, span in enumerate(spans)]

    @pl.when(g == 0)
    def _():
        weight(0).start()
        weight(1).start()
        weight(2).start()

    @pl.when(g < count)
    def _():
        widened = hid_ref[...].astype(jnp.float32)
        rms = lax.rsqrt(jnp.mean(widened * widened, axis=-1, keepdims=True) + RMS_EPS)
        gain = gain_ref[...].reshape(1, widened.shape[1]).astype(jnp.float32)
        n_buf[...] = (widened * rms * gain).astype(jnp.bfloat16)
        for n in range(3):

            @pl.when(g == 0)
            def _():
                weight(n).wait()
                if n == 2:
                    for copy in cache_in:
                        copy.start()

            product = jnp.dot(n_buf[...], w_buf[n], preferred_element_type=jnp.float32)
            for h in range(heads):
                part = product[:, h * head_dim : (h + 1) * head_dim]
                if n < 2:
                    part = part * cos_ref[...] + pltpu.roll(part, head_dim // 2, 1) * sin_ref[...]
                new[g % 2, n, :, h] = part.astype(jnp.bfloat16).reshape(group, nodes, head_dim)

    @pl.when(g == 1)
    def _():
        for copy in cache_in:
            copy.wait()
        for copy in cache_out:
            copy.start()

    turn = (g + 1) % 2

    def first_page(b):
        return jnp.minimum(ctx_ref[b] // page, pages - window)

    def attend(r, _):
        b = (g - 1) * group + r
        ctx = ctx_ref[b]
        first = first_page(b)
        base = first * page
        row = base + lax.broadcasted_iota(jnp.int32, (window * page, nodes), 0)
        node = ctx + lax.broadcasted_iota(jnp.int32, (window * page, nodes), 1)
        place = jnp.where(row == node, 1.0, 0.0).astype(jnp.bfloat16)
        slot_id = base + lax.broadcasted_iota(jnp.int32, (window * page, head_dim), 0)
        fresh = (slot_id >= ctx) & (slot_id < ctx + nodes)
        edge = [table_ref[b, first + i] for i in range(window)]
        for which, buf in ((0, kbuf), (1, vbuf)):
            moved = [jnp.dot(place, new[turn, 1 + which, r, h], preferred_element_type=jnp.float32) for h in range(heads)]
            for i, block in enumerate(edge):
                rows = slice(i * page, (i + 1) * page)
                for h in range(heads):
                    old = buf[block, h].astype(jnp.float32)
                    fixed[which, b, i, h] = jnp.where(fresh[rows], moved[h][rows], old).astype(jnp.bfloat16)
        table = [table_ref[b, s] for s in range(pages)]
        seen = lax.broadcasted_iota(jnp.int32, (nodes, pages * page), 1) < ctx
        linked = mask_ref[r] > 0
        scale = head_dim**-0.5
        old_k = [jnp.concatenate([kbuf[block, h] for block in table], axis=0) for h in range(heads)]
        scores = [jnp.where(seen, dot_nt(new[turn, 0, r, h], old_k[h]) * scale, -jnp.inf) for h in range(heads)]
        fresh_scores = [jnp.where(linked, dot_nt(new[turn, 0, r, h], new[turn, 1, r, h]) * scale, -jnp.inf) for h in range(heads)]
        tops = [
            jnp.maximum(jnp.max(old, axis=-1, keepdims=True), jnp.max(fresh, axis=-1, keepdims=True))
            for old, fresh in zip(scores, fresh_scores)
        ]
        probs = [jnp.exp(score - top) for score, top in zip(scores, tops)]
        fresh_probs = [jnp.exp(score - top) for score, top in zip(fresh_scores, tops)]
        totals = [jnp.sum(old, axis=-1, keepdims=True) + jnp.sum(fresh, axis=-1, keepdims=True) for old, fresh in zip(probs, fresh_probs)]
        old_v = [jnp.concatenate([vbuf[block, h] for block in table], axis=0) for h in range(heads)]
        for h in range(heads):
            mixed = jnp.dot(probs[h].astype(jnp.bfloat16), old_v[h], preferred_element_type=jnp.float32)
            mixed = mixed + jnp.dot(fresh_probs[h].astype(jnp.bfloat16), new[turn, 2, r, h], preferred_element_type=jnp.float32)
            out_ref[r, :, h * head_dim : (h + 1) * head_dim] = (mixed / totals[h]).astype(jnp.bfloat16)
        return 0

    @pl.when(g > 0)
    def _():
        lax.fori_loop(0, group, attend, 0, unroll=4)

    @pl.when(g == count)
    def _():
        for copy in cache_out:
            copy.wait()

        def put(b, _):
            for i in range(window):
                block = table_ref[b, first_page(b) + i]
                pltpu.make_async_copy(fixed.at[0, b, i], ko_ref.at[block], psem).start()
                pltpu.make_async_copy(fixed.at[1, b, i], vo_ref.at[block], psem).start()
            return 0

        lax.fori_loop(0, group * count, put, 0)
        pltpu.make_async_copy(fixed, fixed, psem).wait()


def front_stage(table, ctx_len, hidden, gain, cosine, sine, tree_mask, w_q, w_k, w_v, k_cache, v_cache, group):
    requests, nodes, _ = tree_mask.shape
    rows, dim = hidden.shape
    _, heads, page, head_dim = k_cache.shape
    cols = w_q.shape[1]
    block = group * nodes
    last = requests // group - 1
    anywhere = pl.BlockSpec(memory_space=pl.ANY)
    return pl.pallas_call(
        front_kernel,
        grid_spec=pltpu.PrefetchScalarGridSpec(
            num_scalar_prefetch=2,
            grid=(requests // group + 1,),
            in_specs=[
                pl.BlockSpec((block, dim), lambda i, *_: (jnp.minimum(i, last), 0)),
                pl.BlockSpec((dim,), lambda i, *_: (0,)),
                pl.BlockSpec((block, head_dim), lambda i, *_: (jnp.minimum(i, last), 0)),
                pl.BlockSpec((block, head_dim), lambda i, *_: (jnp.minimum(i, last), 0)),
                pl.BlockSpec((group, nodes, nodes), lambda i, *_: (jnp.maximum(i - 1, 0), 0, 0)),
            ]
            + [anywhere] * 5,
            out_specs=[pl.BlockSpec((group, nodes, cols), lambda i, *_: (jnp.maximum(i - 1, 0), 0, 0)), anywhere, anywhere],
            scratch_shapes=[
                pltpu.VMEM((3, dim, cols), jnp.bfloat16),
                pltpu.VMEM((block, dim), jnp.bfloat16),
                pltpu.VMEM((2, 3, group, heads, nodes, head_dim), jnp.bfloat16),
                pltpu.VMEM(k_cache.shape, jnp.bfloat16),
                pltpu.VMEM(v_cache.shape, jnp.bfloat16),
                pltpu.VMEM((2, requests, nodes // page + 1, heads, page, head_dim), jnp.bfloat16),
                pltpu.SemaphoreType.DMA((3,)),
                pltpu.SemaphoreType.DMA((2, 8)),
                pltpu.SemaphoreType.DMA((2, 8)),
                pltpu.SemaphoreType.DMA,
            ],
        ),
        out_shape=[
            jax.ShapeDtypeStruct((requests, nodes, cols), jnp.bfloat16),
            jax.ShapeDtypeStruct(k_cache.shape, k_cache.dtype),
            jax.ShapeDtypeStruct(v_cache.shape, v_cache.dtype),
        ],
        compiler_params=pltpu.CompilerParams(vmem_limit_bytes=VMEM_MAX),
        name="front_stage",
    )(table, ctx_len, hidden, gain, cosine, sine, tree_mask, w_q, w_k, w_v, k_cache, v_cache)


TILE = 512
HALF = TILE // 2
PAIR, X1, Y1, X2, Y2, GX, GY, GP, FX, FY, PX, PY, PD = range(13)


def seat():
    me = lax.axis_index("tp")
    core = me % 2
    x = (me // 2) % 2
    y = me // 4
    blocks = []
    for dy in range(2):
        for dx in range(2):
            for dc in range(2):
                blocks.append((1 - y if dy else y) * 4 + (1 - x if dx else x) * 2 + (1 - core if dc else core))
    return me, blocks


class Exchange:
    def __init__(self, left, fetch, wbuf, depth, resid, gain, h_buf, mbuf, bufs, ssem, rsem, free, scatter_work, gather_work, compute):
        self.left, self.fetch, self.wbuf, self.depth = left, fetch, wbuf, depth
        self.resid, self.gain, self.h_buf, self.mbuf = resid, gain, h_buf, mbuf
        self.r1, self.rx, self.ry, self.r2x, self.r2y, self.ssq = bufs
        self.ssem, self.rsem, self.free = ssem, rsem, free
        self.scatter_work, self.gather_work, self.compute = scatter_work, gather_work, compute
        _, blocks = seat()
        self.to_pair, self.to_x, self.to_y = blocks[1], blocks[2], blocks[4]
        self.steps = mbuf.shape[0]
        self.tiles = self.steps // 2
        self.rows = mbuf.shape[4]

    def send(self, src, dst, kind, i, target):
        pltpu.make_async_remote_copy(
            src_ref=src,
            dst_ref=dst,
            send_sem=self.ssem.at[i // self.tiles, kind],
            recv_sem=self.rsem.at[kind, i],
            device_id={"tp": target},
            device_id_type=MESH,
        ).start()

    def landed(self, ref, kind, i):
        pltpu.make_async_copy(ref, ref, self.rsem.at[kind, i]).wait()

    def sent(self, ref, kind, h):
        pltpu.make_async_copy(ref, ref, self.ssem.at[h, kind]).wait()

    def scatter_step(self, i):
        mbuf, steps, rows = self.mbuf, self.steps, self.rows
        low = pl.ds(0, HALF)
        high = pl.ds(HALF, HALF)

        @pl.when(i < steps)
        def _():
            self.fetch(i).wait()
            left = self.left[i // self.tiles].reshape(8 * rows, self.depth)
            part = jnp.dot(left, self.wbuf[i % 2, pl.ds(0, self.depth)], preferred_element_type=jnp.float32)
            mbuf[i] = part.astype(jnp.bfloat16).reshape(2, 2, 2, rows, TILE)

            @pl.when(i + 2 < steps)
            def _():
                self.fetch(i + 2).start()

            self.send(mbuf.at[i, :, :, 1], self.r1.at[i], PAIR, i, self.to_pair)

        @pl.when((i >= 1) & (i < steps + 1))
        def _():
            t = i - 1
            self.landed(self.r1.at[t], PAIR, t)
            mbuf[t, :, :, 0] = mbuf[t, :, :, 0] + self.r1[t]
            self.send(mbuf.at[t, :, 1, 0, :, low], self.rx.at[t], X1, t, self.to_x)
            self.send(mbuf.at[t, 1, :, 0, :, high], self.ry.at[t], Y1, t, self.to_y)

        @pl.when((i >= 3) & (i < steps + 3))
        def _():
            t = i - 3
            self.landed(self.rx.at[t], X1, t)
            mbuf[t, :, 0, 0, :, low] = mbuf[t, :, 0, 0, :, low] + self.rx[t]
            self.send(mbuf.at[t, 1, 0, 0, :, low], self.r2y.at[t], Y2, t, self.to_y)
            self.landed(self.ry.at[t], Y1, t)
            mbuf[t, 0, :, 0, :, high] = mbuf[t, 0, :, 0, :, high] + self.ry[t]
            self.send(mbuf.at[t, 0, 1, 0, :, high], self.r2x.at[t], X2, t, self.to_x)

        @pl.when(i >= 5)
        def _():
            t = i - 5
            h = t // self.tiles
            self.landed(self.r2y.at[t], Y2, t)
            self.landed(self.r2x.at[t], X2, t)
            for cols, other in ((low, self.r2y), (high, self.r2x)):
                total = (mbuf[t, 0, 0, 0, :, cols] + other[t]).astype(jnp.float32)
                new = (self.resid[t, :, cols].astype(jnp.float32) + total).astype(jnp.bfloat16)
                self.h_buf[t, :, cols] = new
                wide = new.astype(jnp.float32)
                wide = wide * wide
                self.ssq[h] += sum(wide[:, lane : lane + 128] for lane in range(0, HALF, 128))

        @pl.when(i == self.tiles + 5)
        def _():
            self.norm(0)

        @pl.when(i == steps + 1)
        def _():
            self.open(0)

        self.scatter_work(i)

    def norm(self, h):
        tiles = self.tiles
        part = pl.ds(h * tiles, tiles)
        self.sent(self.r1.at[part], PAIR, h)
        self.sent(self.rx.at[part], X1, h)
        self.sent(self.ry.at[part], Y1, h)
        self.sent(self.r2x.at[part], X2, h)
        self.sent(self.r2y.at[part], Y2, h)
        for target in (self.to_x, self.to_y, self.to_pair):
            pl.semaphore_signal(self.free.at[h], inc=1, device_id={"tp": target}, device_id_type=MESH)
        scale = lax.rsqrt(jnp.sum(self.ssq[h], axis=-1, keepdims=True) * (1.0 / (tiles * TILE)) + RMS_EPS)
        for t in range(tiles):
            gain = self.gain[pl.ds(t * TILE, TILE)].reshape(1, TILE).astype(jnp.float32)
            i = h * tiles + t
            self.mbuf[i, 0, 0, 0] = (self.h_buf[i].astype(jnp.float32) * scale * gain).astype(jnp.bfloat16)

    def own(self, i):
        mine = self.mbuf.at[i, 0, 0, 0]
        self.send(mine, self.mbuf.at[i, 0, 1, 0], GX, i, self.to_x)
        self.send(mine, self.mbuf.at[i, 1, 0, 0], GY, i, self.to_y)
        self.send(mine, self.mbuf.at[i, 0, 0, 1], GP, i, self.to_pair)

    def open(self, h):
        pl.semaphore_wait(self.free.at[h], 3)
        if h == 0:
            for i in range(2):
                self.own(i)

    def gather_step(self, i):
        mbuf, steps, rows = self.mbuf, self.steps, self.rows
        upper = pl.ds(0, rows // 2)
        lower = pl.ds(rows // 2, rows // 2)

        @pl.when(i == 6)
        def _():
            self.open(1)

        @pl.when(i < steps)
        def _():
            self.landed(mbuf.at[i, 0, 1, 0], GX, i)
            self.send(mbuf.at[i, 0, 1, 0, upper], mbuf.at[i, 1, 1, 0, upper], FY, i, self.to_y)
            self.send(mbuf.at[i, 0, 1, 0], mbuf.at[i, 0, 1, 1], PX, i, self.to_pair)
            self.landed(mbuf.at[i, 1, 0, 0], GY, i)
            self.send(mbuf.at[i, 1, 0, 0, lower], mbuf.at[i, 1, 1, 0, lower], FX, i, self.to_x)
            self.send(mbuf.at[i, 1, 0, 0], mbuf.at[i, 1, 0, 1], PY, i, self.to_pair)

        @pl.when(i + 2 < steps)
        def _():
            self.own(i + 2)

        @pl.when((i >= 2) & (i < steps + 2))
        def _():
            t = i - 2
            self.landed(mbuf.at[t, 1, 1, 0, upper], FY, t)
            self.landed(mbuf.at[t, 1, 1, 0, lower], FX, t)
            self.send(mbuf.at[t, 1, 1, 0], mbuf.at[t, 1, 1, 1], PD, t, self.to_pair)

        self.gather_work(i)

        @pl.when(i >= 3)
        def _():
            t = i - 3
            self.landed(mbuf.at[t, 0, 0, 1], GP, t)
            self.landed(mbuf.at[t, 0, 1, 1], PX, t)
            self.landed(mbuf.at[t, 1, 0, 1], PY, t)
            self.landed(mbuf.at[t, 1, 1, 1], PD, t)
            self.compute(t)

    def close(self, h):
        part = pl.ds(h * self.tiles, self.tiles)
        for kind in (GX, GY, GP, PX, PY, PD):
            self.sent(self.h_buf.at[part], kind, h)
        half = pl.ds(h * self.tiles, self.tiles // 2)
        for kind in (FX, FY):
            self.sent(self.h_buf.at[half], kind, h)


def loop(start, stop, step):
    def body(i, _):
        step(i)
        return 0

    lax.fori_loop(start, stop, body, 0)


def tail_kernel(mlp_gain, final_gain, id_ref, att_hbm, hid_hbm, wo_hbm, wg_hbm, wu_hbm, wd_hbm, wl_hbm, out_ref, mbuf, r1, rx, ry, r2x, r2y, ssq, left, prod, resid, h_buf, wbuf, nbuf, acc, stats, ssem, rsem, wsem, nsem, isem, tsem, usem, free):
    me, blocks = seat()
    steps = mbuf.shape[0]
    tiles = steps // 2
    rows = mbuf.shape[4]
    half = 8 * rows
    count = 2 * half
    heads_width = left.shape[3]
    width = wg_hbm.shape[0]
    padded = wbuf.shape[1]
    vocab = wl_hbm.shape[0]
    parts = acc.shape[0]
    side = acc.shape[1]
    piece = pl.cdiv(vocab, parts * 16) * 16
    pieces = [(n * piece, min(piece, vocab - n * piece)) for n in range(parts)]
    others = [(me + i) % 8 for i in range(1, 8)]

    def columns(i):
        return pl.ds(pl.multiple_of(i % tiles * TILE, TILE), TILE)

    def fetch_o(i):
        return pltpu.make_async_copy(wo_hbm.at[:, columns(i)], wbuf.at[i % 2, pl.ds(0, heads_width)], wsem.at[i % 2])

    def fetch_d(i):
        return pltpu.make_async_copy(wd_hbm.at[:, columns(i)], wbuf.at[i % 2, pl.ds(0, width)], wsem.at[i % 2])

    def fetch_in(i):
        slot = i % 2
        return (
            pltpu.make_async_copy(wg_hbm.at[:, columns(i)], nbuf.at[slot, pl.ds(0, width)], nsem.at[0, slot]),
            pltpu.make_async_copy(wu_hbm.at[:, columns(i)], nbuf.at[slot, pl.ds(padded, width)], nsem.at[1, slot]),
        )

    def fetch_l(i):
        slot = i % 2
        return (pltpu.make_async_copy(wl_hbm.at[:, columns(i)], nbuf.at[slot, pl.ds(0, vocab)], nsem.at[0, slot]),)

    fetch_o(0).start()
    for h in range(2):
        for k, block in enumerate(blocks):
            source = pl.ds(pl.multiple_of(block * 2 * rows + h * rows, rows), rows)
            pltpu.make_async_copy(att_hbm.at[source], left.at[h, k], isem.at[0]).start()
    fetch_o(1).start()
    barrier = pltpu.get_barrier_semaphore()
    for other in others:
        pl.semaphore_signal(barrier, inc=1, device_id={"tp": other}, device_id_type=MESH)
    pl.semaphore_wait(barrier, 7)
    for i in range(steps):
        source = pl.ds(pl.multiple_of(me * 2 * rows + i // tiles * rows, rows), rows)
        pltpu.make_async_copy(hid_hbm.at[source, pl.ds(i % tiles * TILE, TILE)], resid.at[i], isem.at[1]).start()
    pltpu.make_async_copy(left, left, isem.at[0]).wait()
    ssq[...] = jnp.zeros_like(ssq)

    def clear(n):
        acc[n] = jnp.zeros(acc.shape[1:], jnp.float32)

    def finish(h):
        some = pl.ds(h * half, half)

        def one(n):
            cols = pl.ds(pl.multiple_of(n % 4 * 256, 256), 256)
            value = jax.nn.silu(acc[n // 4, some, cols]) * acc[2 + n // 4, some, cols]
            prod[h, :, pl.ds(pl.multiple_of(n * 256, 256), 256)] = value.astype(jnp.bfloat16)

        loop(0, padded // 256, one)

    def streamed(fetch, i, work):
        for copy in fetch(i):
            copy.wait()
        work(i % 2, pl.ds(pl.multiple_of(i // tiles * half, half), half))

        @pl.when(i + 2 < steps)
        def _():
            for copy in fetch(i + 2):
                copy.start()

    def work_one(i):
        @pl.when(i < parts)
        def _():
            clear(i)

        @pl.when(i == 4)
        def _():
            pltpu.make_async_copy(resid, resid, isem.at[1]).wait()
            for slot in range(2):
                gap = jnp.zeros((padded - width, TILE), jnp.bfloat16)
                wbuf[slot, pl.ds(width, padded - width)] = gap
                nbuf[slot, pl.ds(width, padded - width)] = gap
                nbuf[slot, pl.ds(padded + width, padded - width)] = gap
                for copy in fetch_in(slot):
                    copy.start()

    def compute_in(i):
        def work(slot, some):
            left_rows = mbuf[i].reshape(half, TILE)
            for which in range(2):
                for n in range(2):
                    wide = min(side, padded - n * side)
                    weights = nbuf[slot, pl.ds(which * padded + n * side, wide)]
                    acc[which * 2 + n, some, pl.ds(0, wide)] += dot_nt(left_rows, weights)

        streamed(fetch_in, i, work)

    def between(i):
        @pl.when(i == 0)
        def _():
            first.norm(1)
            fetch_d(0).start()
            fetch_d(1).start()
            ssq[...] = jnp.zeros_like(ssq)

        @pl.when(i == 13)
        def _():
            finish(0)

        @pl.when(i == 15)
        def _():
            first.close(0)

        @pl.when(i >= steps)
        def _():
            second.scatter_step(i - steps)

    def work_two(i):
        @pl.when(i == 3)
        def _():
            finish(1)
            first.close(1)
            for slot in range(2):
                for copy in fetch_l(slot):
                    copy.start()

        @pl.when((i >= 4) & (i < 4 + parts))
        def _():
            clear(i - 4)

    def compute_head(i):
        def work(slot, some):
            right_rows = mbuf[i].reshape(half, TILE)
            for n, (start, size) in enumerate(pieces):
                acc[n, pl.ds(0, size), some] += dot_nt(nbuf[slot, pl.ds(start, size)], right_rows)

        streamed(fetch_l, i, work)

    def last(i):
        @pl.when(i == 0)
        def _():
            second.norm(1)

    bufs = (r1, rx, ry, r2x, r2y, ssq)
    first = Exchange(left, fetch_o, wbuf, heads_width, resid, mlp_gain, h_buf, mbuf, bufs, ssem, rsem, free.at[0], work_one, between, compute_in)
    second = Exchange(prod, fetch_d, wbuf, padded, h_buf, final_gain, h_buf, mbuf, bufs, ssem, rsem, free.at[1], work_two, last, compute_head)
    loop(0, steps + 5, first.scatter_step)
    loop(0, steps + 3, first.gather_step)
    loop(3, steps + 5, second.scatter_step)
    loop(0, steps + 3, second.gather_step)
    second.close(0)
    second.close(1)

    best = jnp.full((8, count), -jnp.inf, jnp.float32)
    for n, (start, size) in enumerate(pieces):
        best = jnp.maximum(best, jnp.max(acc[n, pl.ds(0, size)].reshape(size // 8, 8, count), axis=0))
    best = jnp.max(best, axis=0, keepdims=True)
    ids = [id_ref[pl.ds(2 * block + h, 1)] for h in range(2) for block in blocks]
    local_id = jnp.concatenate(ids, axis=1) - me * vocab
    total = jnp.zeros((8, count), jnp.float32)
    picked = jnp.zeros((8, count), jnp.float32)
    for n, (start, size) in enumerate(pieces):
        value = acc[n, pl.ds(0, size)]
        hit = lax.broadcasted_iota(jnp.int32, (size, count), 0) + start == local_id
        total = total + jnp.sum(jnp.exp(value - best).reshape(size // 8, 8, count), axis=0)
        picked = picked + jnp.sum(jnp.where(hit, value, 0.0).reshape(size // 8, 8, count), axis=0)
    for n, values in enumerate((best, jnp.sum(total, axis=0, keepdims=True), jnp.sum(picked, axis=0, keepdims=True))):
        for h in range(2):
            for k, block in enumerate(blocks):
                start = h * half + k * rows
                stats[me, n, pl.ds(2 * block + h, 1)] = values[:, start : start + rows]
    copies = []
    for i, other in enumerate(others):
        copy = pltpu.make_async_remote_copy(
            src_ref=stats.at[me], dst_ref=stats.at[me], send_sem=tsem.at[i], recv_sem=usem.at[i], device_id={"tp": other}, device_id_type=MESH
        )
        copy.start()
        copies.append(copy)
    for copy in copies:
        copy.wait()
    top = stats[0, 0]
    for d in range(1, 8):
        top = jnp.maximum(top, stats[d, 0])
    whole = jnp.zeros_like(top)
    score = jnp.zeros_like(top)
    for d in range(8):
        whole = whole + stats[d, 1] * jnp.exp(stats[d, 0] - top)
        score = score + stats[d, 2]
    norm = top + jnp.log(whole)
    out_ref[0] = norm
    out_ref[1] = score - norm


def tail_stage(mlp_gain, final_gain, score_id, attended, hidden, w_o, gate_t, up_t, w_down, head_t):
    count, dim = hidden.shape
    steps = 2 * dim // TILE
    rows = count // 16
    padded = pl.cdiv(gate_t.shape[0], 256) * 256
    vocab = head_t.shape[0]
    vmem = pl.BlockSpec(memory_space=pltpu.VMEM)
    anywhere = pl.BlockSpec(memory_space=pl.ANY)
    bf16 = jnp.bfloat16
    return pl.pallas_call(
        tail_kernel,
        in_specs=[vmem] * 3 + [anywhere] * 7,
        out_specs=vmem,
        out_shape=jax.ShapeDtypeStruct((2,) + score_id.shape, jnp.float32),
        scratch_shapes=[
            pltpu.VMEM((steps, 2, 2, 2, rows, TILE), bf16),
            pltpu.VMEM((steps, 2, 2, rows, TILE), bf16),
            pltpu.VMEM((steps, 2, rows, HALF), bf16),
            pltpu.VMEM((steps, 2, rows, HALF), bf16),
            pltpu.VMEM((steps, rows, HALF), bf16),
            pltpu.VMEM((steps, rows, HALF), bf16),
            pltpu.VMEM((2, rows, 128), jnp.float32),
            pltpu.VMEM((2, 8, rows, w_o.shape[0]), bf16),
            pltpu.VMEM((2, 8 * rows, padded), bf16),
            pltpu.VMEM((steps, rows, TILE), bf16),
            pltpu.VMEM((steps, rows, TILE), bf16),
            pltpu.VMEM((2, padded, TILE), bf16),
            pltpu.VMEM((2, max(2 * padded, vocab), TILE), bf16),
            pltpu.VMEM((4, 1024, count), jnp.float32),
            pltpu.VMEM((8, 3) + score_id.shape, jnp.float32),
            pltpu.SemaphoreType.DMA((2, 13)),
            pltpu.SemaphoreType.DMA((13, steps)),
            pltpu.SemaphoreType.DMA((2,)),
            pltpu.SemaphoreType.DMA((2, 2)),
            pltpu.SemaphoreType.DMA((2,)),
            pltpu.SemaphoreType.DMA((7,)),
            pltpu.SemaphoreType.DMA((7,)),
            pltpu.SemaphoreType.REGULAR((2, 2)),
        ],
        compiler_params=pltpu.CompilerParams(collective_id=1, has_side_effects=True, vmem_limit_bytes=VMEM_MAX),
        name="tail_stage",
    )(mlp_gain, final_gain, score_id, attended, hidden, w_o, gate_t, up_t, w_down, head_t)


def rope_tables(positions, head_dim):
    half = head_dim // 2
    lane = jnp.arange(head_dim, dtype=jnp.int32)
    inv_freq = 1.0 / (ROPE_THETA ** ((lane % half).astype(jnp.float32) * (2.0 / head_dim)))
    angles = positions.astype(jnp.float32)[:, None] * inv_freq
    return jnp.cos(angles), jnp.sin(angles) * jnp.where(lane < half, -1.0, 1.0)


def solution(mesh):
    def group_step(hidden, tree_mask, depth, ctx_len, block_table, score_id, k_cache, v_cache, attn_norm, w_q, w_k, w_v, w_o, mlp_norm, w_gate, w_up, w_down, final_norm, w_lm):
        requests, nodes, dim = hidden.shape
        head_dim = k_cache.shape[3]
        rows = requests * nodes
        flat = hidden.reshape(rows, dim)
        cosine, sine = rope_tables((ctx_len[:, None] + depth).reshape(rows), head_dim)
        old_k = jnp.transpose(k_cache, (0, 2, 1, 3))
        old_v = jnp.transpose(v_cache, (0, 2, 1, 3))
        attended, k_out, v_out = front_stage(block_table, ctx_len, flat, attn_norm, cosine, sine, tree_mask, w_q, w_k, w_v, old_k, old_v, 4)
        attended = attended.reshape(rows, w_q.shape[1])
        k_out = jnp.transpose(k_out, (0, 2, 1, 3))
        v_out = jnp.transpose(v_out, (0, 2, 1, 3))

        scores = tail_stage(mlp_norm, final_norm, score_id, attended, flat, w_o, w_gate.T, w_up.T, w_down, w_lm.T)
        return scores[0], scores[1], k_out, v_out

    request_spec = P("dp", None, None)
    node_spec = P("dp", None)
    cache_spec = P("dp", None, "tp", None)
    shared_spec = P(None)
    column_spec = P(None, "tp")
    row_spec = P("tp", None)
    in_specs = (request_spec, request_spec, node_spec, P("dp"), node_spec, node_spec, cache_spec, cache_spec, shared_spec, column_spec, column_spec, column_spec, row_spec, shared_spec, column_spec, column_spec, row_spec, shared_spec, column_spec)
    out_specs = (node_spec, node_spec, cache_spec, cache_spec)
    return jax.shard_map(group_step, mesh=mesh, in_specs=in_specs, out_specs=out_specs, check_vma=False)
```
